32 devices in a mesh: clip: 2 (over y), seq: 4 (over z), head: 4 (over x, core).
Axes of the slice: x: 2, y: 2, z: 4, core: 2. Of those that a mesh axis runs over, the one named last changes fastest.
Arguments:
- queries: bfloat16 [16, 4, 16, 3072], P(('clip', 'head'), 'seq'), parts along dimension 0, may hold values from -15 to 15
- attn_keys: bfloat16 [16, 4, 16, 3072], P(('clip', 'head'), 'seq'), parts along dimension 0, may hold values from -5 to 5
- attn_values: bfloat16 [16, 4, 16, 3072], P(('clip', 'head'), 'seq'), parts along dimension 0, may hold values from -5 to 5
- residual: bfloat16 [16, 4, 16, 5120], P(('clip', 'head'), 'seq'), parts along dimension 0, may hold values from -6 to 6
- out_weight: bfloat16 [3072, 5120], P('head', 'seq'), may hold values from -0.109375 to 0.109375
- out_gate: float32 [5120], replicated, may hold values from 0.3 to 3
- head_shift: float32 [5120], replicated, may hold values from -3 to 3
- head_scale: float32 [5120], replicated, may hold values from -1.5 to 1.5
- head_weight: bfloat16 [5120, 64], replicated, may hold values from -0.078125 to 0.078125
- head_bias: float32 [64], replicated, may hold values from -3 to 3
- conv_weight: bfloat16 [3, 3, 3, 16, 384], replicated, may hold values from -0.3125 to 0.3125
- conv_bias: float32 [384], replicated, may hold values from -3 to 3
- norm_gain: float32 [384], replicated, may hold values from 0.5 to 2
Outputs:
- hidden: bfloat16 [16, 4, 16, 5120], P(('clip', 'head'), 'seq'), parts along dimension 0
- features: bfloat16 [16, 8, 32, 384], P(('clip', 'head'), 'seq'), parts along dimension 0
The draws below stay inside these ranges and needn't reach their ends.
There are 2 independent parts, one for each index of `clip`. The reference program is written for one: setup_inputs(seed, part) draws one part's arguments, and reference() takes and returns one part's arrays. A program takes and returns all parts, laid end to end along the dimension named above; an argument that names none is the same for every part. Nothing has to cross between parts.
All inputs are finite; a program needn't handle non-finite values.
Results may differ from the reference program's by a relative error of at most 0.013.
Values may be sent and summed in bfloat16 or wider, within the bound.
A program may use at most 128 MiB of HBM per device.

```python
import math
import jax
import jax.numpy as jnp
from jax import lax

D = 5120
HEAD_DIM = 128
HEADS = 24
LAT_CH = 16
VAE_CH = 384
WP = 16
F = 8
HP = 4
N_HEAD = 4


def draw_queries(key, part):
    count = F * HP * WP
    values = 3.0 * jnp.clip(jax.random.normal(jax.random.fold_in(key, 11), (count, HEADS, HEAD_DIM), jnp.float32), -5.0, 5.0)
    return values.reshape(F, HP, WP, HEADS * HEAD_DIM).astype(jnp.bfloat16)


def draw_attn_keys(key, part):
    count = F * HP * WP
    values = jnp.clip(jax.random.normal(jax.random.fold_in(key, 12), (count, HEADS, HEAD_DIM), jnp.float32), -5.0, 5.0)
    return values.reshape(F, HP, WP, HEADS * HEAD_DIM).astype(jnp.bfloat16)


def block_levels(own_key, dims, shards, low, top_value):
    def one(dim, shards_of):
        heights = jax.random.uniform(jax.random.fold_in(jax.random.fold_in(own_key, 6), dim), (shards_of,), jnp.float32, low / len(shards), top_value / len(shards))
        return jnp.repeat(jnp.exp(heights), dims[dim] // shards_of).reshape((-1,) + (1,) * (len(dims) - dim - 1))

    loudness = one(*shards[0])
    for cut in shards[1:]:
        loudness = loudness * one(*cut)
    return loudness


def centred(own_key, shape, deviation, reach, split=(), held_as=jnp.bfloat16):
    level = block_levels(own_key, shape, split, -0.22, 0.18) if split else 1.0
    entries = jax.random.normal(own_key, shape, jnp.float32) * deviation * level
    return jnp.minimum(jnp.maximum(entries, -reach), reach).astype(held_as)


def setup_inputs(seed: int = 0, part: int = 0) -> dict:
    key_list = jax.random.split(jax.random.key(seed), 14)
    own_keys = jax.random.split(jax.random.fold_in(key_list[13], part), 14)
    queries = draw_queries(jax.random.fold_in(jax.random.fold_in(key_list[13], part), 71), part)
    attn_keys = draw_attn_keys(jax.random.fold_in(jax.random.fold_in(key_list[13], part), 71), part)
    attn_values = centred(own_keys[2], (F, HP, WP, HEADS * HEAD_DIM), 1.0, 5.0, ((0, 4), (1, 4)))
    residual = centred(own_keys[3], (F, HP, WP, D), 1.0, 6.0, ((0, 4), (1, 4)))
    out_weight = centred(key_list[4], (HEADS * HEAD_DIM, D), (HEADS * HEAD_DIM) ** -0.5, 0.109375, ((0, 4), (1, 4)))
    out_gate = jnp.clip(jnp.exp(jax.random.uniform(key_list[5], (D,), jnp.float32, math.log(0.3), math.log(3.0))), 0.3, 3.0)
    head_shift = centred(key_list[6], (D,), 0.5, 3.0, (), jnp.float32)
    head_scale = centred(key_list[7], (D,), 0.3, 1.5, (), jnp.float32)
    head_weight = centred(key_list[8], (D, 4 * LAT_CH), D ** -0.5, 0.078125)
    head_bias = centred(key_list[9], (4 * LAT_CH,), 0.5, 3.0, (), jnp.float32)
    conv_weight = centred(key_list[10], (3, 3, 3, LAT_CH, VAE_CH), (27 * LAT_CH) ** -0.5, 0.3125)
    conv_bias = centred(key_list[11], (VAE_CH,), 0.5, 3.0, (), jnp.float32)
    norm_gain = jnp.clip(jnp.exp(jax.random.uniform(key_list[12], (VAE_CH,), jnp.float32, math.log(0.5), math.log(2.0))), 0.5, 2.0)
    return {"queries": queries, "attn_keys": attn_keys, "attn_values": attn_values, "residual": residual, "out_weight": out_weight, "out_gate": out_gate, "head_shift": head_shift, "head_scale": head_scale, "head_weight": head_weight, "head_bias": head_bias, "conv_weight": conv_weight, "conv_bias": conv_bias, "norm_gain": norm_gain}


def head_latent(hidden, head_shift, head_scale, head_weight, head_bias):
    values = hidden.astype(jnp.float32)
    center = values - lax.optimization_barrier(jnp.mean(values, -1, keepdims=True))
    spread = lax.optimization_barrier(jnp.mean(center * center, -1, keepdims=True))
    normed = (center * lax.rsqrt(spread + 1e-06) * (1.0 + head_scale) + head_shift).astype(jnp.bfloat16)
    flat = normed.reshape(-1, normed.shape[-1])
    latent = (jnp.dot(flat, head_weight, preferred_element_type=jnp.float32) + head_bias).astype(jnp.bfloat16)
    frames, height, breadth = (hidden.shape[0], hidden.shape[1], hidden.shape[2])
    channels = head_weight.shape[1] // 4
    patches = latent.reshape(frames, height, breadth, 2, 2, channels).transpose(0, 1, 3, 2, 4, 5)
    return patches.reshape(frames, height * 2, breadth * 2, channels)

def convolve(padded, frames, conv_weight, conv_bias, norm_gain):
    height = padded.shape[1] - 2
    breadth = padded.shape[2] - 2
    stacked = jnp.concatenate([padded[time_off:time_off + frames, row_off:row_off + height, col_off:col_off + breadth] for time_off in range(3) for row_off in range(3) for col_off in range(3)], -1)
    kernel = conv_weight.reshape(-1, conv_weight.shape[-1])
    linear = jnp.dot(stacked.reshape(-1, stacked.shape[-1]), kernel, preferred_element_type=jnp.float32) + conv_bias
    normed = linear * lax.rsqrt(lax.optimization_barrier(jnp.mean(linear * linear, -1, keepdims=True)) + 1e-06) * norm_gain
    return jax.nn.silu(normed).astype(jnp.bfloat16).reshape(frames, height, breadth, -1)

def one_head(triple):
    query_one, key_one, value_one = triple
    scores = jnp.dot(query_one, key_one.T, preferred_element_type=jnp.float32) * query_one.shape[-1] ** (-0.5)
    peak = lax.optimization_barrier(jnp.max(scores, -1, keepdims=True))
    weights = jnp.exp(scores - peak)
    denominator = lax.optimization_barrier(jnp.sum(weights, -1, keepdims=True))
    product = jnp.dot(weights.astype(jnp.bfloat16), value_one, preferred_element_type=jnp.float32)
    return (product / denominator).astype(jnp.bfloat16)

def add_group(running_sum, pair):
    term = jnp.dot(pair[0], pair[1], preferred_element_type=jnp.float32).astype(jnp.bfloat16)
    term = lax.optimization_barrier(term).astype(jnp.float32)
    return (running_sum + term, None)

def reference(queries, attn_keys, attn_values, residual, out_weight, out_gate, head_shift, head_scale, head_weight, head_bias, conv_weight, conv_bias, norm_gain):
    count = F * HP * WP
    query_heads = queries.reshape(count, HEADS, HEAD_DIM).transpose(1, 0, 2)
    key_heads = attn_keys.reshape(count, HEADS, HEAD_DIM).transpose(1, 0, 2)
    value_heads = attn_values.reshape(count, HEADS, HEAD_DIM).transpose(1, 0, 2)
    attended = lax.map(one_head, (query_heads, key_heads, value_heads))
    attended = attended.transpose(1, 0, 2).reshape(count, HEADS * HEAD_DIM)
    group_width = HEADS // N_HEAD * HEAD_DIM
    groups_in = attended.reshape(count, N_HEAD, group_width).transpose(1, 0, 2)
    weights_in = out_weight.reshape(N_HEAD, group_width, D)
    projected, _ = lax.scan(add_group, jnp.zeros((count, D), jnp.float32), (groups_in, weights_in))
    projected = projected.reshape(F, HP, WP, D)
    hidden = (residual.astype(jnp.float32) + out_gate * projected).astype(jnp.bfloat16)
    video = head_latent(hidden, head_shift, head_scale, head_weight, head_bias)
    padded = jnp.pad(video, ((2, 0), (1, 1), (1, 1), (0, 0)))
    features = convolve(padded, F, conv_weight, conv_bias, norm_gain)
    return (hidden, features)
```

```python
import functools
import math

import jax
import jax.numpy as jnp
from jax import lax
from jax.experimental import pallas as pl
from jax.experimental.pallas import tpu as pltpu
from jax.sharding import PartitionSpec as P

HEAD_DIM = 128


def from_behind(value, axis, steps):
    count = lax.axis_size(axis)
    first, last = (max(0, -steps), min(count, count - steps))
    return lax.ppermute(value, axis, [(source, source + steps) for source in range(first, last)])


def padded_2(x, sides, width):
    for axis, dim in sides:
        peers, length = (lax.axis_size(axis), x.shape[dim])
        up = [(i, (i + 1) % peers) for i in range(peers - 1)]
        down = [(j, i) for i, j in up]
        last = lax.slice_in_dim(x, length - width, length, axis=dim)
        first = lax.slice_in_dim(x, 0, width, axis=dim)
        before = lax.ppermute(last, axis, up)
        after = lax.ppermute(first, axis, down)
        x = jnp.concatenate([before, x, after], axis=dim)
    return x


def head_latent(hidden, head_shift, head_scale, head_weight, head_bias):
    values = hidden.astype(jnp.float32)
    center = values - jnp.mean(values, -1, keepdims=True)
    spread = jnp.mean(center * center, -1, keepdims=True)
    normed = (center * lax.rsqrt(spread + 1e-06) * (1.0 + head_scale) + head_shift).astype(
        jnp.bfloat16
    )
    flat = normed.reshape(-1, normed.shape[-1])
    latent = (jnp.dot(flat, head_weight, preferred_element_type=jnp.float32) + head_bias).astype(
        jnp.bfloat16
    )
    frames, height, breadth = (hidden.shape[0], hidden.shape[1], hidden.shape[2])
    channels = head_weight.shape[1] // 4
    patches = latent.reshape(frames, height, breadth, 2, 2, channels).transpose(0, 1, 3, 2, 4, 5)
    return patches.reshape(frames, height * 2, breadth * 2, channels)


def convolve(padded, frames, conv_weight, conv_bias, norm_gain):
    height = padded.shape[1] - 2
    breadth = padded.shape[2] - 2
    stacked = jnp.concatenate(
        [
            padded[
                time_off : time_off + frames,
                row_off : row_off + height,
                col_off : col_off + breadth,
            ]
            for time_off in range(3)
            for row_off in range(3)
            for col_off in range(3)
        ],
        -1,
    )
    kernel = conv_weight.reshape(-1, conv_weight.shape[-1])
    linear = (
        jnp.dot(stacked.reshape(-1, stacked.shape[-1]), kernel, preferred_element_type=jnp.float32)
        + conv_bias
    )
    normed = linear * lax.rsqrt(jnp.mean(linear * linear, -1, keepdims=True) + 1e-06) * norm_gain
    return jax.nn.silu(normed).astype(jnp.bfloat16).reshape(frames, height, breadth, -1)


def attend_block(carried, block_keys, block_values, query_heads):
    running, denominator, weighted = carried
    scores = jnp.einsum("hqd,khd->hqk", query_heads, block_keys, preferred_element_type=jnp.float32)
    scores = scores * query_heads.shape[-1] ** (-0.5)
    newmax = jnp.maximum(running, jnp.max(scores, -1))
    factor = jnp.exp(running - newmax)
    weights = jnp.exp(scores - newmax[..., None])
    denominator = denominator * factor + jnp.sum(weights, -1)
    product = jnp.einsum(
        "hqk,khd->hqd",
        weights.astype(jnp.bfloat16),
        block_values,
        preferred_element_type=jnp.float32,
    )
    weighted = weighted * factor[..., None] + product
    return (newmax, denominator, weighted)


def fold_pieces(query_heads, carried, pieces):
    key_piece, value_piece = pieces
    frames, height, breadth = (key_piece.shape[0], key_piece.shape[1], key_piece.shape[2])
    heads_here, head_width = (query_heads.shape[0], query_heads.shape[2])
    group_rows = 4

    def regroup(one_piece):
        shaped = one_piece.reshape(
            frames, height // group_rows, group_rows, breadth, heads_here, head_width
        )
        shaped = shaped.transpose(1, 0, 2, 3, 4, 5)
        return shaped.reshape(
            height // group_rows, frames * group_rows * breadth, heads_here, head_width
        )

    def advance(inner, blocks):
        return (attend_block(inner, blocks[0], blocks[1], query_heads), None)

    carried, _ = lax.scan(advance, carried, (regroup(key_piece), regroup(value_piece)))
    return carried


def on_device_gathered(
    queries,
    attn_keys,
    attn_values,
    residual,
    out_weight,
    out_gate,
    head_shift,
    head_scale,
    head_weight,
    head_bias,
    conv_weight,
    conv_bias,
    norm_gain,
):
    head_count = lax.axis_size("head")
    frames_dev = queries.shape[0]
    group_width = queries.shape[3] // head_count
    head_width = HEAD_DIM
    heads_here = group_width // head_width
    local_queries, local_keys, local_values = (
        lax.all_to_all(queries, "head", split_axis=3, concat_axis=0, tiled=True),
        lax.all_to_all(attn_keys, "head", split_axis=3, concat_axis=0, tiled=True),
        lax.all_to_all(attn_values, "head", split_axis=3, concat_axis=0, tiled=True),
    )
    frames_all, height, breadth = (
        local_queries.shape[0],
        local_queries.shape[1],
        local_queries.shape[2],
    )
    count = frames_all * height * breadth
    query_heads = local_queries.reshape(count, heads_here, head_width).transpose(1, 0, 2)
    initial = (
        jnp.full((heads_here, count), -1e30, jnp.float32),
        jnp.zeros((heads_here, count), jnp.float32),
        jnp.zeros((heads_here, count, head_width), jnp.float32),
    )
    carried = fold_pieces(
        query_heads,
        initial,
        (
            lax.all_gather(local_keys, "seq", axis=1, tiled=True),
            lax.all_gather(local_values, "seq", axis=1, tiled=True),
        ),
    )
    running, denominator, weighted = carried
    attended = (weighted / denominator[..., None]).astype(jnp.bfloat16)
    attended = attended.transpose(1, 0, 2).reshape(count, group_width)
    partial_value = jnp.dot(
        attended,
        lax.all_gather(out_weight, "seq", axis=1, tiled=True),
        preferred_element_type=jnp.float32,
    )
    partial_value = partial_value.reshape(frames_all, height, breadth, partial_value.shape[-1])
    owned = lax.psum_scatter(
        partial_value.astype(jnp.bfloat16), "head", scatter_dimension=0, tiled=True
    ).astype(jnp.float32)
    hidden = (residual.astype(jnp.float32) + out_gate * owned).astype(jnp.bfloat16)
    own_video = head_latent(hidden, head_shift, head_scale, head_weight, head_bias)
    earlier = from_behind(own_video, "head", 1)
    video = jnp.concatenate([earlier, own_video], 0)
    extended = padded_2(video, (("seq", 1),), 1)
    padded = jnp.pad(extended, ((0, 0), (0, 0), (1, 1), (0, 0)))
    features = convolve(padded, frames_dev, conv_weight, conv_bias, norm_gain)
    return (hidden, features)


MESH = pl.DeviceIdType.MESH


class Plan:
    def __init__(self, ns, nh, queries, residual, out_weight):
        self.ns, self.nh = ns, nh
        self.frames = queries.shape[0]
        self.cells = queries.shape[1] * queries.shape[2]
        self.inner = queries.shape[3]
        self.tokens = self.frames * self.cells
        self.group = self.inner // nh // HEAD_DIM
        self.few = max(1, self.group // 6)
        self.width = residual.shape[3]
        self.columns = out_weight.shape[1]
        self.slots = ns * nh
        self.chunk = 256 if self.columns % 256 == 0 else 128
        self.chunks = self.columns // self.chunk
        self.counts = (2 * self.few, self.few, self.few, 2 * self.few)
        self.owner = [o for o, count in enumerate(self.counts) for _ in range(count)]

    def fits(self, queries):
        return (
            self.nh == 4
            and self.ns == 4
            and self.group == 6 * self.few
            and self.inner == self.nh * self.group * HEAD_DIM
            and self.frames == 2
            and self.cells % 16 == 0
            and self.columns % 128 == 0
            and self.slots * self.tokens <= 1024
        )


SENDS = ((2, 1), (2, 0), (1, 3), (1, 2))
RELAY = ((2, 3), (2, 3), (1, 0), (1, 0))


def block_kernel(
    plan,
    q_hbm, k_hbm, v_hbm, res_hbm, w_hbm, hw_hbm,
    gate_ref, shift_ref, scale_ref, bias_ref,
    hidden_ref, near_ref,
    qkv, qs, kv, att, weight, res, head_w, term, landed0, landed1, final, patch, halo,
    local_sem, s1, r1, s3, r3, s5, r5, s6, r6, s7, r7,
):
    p = plan
    s = lax.axis_index("seq")
    h = lax.axis_index("head")
    core, across = h & 1, h >> 1

    def slot(seq_index, head_index):
        return ((head_index & 1) * 2 + (head_index >> 1)) * p.ns + seq_index

    here = slot(s, h)
    at_end = (s == 0) | (s == p.ns - 1)
    offsets = [(ds, dh) for ds in (2, 1, 3, 0) for dh in range(p.nh) if ds or dh]
    widths = ((2 * p.few, True), (p.few, False))

    def columns_of(seq_index, head_index):
        before = p.few * (seq_index + jnp.minimum(seq_index, 1))
        return pl.multiple_of((head_index * p.group + before) * HEAD_DIM, HEAD_DIM)

    loads = [
        pltpu.make_async_copy(q_hbm, qkv.at[0], local_sem.at[0]),
        pltpu.make_async_copy(k_hbm, qkv.at[1], local_sem.at[1]),
        pltpu.make_async_copy(v_hbm, qkv.at[2], local_sem.at[2]),
    ]
    late = [
        pltpu.make_async_copy(w_hbm, weight, local_sem.at[3]),
        pltpu.make_async_copy(res_hbm, res, local_sem.at[4]),
        pltpu.make_async_copy(hw_hbm, head_w, local_sem.at[5]),
    ]

    def own_copies(heads):
        cols, fill = pl.ds(columns_of(s, h), heads * HEAD_DIM), pl.ds(0, heads * HEAD_DIM)
        return [
            pltpu.make_async_copy(q_hbm.at[:, :, cols], qs.at[:, here, :, fill], local_sem.at[6]),
            pltpu.make_async_copy(k_hbm.at[:, :, cols], kv.at[0, :, here, :, fill], local_sem.at[7]),
            pltpu.make_async_copy(v_hbm.at[:, :, cols], kv.at[1, :, here, :, fill], local_sem.at[8]),
        ]

    def by_class(end, act):
        for heads, wanted in widths:
            pl.when(end == wanted)(functools.partial(act, heads))

    for copy in loads:
        copy.start()

    barrier = pltpu.get_barrier_semaphore()
    for ds, dh in offsets:
        pl.semaphore_signal(
            barrier,
            inc=1,
            device_id={"seq": lax.rem(s + ds, p.ns), "head": lax.rem(h + dh, p.nh)},
            device_id_type=MESH,
        )

    @functools.partial(by_class, at_end)
    def _(heads):
        for copy in own_copies(heads):
            copy.start()

    for copy in loads:
        copy.wait()
    pl.semaphore_wait(barrier, len(offsets))

    def exchange(phase, index, from_slot, to_s, to_h, heads):
        cols, fill = pl.ds(columns_of(to_s, to_h), heads * HEAD_DIM), pl.ds(0, heads * HEAD_DIM)
        if phase == 0:
            source, target = qkv.at[pl.ds(1, 2), :, :, cols], kv.at[:, :, from_slot, :, fill]
        else:
            source, target = qkv.at[0, phase - 1, :, cols], qs.at[phase - 1, from_slot, :, fill]
        return pltpu.make_async_remote_copy(
            src_ref=source,
            dst_ref=target,
            send_sem=s1.at[phase, index],
            recv_sem=r1.at[phase, index],
            device_id={"seq": to_s, "head": to_h},
            device_id_type=MESH,
        )

    def for_sends(phase, act):
        for ds in sorted(set(ds for ds, _ in offsets), key=[2, 1, 3, 0].index):
            to_s = lax.rem(s + ds, p.ns)

            @functools.partial(by_class, (to_s == 0) | (to_s == p.ns - 1))
            def _(heads, ds=ds, to_s=to_s):
                for index, (ds2, dh) in enumerate(offsets):
                    if ds2 == ds:
                        act(exchange(phase, index, here, to_s, lax.rem(h + dh, p.nh), heads))

    def arrivals(phase):
        @functools.partial(by_class, at_end)
        def _(heads):
            for index, (ds, dh) in enumerate(offsets):
                from_s, from_h = lax.rem(s - ds + p.ns, p.ns), lax.rem(h - dh + p.nh, p.nh)
                exchange(phase, index, slot(from_s, from_h), s, h, heads).wait_recv()

    for phase in range(3):
        for_sends(phase, lambda copy: copy.start())
    for copy in late:
        copy.start()

    def hop(head, f, to_s, way):
        return pltpu.make_async_remote_copy(
            src_ref=att.at[f, head],
            dst_ref=att.at[f, head],
            send_sem=s3.at[way, f, head],
            recv_sem=r3.at[f, head],
            device_id={"seq": to_s},
            device_id_type=MESH,
        )

    def attend(f, j):
        lanes = slice(j * HEAD_DIM, (j + 1) * HEAD_DIM)
        q = qs[f, :, :, lanes].reshape(-1, HEAD_DIM)
        k = kv[0, :, :, :, lanes].reshape(-1, HEAD_DIM)
        v = kv[1, :, :, :, lanes].reshape(-1, HEAD_DIM)
        scores = lax.dot_general(
            q, k, (((1,), (1,)), ((), ())), preferred_element_type=jnp.float32
        )
        scores = scores * HEAD_DIM ** (-0.5)
        weights = jnp.exp(scores - jnp.max(scores, -1, keepdims=True))
        denominator = jnp.sum(weights, -1, keepdims=True)
        product = jnp.dot(weights.astype(jnp.bfloat16), v, preferred_element_type=jnp.float32)
        att[f, p.few * (s + jnp.minimum(s, 1)) + j] = (product / denominator).astype(jnp.bfloat16)

    def send_own(f, j, way):
        for o in range(p.ns):
            if j < p.counts[o]:
                head = p.owner.index(o) + j

                @pl.when(s == o)
                def _():
                    hop(head, f, SENDS[o][way], way).start()

    for f in range(p.frames):
        if f == 0:
            @functools.partial(by_class, at_end)
            def _(heads):
                for copy in own_copies(heads):
                    copy.wait()

            arrivals(0)
        arrivals(1 + f)
        for j in range(p.few):
            attend(f, j)
            send_own(f, j, 0)
        for j in range(p.few, 2 * p.few):
            @pl.when(at_end)
            def _():
                attend(f, j)

            send_own(f, j, 0)
        for j in range(2 * p.few):
            send_own(f, j, 1)

    def order(row):
        others = [head for head in range(p.group) if p.owner[head] != row]
        relayed = {head: row == RELAY[p.owner[head]][0] for head in others}
        return sorted(
            others,
            key=lambda head: (
                abs(p.owner[head] - row) if relayed[head] or row in (0, p.ns - 1) else 9, head,
            ),
        )

    def take(f, head, row):
        hop(head, f, row, 0).wait_recv()
        relay, last = RELAY[p.owner[head]]
        if row == relay:
            hop(head, f, last, 0).start()

    def gather(todo):
        for row in range(p.ns):
            @pl.when(s == row)
            def _():
                for f, head in todo(row):
                    take(f, head, row)

    def first_part(row):
        heads = order(row)
        near = [head for head in heads if abs(p.owner[head] - row) == 1 and p.owner[head] in (1, 2)]
        early = near if row in (1, 2) else []
        return [(0, head) for head in early] + [(1, head) for head in early] + [
            (0, head) for head in heads if head not in early
        ]

    def second_part(row):
        done = first_part(row)
        return [(1, head) for head in order(row) if (1, head) not in done]

    def halving(f, c, b):
        bit = core if b == 0 else across
        source = term.at[f, c, 1 - bit] if b == 0 else landed0.at[f, c, 1 - bit]
        target = landed0.at[f, c] if b == 0 else landed1.at[f, c]
        return pltpu.make_async_remote_copy(
            src_ref=source,
            dst_ref=target,
            send_sem=s5.at[b, f, c],
            recv_sem=r5.at[b, f, c],
            device_id={"head": h + (1 - 2 * bit) * (1 << b)},
            device_id_type=MESH,
        )

    def project(f, c):
        cols = pl.ds(c * p.chunk, p.chunk)
        rows = jnp.concatenate([att[f, head] for head in range(p.group)], axis=1)
        product = jnp.dot(rows, weight[:, cols], preferred_element_type=jnp.float32)
        term[f, c] = product.astype(jnp.bfloat16).reshape(term.shape[2:])
        halving(f, c, 0).start()

    def pair_sum(f, c):
        halving(f, c, 0).wait_recv()
        total = term[f, c, core].astype(jnp.float32) + landed0[f, c].astype(jnp.float32)
        landed0[f, c] = total.astype(jnp.bfloat16)
        halving(f, c, 1).start()

    def to_owner(f, c, ds, row):
        to_s = lax.rem(s + ds, p.ns)
        return pltpu.make_async_remote_copy(
            src_ref=landed1.at[f, c, to_s],
            dst_ref=final.at[f, c, row],
            send_sem=s6.at[ds - 1, f, c],
            recv_sem=r6.at[ds - 1, f, c],
            device_id={"seq": to_s},
            device_id_type=MESH,
        )

    def full_sum(f, c):
        halving(f, c, 1).wait_recv()
        total = landed0[f, c, across].astype(jnp.float32) + landed1[f, c].astype(jnp.float32)
        landed1[f, c] = total.astype(jnp.bfloat16)
        for ds in (2, 1, 3):
            to_owner(f, c, ds, s).start()
        final[f, c, s] = landed1[f, c, s]

    gather(first_part)
    late[0].wait()
    for c in range(p.chunks):
        project(0, c)
    for c in range(p.chunks):
        pair_sum(0, c)
    gather(second_part)
    for c in range(p.chunks):
        project(1, c)
    for c in range(p.chunks):
        pair_sum(1, c)
        full_sum(0, c)
    for copy in late[1:]:
        copy.wait()

    def finish(f, c, sums):
        for ds in range(1, p.ns):
            to_owner(f, c, ds, lax.rem(s - ds + p.ns, p.ns)).wait_recv()
        rows = slice(f * p.cells, (f + 1) * p.cells)
        for j in range(p.ns):
            cols = slice(j * p.columns + c * p.chunk, j * p.columns + (c + 1) * p.chunk)
            added = gate_ref[:, cols] * final[f, c, j].astype(jnp.float32)
            value = (res[rows, cols].astype(jnp.float32) + added).astype(jnp.bfloat16)
            hidden_ref[rows, cols] = value
            sums = sums + jnp.sum(value.astype(jnp.float32), -1, keepdims=True)
        return sums

    sums = [jnp.zeros((p.cells, 1), jnp.float32) for _ in range(p.frames)]
    for c in range(p.chunks):
        full_sum(1, c)
        sums[0] = finish(0, c, sums[0])
    for c in range(p.chunks):
        sums[1] = finish(1, c, sums[1])
    mean = jnp.concatenate(sums, axis=0) / p.width
    center = hidden_ref[...].astype(jnp.float32) - mean
    spread = jnp.mean(center * center, -1, keepdims=True)
    normed = center * lax.rsqrt(spread + 1e-06) * (1.0 + scale_ref[...]) + shift_ref[...]
    values = lax.dot_general(
        normed.astype(jnp.bfloat16),
        head_w[...],
        (((1,), (1,)), ((), ())),
        preferred_element_type=jnp.float32,
    )
    values = (values + bias_ref[...]).astype(jnp.bfloat16)
    features = values.shape[-1]
    patch[...] = jnp.zeros_like(patch)
    patch[:, :features] = values

    moves = [(0, 1), (0, -1), (1, 0), (1, 1), (1, -1)]

    def edge(index, sign):
        dh, ds = moves[index]
        return (
            (h + sign * dh >= 0) & (h + sign * dh < p.nh)
            & (s + sign * ds >= 0) & (s + sign * ds < p.ns)
        )

    def reach(index):
        dh, ds = moves[index]
        return pltpu.make_async_remote_copy(
            src_ref=patch,
            dst_ref=halo.at[index],
            send_sem=s7.at[index],
            recv_sem=r7.at[index],
            device_id={"seq": lax.rem(s + ds + p.ns, p.ns), "head": lax.rem(h + dh, p.nh)},
            device_id_type=MESH,
        )

    for index in range(len(moves)):

        @pl.when(edge(index, 1))
        def _():
            reach(index).start()

    near_ref[1, 1] = values
    for index, (dh, ds) in enumerate(moves):

        @pl.when(edge(index, -1))
        def _():
            reach(index).wait_recv()
            near_ref[1 - dh, 1 - ds] = halo[index][:, :features]

        @pl.when(jnp.logical_not(edge(index, -1)))
        def _():
            near_ref[1 - dh, 1 - ds] = jnp.zeros_like(values)

    for index in range(len(moves)):

        @pl.when(edge(index, 1))
        def _():
            reach(index).wait_send()

    for phase in range(3):
        for_sends(phase, lambda copy: copy.wait_send())

    for row in range(p.ns):
        @pl.when(s == row)
        def _():
            for f in range(p.frames):
                for head in range(p.group):
                    o = p.owner[head]
                    if o == row:
                        for way in range(2):
                            hop(head, f, SENDS[o][way], way).wait_send()
                    elif RELAY[o][0] == row:
                        hop(head, f, RELAY[o][1], 0).wait_send()

    for f in range(p.frames):
        for c in range(p.chunks):
            for b in range(2):
                halving(f, c, b).wait_send()
            for ds in range(1, p.ns):
                to_owner(f, c, ds, s).wait_send()


def on_device(
    queries,
    attn_keys,
    attn_values,
    residual,
    out_weight,
    out_gate,
    head_shift,
    head_scale,
    head_weight,
    head_bias,
    conv_weight,
    conv_bias,
    norm_gain,
):
    ns, nh = lax.axis_size("seq"), lax.axis_size("head")
    p = Plan(ns, nh, queries, residual, out_weight)
    if not p.fits(queries):
        return on_device_gathered(
            queries, attn_keys, attn_values, residual, out_weight, out_gate, head_shift,
            head_scale, head_weight, head_bias, conv_weight, conv_bias, norm_gain,
        )
    frames, height, breadth, inner = queries.shape
    t, cells, width, patch_size = p.tokens, p.cells, p.width, head_weight.shape[1]
    dma, bf16 = pltpu.SemaphoreType.DMA, jnp.bfloat16
    lanes = -(-patch_size // 128) * 128
    most = 2 * p.few * HEAD_DIM
    any_spec = pl.BlockSpec(memory_space=pl.ANY)
    vmem = pl.BlockSpec(memory_space=pltpu.VMEM)
    hidden, near = pl.pallas_call(
        functools.partial(block_kernel, p),
        out_shape=(
            jax.ShapeDtypeStruct((t, width), bf16),
            jax.ShapeDtypeStruct((2, 3, t, patch_size), bf16),
        ),
        in_specs=[any_spec] * 6 + [vmem] * 4,
        out_specs=(vmem, vmem),
        scratch_shapes=[
            pltpu.VMEM((3, frames, cells, inner), bf16),
            pltpu.VMEM((frames, p.slots, cells, most), bf16),
            pltpu.VMEM((2, frames, p.slots, cells, most), bf16),
            pltpu.VMEM((frames, p.group, p.slots * cells, HEAD_DIM), bf16),
            pltpu.VMEM(out_weight.shape, bf16),
            pltpu.VMEM((t, width), bf16),
            pltpu.VMEM(head_weight.shape[::-1], bf16),
            pltpu.VMEM((frames, p.chunks, 2, 2, ns, cells, p.chunk), bf16),
            pltpu.VMEM((frames, p.chunks, 2, ns, cells, p.chunk), bf16),
            pltpu.VMEM((frames, p.chunks, ns, cells, p.chunk), bf16),
            pltpu.VMEM((frames, p.chunks, ns, cells, p.chunk), bf16),
            pltpu.VMEM((t, lanes), bf16),
            pltpu.VMEM((5, t, lanes), bf16),
            dma((9,)),
            dma((3, p.slots - 1)),
            dma((3, p.slots - 1)),
            dma((2, frames, p.group)),
            dma((frames, p.group)),
            dma((2, frames, p.chunks)),
            dma((2, frames, p.chunks)),
            dma((ns - 1, frames, p.chunks)),
            dma((ns - 1, frames, p.chunks)),
            dma((5,)),
            dma((5,)),
        ],
        compiler_params=pltpu.CompilerParams(
            collective_id=0, has_side_effects=True, vmem_limit_bytes=60 * 1024 * 1024
        ),
    )(
        queries.reshape(frames, cells, inner),
        attn_keys.reshape(frames, cells, inner),
        attn_values.reshape(frames, cells, inner),
        residual.reshape(t, width),
        out_weight,
        head_weight.T,
        out_gate.reshape(1, -1),
        head_shift.reshape(1, -1),
        head_scale.reshape(1, -1),
        head_bias.reshape(1, -1),
    )
    channels = patch_size // 4
    video = near.reshape(2, 3, frames, height, breadth, 2, 2, channels)
    video = video.transpose(0, 2, 1, 3, 5, 4, 6, 7)
    video = video.reshape(2, frames, 3 * height * 2, breadth * 2, channels)
    video = jnp.concatenate([video[0, -2:], video[1]], 0)
    rows = height * 2
    video = video[:, rows - 1 : 2 * rows + 1]
    padded = jnp.pad(video, ((0, 0), (0, 0), (1, 1), (0, 0)))
    features = convolve(padded, frames, conv_weight, conv_bias, norm_gain)
    return (hidden.reshape(residual.shape), features)


def solution(mesh):
    return jax.shard_map(
        on_device,
        mesh=mesh,
        in_specs=(
            P(("clip", "head"), "seq", None, None),
            P(("clip", "head"), "seq", None, None),
            P(("clip", "head"), "seq", None, None),
            P(("clip", "head"), "seq", None, None),
            P("head", "seq"),
            P(),
            P(),
            P(),
            P(),
            P(),
            P(),
            P(),
            P(),
        ),
        out_specs=(P(("clip", "head"), "seq", None, None), P(("clip", "head"), "seq", None, None)),
        check_vma=False,
    )
```

```python
import functools
import math

import jax
import jax.numpy as jnp
from jax import lax
from jax.experimental import pallas as pl
from jax.experimental.pallas import tpu as pltpu
from jax.sharding import PartitionSpec as P

HEAD_DIM = 128


def from_behind(value, axis, steps):
    count = lax.axis_size(axis)
    first, last = (max(0, -steps), min(count, count - steps))
    return lax.ppermute(value, axis, [(source, source + steps) for source in range(first, last)])


def padded_2(x, sides, width):
    for axis, dim in sides:
        peers, length = (lax.axis_size(axis), x.shape[dim])
        up = [(i, (i + 1) % peers) for i in range(peers - 1)]
        down = [(j, i) for i, j in up]
        last = lax.slice_in_dim(x, length - width, length, axis=dim)
        first = lax.slice_in_dim(x, 0, width, axis=dim)
        before = lax.ppermute(last, axis, up)
        after = lax.ppermute(first, axis, down)
        x = jnp.concatenate([before, x, after], axis=dim)
    return x


def head_latent(hidden, head_shift, head_scale, head_weight, head_bias):
    values = hidden.astype(jnp.float32)
    center = values - jnp.mean(values, -1, keepdims=True)
    spread = jnp.mean(center * center, -1, keepdims=True)
    normed = (center * lax.rsqrt(spread + 1e-06) * (1.0 + head_scale) + head_shift).astype(
        jnp.bfloat16
    )
    flat = normed.reshape(-1, normed.shape[-1])
    latent = (jnp.dot(flat, head_weight, preferred_element_type=jnp.float32) + head_bias).astype(
        jnp.bfloat16
    )
    frames, height, breadth = (hidden.shape[0], hidden.shape[1], hidden.shape[2])
    channels = head_weight.shape[1] // 4
    patches = latent.reshape(frames, height, breadth, 2, 2, channels).transpose(0, 1, 3, 2, 4, 5)
    return patches.reshape(frames, height * 2, breadth * 2, channels)


def convolve(padded, frames, conv_weight, conv_bias, norm_gain):
    height = padded.shape[1] - 2
    breadth = padded.shape[2] - 2
    stacked = jnp.concatenate(
        [
            padded[
                time_off : time_off + frames,
                row_off : row_off + height,
                col_off : col_off + breadth,
            ]
            for time_off in range(3)
            for row_off in range(3)
            for col_off in range(3)
        ],
        -1,
    )
    kernel = conv_weight.reshape(-1, conv_weight.shape[-1])
    linear = (
        jnp.dot(stacked.reshape(-1, stacked.shape[-1]), kernel, preferred_element_type=jnp.float32)
        + conv_bias
    )
    normed = linear * lax.rsqrt(jnp.mean(linear * linear, -1, keepdims=True) + 1e-06) * norm_gain
    return jax.nn.silu(normed).astype(jnp.bfloat16).reshape(frames, height, breadth, -1)


def attend_block(carried, block_keys, block_values, query_heads):
    running, denominator, weighted = carried
    scores = jnp.einsum("hqd,khd->hqk", query_heads, block_keys, preferred_element_type=jnp.float32)
    scores = scores * query_heads.shape[-1] ** (-0.5)
    newmax = jnp.maximum(running, jnp.max(scores, -1))
    factor = jnp.exp(running - newmax)
    weights = jnp.exp(scores - newmax[..., None])
    denominator = denominator * factor + jnp.sum(weights, -1)
    product = jnp.einsum(
        "hqk,khd->hqd",
        weights.astype(jnp.bfloat16),
        block_values,
        preferred_element_type=jnp.float32,
    )
    weighted = weighted * factor[..., None] + product
    return (newmax, denominator, weighted)


def fold_pieces(query_heads, carried, pieces):
    key_piece, value_piece = pieces
    frames, height, breadth = (key_piece.shape[0], key_piece.shape[1], key_piece.shape[2])
    heads_here, head_width = (query_heads.shape[0], query_heads.shape[2])
    group_rows = 4

    def regroup(one_piece):
        shaped = one_piece.reshape(
            frames, height // group_rows, group_rows, breadth, heads_here, head_width
        )
        shaped = shaped.transpose(1, 0, 2, 3, 4, 5)
        return shaped.reshape(
            height // group_rows, frames * group_rows * breadth, heads_here, head_width
        )

    def advance(inner, blocks):
        return (attend_block(inner, blocks[0], blocks[1], query_heads), None)

    carried, _ = lax.scan(advance, carried, (regroup(key_piece), regroup(value_piece)))
    return carried


def on_device_gathered(
    queries,
    attn_keys,
    attn_values,
    residual,
    out_weight,
    out_gate,
    head_shift,
    head_scale,
    head_weight,
    head_bias,
    conv_weight,
    conv_bias,
    norm_gain,
):
    head_count = lax.axis_size("head")
    frames_dev = queries.shape[0]
    group_width = queries.shape[3] // head_count
    head_width = HEAD_DIM
    heads_here = group_width // head_width
    local_queries, local_keys, local_values = (
        lax.all_to_all(queries, "head", split_axis=3, concat_axis=0, tiled=True),
        lax.all_to_all(attn_keys, "head", split_axis=3, concat_axis=0, tiled=True),
        lax.all_to_all(attn_values, "head", split_axis=3, concat_axis=0, tiled=True),
    )
    frames_all, height, breadth = (
        local_queries.shape[0],
        local_queries.shape[1],
        local_queries.shape[2],
    )
    count = frames_all * height * breadth
    query_heads = local_queries.reshape(count, heads_here, head_width).transpose(1, 0, 2)
    initial = (
        jnp.full((heads_here, count), -1e30, jnp.float32),
        jnp.zeros((heads_here, count), jnp.float32),
        jnp.zeros((heads_here, count, head_width), jnp.float32),
    )
    carried = fold_pieces(
        query_heads,
        initial,
        (
            lax.all_gather(local_keys, "seq", axis=1, tiled=True),
            lax.all_gather(local_values, "seq", axis=1, tiled=True),
        ),
    )
    running, denominator, weighted = carried
    attended = (weighted / denominator[..., None]).astype(jnp.bfloat16)
    attended = attended.transpose(1, 0, 2).reshape(count, group_width)
    partial_value = jnp.dot(
        attended,
        lax.all_gather(out_weight, "seq", axis=1, tiled=True),
        preferred_element_type=jnp.float32,
    )
    partial_value = partial_value.reshape(frames_all, height, breadth, partial_value.shape[-1])
    owned = lax.psum_scatter(
        partial_value.astype(jnp.bfloat16), "head", scatter_dimension=0, tiled=True
    ).astype(jnp.float32)
    hidden = (residual.astype(jnp.float32) + out_gate * owned).astype(jnp.bfloat16)
    own_video = head_latent(hidden, head_shift, head_scale, head_weight, head_bias)
    earlier = from_behind(own_video, "head", 1)
    video = jnp.concatenate([earlier, own_video], 0)
    extended = padded_2(video, (("seq", 1),), 1)
    padded = jnp.pad(extended, ((0, 0), (0, 0), (1, 1), (0, 0)))
    features = convolve(padded, frames_dev, conv_weight, conv_bias, norm_gain)
    return (hidden, features)


MESH = pl.DeviceIdType.MESH


class Plan:
    def __init__(self, ns, nh, queries, residual, out_weight):
        self.ns, self.nh = ns, nh
        self.frames = queries.shape[0]
        self.cells = queries.shape[1] * queries.shape[2]
        self.inner = queries.shape[3]
        self.tokens = self.frames * self.cells
        self.group = self.inner // nh // HEAD_DIM
        self.few = max(1, self.group // 6)
        self.width = residual.shape[3]
        self.columns = out_weight.shape[1]
        self.slots = ns * nh
        self.chunk = 256 if self.columns % 256 == 0 else 128
        self.chunks = self.columns // self.chunk
        self.cuts = 2
        self.counts = (2 * self.few, self.few, self.few, 2 * self.few)
        self.owner = [o for o, count in enumerate(self.counts) for _ in range(count)]

    def fits(self, queries, head_weight, conv_weight):
        return (
            self.nh == 4
            and self.ns == 4
            and self.group == 6 * self.few
            and self.inner == self.nh * self.group * HEAD_DIM
            and self.frames == 2
            and self.cells % 16 == 0
            and self.columns % 128 == 0
            and queries.shape[1] == 1
            and head_weight.shape[1] == 64
            and conv_weight.shape[3] == 16
            and conv_weight.shape[4] % 128 == 0
            and self.slots * self.tokens <= 1024
        )


def source_row(o, j, row):
    step = 1 if row > o else -1
    if o in (1, 2) or j % 2 == 0:
        return row - step
    return o if abs(row - o) < 3 else row - step


def due(o, j, f, row):
    away = abs(row - o)
    if o in (1, 2):
        return 3.0 * away
    if j % 2 == 0:
        return 14.4 + 2.8 * f + 2.8 * away
    return 20.4 + 1.4 * f + 2.4 if away == 1 else 16.7 + 2.8 * f + 2.8 * (away - 1)


def block_kernel(
    plan,
    q_hbm, k_hbm, v_hbm, res_hbm, w_hbm, hw_hbm,
    gate_hbm, shift_hbm, scale_hbm, bias_hbm, cw_hbm, cb_hbm, gain_hbm,
    hidden_ref, near_ref, wide_ref, rows_ref,
    qkv, got, att, weight, res, head_w, gate_ref, shift_ref, scale_ref, bias_ref, conv_w, bias_row, gain_row, term, landed0, landed1, final, patch, halo,
    local_sem, s1, r1, s3, r3, s5, r5, s6, r6, s7, r7,
):
    p = plan
    s = lax.axis_index("seq")
    h = lax.axis_index("head")
    core, across = h & 1, h >> 1
    row_pair = (bias_row, gain_row)

    def slot(seq_index, head_index):
        return ((head_index & 1) * 2 + (head_index >> 1)) * p.ns + seq_index

    here = slot(s, h)
    at_end = (s == 0) | (s == p.ns - 1)
    offsets = [(ds, dh) for ds in (2, 1, 3, 0) for dh in range(p.nh) if ds or dh]
    widths = ((2 * p.few, True), (p.few, False))

    def columns_of(seq_index, head_index):
        before = p.few * (seq_index + jnp.minimum(seq_index, 1))
        return pl.multiple_of((head_index * p.group + before) * HEAD_DIM, HEAD_DIM)

    loads = [
        pltpu.make_async_copy(q_hbm, qkv.at[0], local_sem.at[0]),
        pltpu.make_async_copy(k_hbm, qkv.at[1], local_sem.at[1]),
        pltpu.make_async_copy(v_hbm, qkv.at[2], local_sem.at[2]),
    ]
    late = [
        pltpu.make_async_copy(w_hbm, weight, local_sem.at[3]),
        pltpu.make_async_copy(res_hbm, res, local_sem.at[4]),
        pltpu.make_async_copy(hw_hbm, head_w, local_sem.at[5]),
        pltpu.make_async_copy(gate_hbm, gate_ref, local_sem.at[9]),
        pltpu.make_async_copy(shift_hbm, shift_ref, local_sem.at[10]),
        pltpu.make_async_copy(scale_hbm, scale_ref, local_sem.at[11]),
        pltpu.make_async_copy(bias_hbm, bias_ref, local_sem.at[12]),
        pltpu.make_async_copy(cb_hbm, row_pair[0], local_sem.at[13]),
        pltpu.make_async_copy(gain_hbm, row_pair[1], local_sem.at[14]),
    ]
    conv_load = pltpu.make_async_copy(cw_hbm, conv_w, local_sem.at[15])

    def own_copies(heads):
        cols, fill = pl.ds(columns_of(s, h), heads * HEAD_DIM), pl.ds(0, heads * HEAD_DIM)
        return [
            pltpu.make_async_copy(
                ref.at[:, :, cols], got.at[i, :, here, :, fill], local_sem.at[6 + i]
            )
            for i, ref in enumerate((q_hbm, k_hbm, v_hbm))
        ]

    def by_class(end, act):
        for heads, wanted in widths:
            pl.when(end == wanted)(functools.partial(act, heads))

    for copy in loads:
        copy.start()

    barrier = pltpu.get_barrier_semaphore()
    for ds, dh in offsets:
        pl.semaphore_signal(
            barrier,
            inc=1,
            device_id={"seq": lax.rem(s + ds, p.ns), "head": lax.rem(h + dh, p.nh)},
            device_id_type=MESH,
        )

    @functools.partial(by_class, at_end)
    def _(heads):
        for copy in own_copies(heads):
            copy.start()

    for copy in loads:
        copy.wait()
    pl.semaphore_wait(barrier, len(offsets))

    def exchange(phase, index, from_slot, to_s, to_h, heads):
        cols, fill = pl.ds(columns_of(to_s, to_h), heads * HEAD_DIM), pl.ds(0, heads * HEAD_DIM)
        if heads == p.few:
            source, target = qkv.at[:, :, :, cols], got.at[:, :, from_slot, :, fill]
        elif phase == 0:
            kinds = pl.ds(1, 2)
            source, target = qkv.at[kinds, :, :, cols], got.at[kinds, :, from_slot, :, fill]
        else:
            f = phase - 1
            source, target = qkv.at[0, f, :, cols], got.at[0, f, from_slot, :, fill]
        return pltpu.make_async_remote_copy(
            src_ref=source,
            dst_ref=target,
            send_sem=s1.at[phase, index],
            recv_sem=r1.at[phase, index],
            device_id={"seq": to_s, "head": to_h},
            device_id_type=MESH,
        )

    def for_sends(phase, heads, act):
        for ds in range(p.ns):
            to_s = lax.rem(s + ds, p.ns)

            @pl.when(((to_s == 0) | (to_s == p.ns - 1)) == (heads > p.few))
            def _():
                for index, (ds2, dh) in enumerate(offsets):
                    if ds2 == ds:
                        act(exchange(phase, index, here, to_s, lax.rem(h + dh, p.nh), heads))

    def arrivals(phase, heads):
        @pl.when(at_end == (heads > p.few))
        def _():
            for index, (ds, dh) in enumerate(offsets):
                from_s, from_h = lax.rem(s - ds + p.ns, p.ns), lax.rem(h - dh + p.nh, p.nh)
                exchange(phase, index, slot(from_s, from_h), s, h, heads).wait_recv()

    stages = [(0, p.few)] + [(phase, 2 * p.few) for phase in range(1 + p.frames)]
    for phase, heads in stages:
        for_sends(phase, heads, lambda copy: copy.start())
    conv_load.start()
    for copy in late:
        copy.start()
    wide_ref[...] = jnp.zeros_like(wide_ref)
    conv_load.wait()
    spread_weights(conv_w, wide_ref)

    def hop(f, head, cut, to_s, way=0):
        rows = p.slots * p.cells // p.cuts
        piece = att.at[f, head, pl.ds(cut * rows, rows)]
        return pltpu.make_async_remote_copy(
            src_ref=piece,
            dst_ref=piece,
            send_sem=s3.at[way, f, head, cut],
            recv_sem=r3.at[f, head, cut],
            device_id={"seq": to_s},
            device_id_type=MESH,
        )

    def attend(f, j):
        lanes = slice(j * HEAD_DIM, (j + 1) * HEAD_DIM)
        q = got[0, f, :, :, lanes].reshape(-1, HEAD_DIM)
        k = got[1, :, :, :, lanes].reshape(-1, HEAD_DIM)
        v = got[2, :, :, :, lanes].reshape(-1, HEAD_DIM)
        scores = lax.dot_general(
            q, k, (((1,), (1,)), ((), ())), preferred_element_type=jnp.float32
        )
        scale = HEAD_DIM ** (-0.5) * math.log2(math.e)
        weights = jnp.exp2((scores - jnp.max(scores, -1, keepdims=True)) * scale)
        denominator = jnp.sum(weights, -1, keepdims=True)
        product = jnp.dot(weights.astype(jnp.bfloat16), v, preferred_element_type=jnp.float32)
        att[f, p.few * (s + jnp.minimum(s, 1)) + j] = (product / denominator).astype(jnp.bfloat16)

    def targets(head, row):
        o = p.owner[head]
        rows = [r for r in range(p.ns) if r != o and source_row(o, head - p.owner.index(o), r) == row]
        return sorted(rows, key=lambda r: -abs(r - row))

    def hand_on(f, head, row, way):
        rows = targets(head, row)
        if way < len(rows):
            for cut in range(p.cuts):
                hop(f, head, cut, rows[way], way).start()

    def send_own(f, j, way):
        for row in range(p.ns):
            if j < p.counts[row]:

                @pl.when(s == row)
                def _():
                    hand_on(f, p.owner.index(row) + j, row, way)

    @functools.partial(by_class, at_end)
    def _(heads):
        for copy in own_copies(heads):
            copy.wait()

    arrivals(0, p.few)
    arrivals(0, 2 * p.few)
    for f in range(p.frames):
        arrivals(1 + f, 2 * p.few)
        for j in range(p.few):
            attend(f, j)
            send_own(f, j, 0)
        for j in range(p.few, 2 * p.few):
            @pl.when(at_end)
            def _():
                attend(f, j)

            send_own(f, j, 0)
        for j in range(p.few):
            pl.when(jnp.logical_not(at_end))(functools.partial(send_own, f, j, 1))
    for f in range(p.frames):
        for j in range(2 * p.few):
            pl.when(at_end)(functools.partial(send_own, f, j, 1))

    def order(row):
        def when(item):
            f, head = item
            o = p.owner[head]
            return (due(o, head - p.owner.index(o), f, row), f, head)

        every = [(f, head) for f in range(p.frames) for head in range(p.group)]
        return sorted((item for item in every if p.owner[item[1]] != row), key=when)

    def first_part(row):
        items = order(row)
        last = max(i for i, (f, _) in enumerate(items) if f == 0)
        return items[: last + 1]

    def second_part(row):
        return order(row)[len(first_part(row)) :]

    def gather(todo):
        for row in range(p.ns):
            @pl.when(s == row)
            def _():
                for f, head in todo(row):
                    for cut in range(p.cuts):
                        hop(f, head, cut, row).wait_recv()
                        for way, to_s in enumerate(targets(head, row)):
                            hop(f, head, cut, to_s, way).start()

    def halving(f, c, b):
        bit = core if b == 0 else across
        source = term.at[f, c, 1 - bit] if b == 0 else landed0.at[f, c, 1 - bit]
        target = landed0.at[f, c] if b == 0 else landed1.at[f, c]
        return pltpu.make_async_remote_copy(
            src_ref=source,
            dst_ref=target,
            send_sem=s5.at[b, f, c],
            recv_sem=r5.at[b, f, c],
            device_id={"head": h + (1 - 2 * bit) * (1 << b)},
            device_id_type=MESH,
        )

    groups = [range(2), range(2, p.chunks)] if p.chunks > 3 else [range(p.chunks)]

    def project(f):
        rows = jnp.concatenate([att[f, head] for head in range(p.group)], axis=1)
        for group in groups:
            for c in group:
                cols = pl.ds(c * p.chunk, p.chunk)
                product = jnp.dot(rows, weight[:, cols], preferred_element_type=jnp.float32)
                term[f, c] = product.astype(jnp.bfloat16).reshape(term.shape[2:])
            for c in group:
                halving(f, c, 0).start()

    def pair_sum(f, c):
        halving(f, c, 0).wait_recv()
        total = term[f, c, core].astype(jnp.float32) + landed0[f, c].astype(jnp.float32)
        landed0[f, c] = total.astype(jnp.bfloat16)
        halving(f, c, 1).start()

    def to_owner(f, c, ds, row):
        to_s = lax.rem(s + ds, p.ns)
        return pltpu.make_async_remote_copy(
            src_ref=landed1.at[f, c, to_s],
            dst_ref=final.at[f, c, row],
            send_sem=s6.at[ds - 1, f, c],
            recv_sem=r6.at[ds - 1, f, c],
            device_id={"seq": to_s},
            device_id_type=MESH,
        )

    def full_sum(f, c):
        halving(f, c, 1).wait_recv()
        total = landed0[f, c, across].astype(jnp.float32) + landed1[f, c].astype(jnp.float32)
        landed1[f, c] = total.astype(jnp.bfloat16)
        for ds in (2, 1, 3):
            to_owner(f, c, ds, s).start()
        final[f, c, s] = landed1[f, c, s]

    gather(first_part)
    late[0].wait()
    project(0)
    def pair_sums():
        for c in range(p.chunks):
            pair_sum(0, c)

    pl.when(at_end)(pair_sums)
    gather(second_part)
    pl.when(jnp.logical_not(at_end))(pair_sums)
    project(1)
    for c in range(p.chunks):
        pair_sum(1, c)
        full_sum(0, c)
    for copy in late[1:]:
        copy.wait()
    for i, row in enumerate(row_pair):
        rows_ref[i] = row[...]

    def finish(f, c, sums):
        for ds in range(1, p.ns):
            to_owner(f, c, ds, lax.rem(s - ds + p.ns, p.ns)).wait_recv()
        rows = slice(f * p.cells, (f + 1) * p.cells)
        for j in range(p.ns):
            cols = slice(j * p.columns + c * p.chunk, j * p.columns + (c + 1) * p.chunk)
            added = gate_ref[:, cols] * final[f, c, j].astype(jnp.float32)
            value = (res[rows, cols].astype(jnp.float32) + added).astype(jnp.bfloat16)
            hidden_ref[rows, cols] = value
            sums = sums + jnp.sum(value.astype(jnp.float32), -1, keepdims=True)
        return sums

    sums = [jnp.zeros((p.cells, 1), jnp.float32) for _ in range(p.frames)]
    for c in range(p.chunks):
        full_sum(1, c)
        sums[0] = finish(0, c, sums[0])
    for c in range(p.chunks):
        sums[1] = finish(1, c, sums[1])
    mean = jnp.concatenate(sums, axis=0) / p.width
    center = hidden_ref[...].astype(jnp.float32) - mean
    spread = jnp.mean(center * center, -1, keepdims=True)
    normed = center * lax.rsqrt(spread + 1e-06) * (1.0 + scale_ref[...]) + shift_ref[...]
    values = lax.dot_general(
        normed.astype(jnp.bfloat16),
        head_w[...],
        (((1,), (1,)), ((), ())),
        preferred_element_type=jnp.float32,
    )
    values = (values + bias_ref[...]).astype(jnp.bfloat16)
    features = values.shape[-1]
    patch[...] = jnp.zeros_like(patch)
    patch[:, :features] = values
    blank = jnp.zeros(patch.shape, patch.dtype)

    moves = [(0, 1), (0, -1), (1, 0), (1, 1), (1, -1)]

    def edge(index, sign):
        dh, ds = moves[index]
        return (
            (h + sign * dh >= 0) & (h + sign * dh < p.nh)
            & (s + sign * ds >= 0) & (s + sign * ds < p.ns)
        )

    def reach(index):
        dh, ds = moves[index]
        return pltpu.make_async_remote_copy(
            src_ref=patch,
            dst_ref=halo.at[index],
            send_sem=s7.at[index],
            recv_sem=r7.at[index],
            device_id={"seq": lax.rem(s + ds + p.ns, p.ns), "head": lax.rem(h + dh, p.nh)},
            device_id_type=MESH,
        )

    for index in range(len(moves)):

        @pl.when(edge(index, 1))
        def _():
            reach(index).start()

    near_ref[1, 1] = patch[...]
    for index, (dh, ds) in enumerate(moves):

        @pl.when(edge(index, -1))
        def _():
            reach(index).wait_recv()
            near_ref[1 - dh, 1 - ds] = halo[index]

        @pl.when(jnp.logical_not(edge(index, -1)))
        def _():
            near_ref[1 - dh, 1 - ds] = blank

    for index in range(len(moves)):

        @pl.when(edge(index, 1))
        def _():
            reach(index).wait_send()

    for phase, heads in stages:
        for_sends(phase, heads, lambda copy: copy.wait_send())

    for row in range(p.ns):
        @pl.when(s == row)
        def _():
            for f in range(p.frames):
                for head in range(p.group):
                    for way, to_s in enumerate(targets(head, row)):
                        for cut in range(p.cuts):
                            hop(f, head, cut, to_s, way).wait_send()

    for f in range(p.frames):
        for c in range(p.chunks):
            for b in range(2):
                halving(f, c, b).wait_send()
            for ds in range(1, p.ns):
                to_owner(f, c, ds, s).wait_send()


def spread_weights(conv_w, wide_ref):
    taps, depth, channels = conv_w.shape
    part = depth // 3
    for a in range(2):
        for dt in range(3):
            for dy in range(3):
                base = (1 - a + dy) * 4 * part
                tap = conv_w[dt * 3 + dy]
                wide_ref[a, dt, base : base + depth, :channels] = tap
                wide_ref[a, dt, base + part : base + part + depth, channels:] = tap


def conv_kernel(
    cells, hidden_ref, near_ref, wide_ref, rows_ref, hidden_out, features_out, mixed, features, sems
):
    tokens = near_ref.shape[2]
    lanes = near_ref.shape[3]
    part = lanes // 8
    channels = features.shape[-1]
    hidden_copy = pltpu.make_async_copy(hidden_ref, hidden_out, sems.at[0])
    hidden_copy.start()

    values = near_ref[...].reshape(-1, lanes).astype(jnp.float32)
    total = values.shape[0]
    column = lax.broadcasted_iota(jnp.int32, values.shape, 0) % cells
    left = jnp.where(column == 0, 0.0, pltpu.roll(values, 1, 0))
    right = jnp.where(column == cells - 1, 0.0, pltpu.roll(values, total - 1, 0))

    source = lax.broadcasted_iota(jnp.int32, (lanes, lanes), 0)
    target = lax.broadcasted_iota(jnp.int32, (lanes, lanes), 1)
    upper, place = target // (4 * part), target % (4 * part)
    start = upper * 2 * part

    def moved(x, low, high, first):
        pick = (place >= low * part) & (place < high * part)
        pick = pick & (source == start + place + (first - low) * part)
        matrix = jnp.where(pick, 1.0, 0.0).astype(jnp.bfloat16)
        return jnp.dot(x.astype(jnp.bfloat16), matrix, preferred_element_type=jnp.float32)

    strip = moved(left, 0, 1, 1) + moved(values, 1, 3, 0) + moved(right, 3, 4, 0)
    strip = strip.reshape(2, 3, tokens, lanes).astype(jnp.bfloat16)

    def at_time(dt, row):
        if dt == 1:
            return jnp.concatenate([strip[0, row, cells:], strip[1, row, :cells]], axis=0)
        return strip[dt // 2, row]

    for a in range(2):
        taken = [at_time(dt, row) for dt in range(3) for row in (a, a + 1)]
        linear = jnp.dot(
            jnp.concatenate(taken, axis=1),
            wide_ref[a].reshape(-1, 2 * channels),
            preferred_element_type=jnp.float32,
        )
        for b in range(2):
            value = linear[:, b * channels : (b + 1) * channels] + rows_ref[0:1]
            square = jnp.mean(value * value, -1, keepdims=True)
            value = value * lax.rsqrt(square + 1e-06) * rows_ref[1:2]
            value = value / (1.0 + jnp.exp(-value))
            for k in range(channels // 128):
                for f in range(2):
                    piece = value[f * cells : (f + 1) * cells, k * 128 : (k + 1) * 128]
                    mixed[k, f, a, pl.ds(b, cells, 2)] = piece
    for k in range(channels // 128):
        features[:, :, :, k * 128 : (k + 1) * 128] = mixed[k].astype(jnp.bfloat16)
    features_copy = pltpu.make_async_copy(features, features_out, sems.at[1])
    features_copy.start()
    hidden_copy.wait()
    features_copy.wait()


def on_device(
    queries,
    attn_keys,
    attn_values,
    residual,
    out_weight,
    out_gate,
    head_shift,
    head_scale,
    head_weight,
    head_bias,
    conv_weight,
    conv_bias,
    norm_gain,
):
    ns, nh = lax.axis_size("seq"), lax.axis_size("head")
    p = Plan(ns, nh, queries, residual, out_weight)
    if not p.fits(queries, head_weight, conv_weight):
        return on_device_gathered(
            queries, attn_keys, attn_values, residual, out_weight, out_gate, head_shift,
            head_scale, head_weight, head_bias, conv_weight, conv_bias, norm_gain,
        )
    frames, height, breadth, inner = queries.shape
    t, cells, width, patch_size = p.tokens, p.cells, p.width, head_weight.shape[1]
    dma, bf16 = pltpu.SemaphoreType.DMA, jnp.bfloat16
    lanes = -(-patch_size // 128) * 128
    most = 2 * p.few * HEAD_DIM
    channels = conv_weight.shape[-1]
    hbm = pl.BlockSpec(memory_space=pltpu.HBM)
    vmem = pl.BlockSpec(memory_space=pltpu.VMEM)
    hidden, near, wide, conv_rows = pl.pallas_call(
        functools.partial(block_kernel, p),
        out_shape=(
            jax.ShapeDtypeStruct((t, width), bf16),
            jax.ShapeDtypeStruct((2, 3, t, lanes), bf16),
            jax.ShapeDtypeStruct((2, 3, 2 * lanes, 2 * channels), bf16),
            jax.ShapeDtypeStruct((2, channels), jnp.float32),
        ),
        in_specs=[hbm] * 13,
        out_specs=(vmem,) * 4,
        scratch_shapes=[
            pltpu.VMEM((3, frames, cells, inner), bf16),
            pltpu.VMEM((3, frames, p.slots, cells, most), bf16),
            pltpu.VMEM((frames, p.group, p.slots * cells, HEAD_DIM), bf16),
            pltpu.VMEM(out_weight.shape, bf16),
            pltpu.VMEM((t, width), bf16),
            pltpu.VMEM(head_weight.shape[::-1], bf16),
            pltpu.VMEM((1, width), jnp.float32),
            pltpu.VMEM((1, width), jnp.float32),
            pltpu.VMEM((1, width), jnp.float32),
            pltpu.VMEM((1, patch_size), jnp.float32),
            pltpu.VMEM((9, 3 * conv_weight.shape[3], channels), bf16),
            pltpu.VMEM((channels,), jnp.float32),
            pltpu.VMEM((channels,), jnp.float32),
            pltpu.VMEM((frames, p.chunks, 2, 2, ns, cells, p.chunk), bf16),
            pltpu.VMEM((frames, p.chunks, 2, ns, cells, p.chunk), bf16),
            pltpu.VMEM((frames, p.chunks, ns, cells, p.chunk), bf16),
            pltpu.VMEM((frames, p.chunks, ns, cells, p.chunk), bf16),
            pltpu.VMEM((t, lanes), bf16),
            pltpu.VMEM((5, t, lanes), bf16),
            dma((16,)),
            dma((3, p.slots - 1)),
            dma((3, p.slots - 1)),
            dma((2, frames, p.group, p.cuts)),
            dma((frames, p.group, p.cuts)),
            dma((2, frames, p.chunks)),
            dma((2, frames, p.chunks)),
            dma((ns - 1, frames, p.chunks)),
            dma((ns - 1, frames, p.chunks)),
            dma((5,)),
            dma((5,)),
        ],
        compiler_params=pltpu.CompilerParams(
            collective_id=0, has_side_effects=True, vmem_limit_bytes=16 * 1024 * 1024
        ),
    )(*(pltpu.with_memory_space_constraint(x, pltpu.HBM) for x in (
        queries.reshape(frames, cells, inner),
        attn_keys.reshape(frames, cells, inner),
        attn_values.reshape(frames, cells, inner),
        residual.reshape(t, width),
        out_weight,
        head_weight.T,
        out_gate.reshape(1, -1),
        head_shift.reshape(1, -1),
        head_scale.reshape(1, -1),
        head_bias.reshape(1, -1),
        conv_weight.reshape(9, -1, channels),
        conv_bias,
        norm_gain,
    )))
    hidden, features = pl.pallas_call(
        functools.partial(conv_kernel, cells),
        out_shape=(
            jax.ShapeDtypeStruct((t, width), bf16),
            jax.ShapeDtypeStruct((frames, 2, 2 * cells, channels), bf16),
        ),
        in_specs=[vmem] * 4,
        out_specs=(hbm, hbm),
        scratch_shapes=[
            pltpu.VMEM((channels // 128, frames, 2, 2 * cells, 128), jnp.float32),
            pltpu.VMEM((frames, 2, 2 * cells, channels), bf16),
            dma((2,)),
        ],
        compiler_params=pltpu.CompilerParams(vmem_limit_bytes=8 * 1024 * 1024),
    )(hidden, near, wide, conv_rows)
    return (hidden.reshape(residual.shape), features)


def solution(mesh):
    return jax.shard_map(
        on_device,
        mesh=mesh,
        in_specs=(
            P(("clip", "head"), "seq", None, None),
            P(("clip", "head"), "seq", None, None),
            P(("clip", "head"), "seq", None, None),
            P(("clip", "head"), "seq", None, None),
            P("head", "seq"),
            P(),
            P(),
            P(),
            P(),
            P(),
            P(),
            P(),
            P(),
        ),
        out_specs=(P(("clip", "head"), "seq", None, None), P(("clip", "head"), "seq", None, None)),
        check_vma=False,
    )
```

```python
import functools
import math

import jax
import jax.numpy as jnp
from jax import lax
from jax.experimental import pallas as pl
from jax.experimental.pallas import tpu as pltpu
from jax.sharding import PartitionSpec as P

HEAD_DIM = 128


def from_behind(value, axis, steps):
    count = lax.axis_size(axis)
    first, last = (max(0, -steps), min(count, count - steps))
    return lax.ppermute(value, axis, [(source, source + steps) for source in range(first, last)])


def padded_2(x, sides, width):
    for axis, dim in sides:
        peers, length = (lax.axis_size(axis), x.shape[dim])
        up = [(i, (i + 1) % peers) for i in range(peers - 1)]
        down = [(j, i) for i, j in up]
        last = lax.slice_in_dim(x, length - width, length, axis=dim)
        first = lax.slice_in_dim(x, 0, width, axis=dim)
        before = lax.ppermute(last, axis, up)
        after = lax.ppermute(first, axis, down)
        x = jnp.concatenate([before, x, after], axis=dim)
    return x


def head_latent(hidden, head_shift, head_scale, head_weight, head_bias):
    values = hidden.astype(jnp.float32)
    center = values - jnp.mean(values, -1, keepdims=True)
    spread = jnp.mean(center * center, -1, keepdims=True)
    normed = (center * lax.rsqrt(spread + 1e-06) * (1.0 + head_scale) + head_shift).astype(
        jnp.bfloat16
    )
    flat = normed.reshape(-1, normed.shape[-1])
    latent = (jnp.dot(flat, head_weight, preferred_element_type=jnp.float32) + head_bias).astype(
        jnp.bfloat16
    )
    frames, height, breadth = (hidden.shape[0], hidden.shape[1], hidden.shape[2])
    channels = head_weight.shape[1] // 4
    patches = latent.reshape(frames, height, breadth, 2, 2, channels).transpose(0, 1, 3, 2, 4, 5)
    return patches.reshape(frames, height * 2, breadth * 2, channels)


def convolve(padded, frames, conv_weight, conv_bias, norm_gain):
    height = padded.shape[1] - 2
    breadth = padded.shape[2] - 2
    stacked = jnp.concatenate(
        [
            padded[
                time_off : time_off + frames,
                row_off : row_off + height,
                col_off : col_off + breadth,
            ]
            for time_off in range(3)
            for row_off in range(3)
            for col_off in range(3)
        ],
        -1,
    )
    kernel = conv_weight.reshape(-1, conv_weight.shape[-1])
    linear = (
        jnp.dot(stacked.reshape(-1, stacked.shape[-1]), kernel, preferred_element_type=jnp.float32)
        + conv_bias
    )
    normed = linear * lax.rsqrt(jnp.mean(linear * linear, -1, keepdims=True) + 1e-06) * norm_gain
    return jax.nn.silu(normed).astype(jnp.bfloat16).reshape(frames, height, breadth, -1)


def attend_block(carried, block_keys, block_values, query_heads):
    running, denominator, weighted = carried
    scores = jnp.einsum("hqd,khd->hqk", query_heads, block_keys, preferred_element_type=jnp.float32)
    scores = scores * query_heads.shape[-1] ** (-0.5)
    newmax = jnp.maximum(running, jnp.max(scores, -1))
    factor = jnp.exp(running - newmax)
    weights = jnp.exp(scores - newmax[..., None])
    denominator = denominator * factor + jnp.sum(weights, -1)
    product = jnp.einsum(
        "hqk,khd->hqd",
        weights.astype(jnp.bfloat16),
        block_values,
        preferred_element_type=jnp.float32,
    )
    weighted = weighted * factor[..., None] + product
    return (newmax, denominator, weighted)


def fold_pieces(query_heads, carried, pieces):
    key_piece, value_piece = pieces
    frames, height, breadth = (key_piece.shape[0], key_piece.shape[1], key_piece.shape[2])
    heads_here, head_width = (query_heads.shape[0], query_heads.shape[2])
    group_rows = 4

    def regroup(one_piece):
        shaped = one_piece.reshape(
            frames, height // group_rows, group_rows, breadth, heads_here, head_width
        )
        shaped = shaped.transpose(1, 0, 2, 3, 4, 5)
        return shaped.reshape(
            height // group_rows, frames * group_rows * breadth, heads_here, head_width
        )

    def advance(inner, blocks):
        return (attend_block(inner, blocks[0], blocks[1], query_heads), None)

    carried, _ = lax.scan(advance, carried, (regroup(key_piece), regroup(value_piece)))
    return carried


def on_device_gathered(
    queries,
    attn_keys,
    attn_values,
    residual,
    out_weight,
    out_gate,
    head_shift,
    head_scale,
    head_weight,
    head_bias,
    conv_weight,
    conv_bias,
    norm_gain,
):
    head_count = lax.axis_size("head")
    frames_dev = queries.shape[0]
    group_width = queries.shape[3] // head_count
    head_width = HEAD_DIM
    heads_here = group_width // head_width
    local_queries, local_keys, local_values = (
        lax.all_to_all(queries, "head", split_axis=3, concat_axis=0, tiled=True),
        lax.all_to_all(attn_keys, "head", split_axis=3, concat_axis=0, tiled=True),
        lax.all_to_all(attn_values, "head", split_axis=3, concat_axis=0, tiled=True),
    )
    frames_all, height, breadth = (
        local_queries.shape[0],
        local_queries.shape[1],
        local_queries.shape[2],
    )
    count = frames_all * height * breadth
    query_heads = local_queries.reshape(count, heads_here, head_width).transpose(1, 0, 2)
    initial = (
        jnp.full((heads_here, count), -1e30, jnp.float32),
        jnp.zeros((heads_here, count), jnp.float32),
        jnp.zeros((heads_here, count, head_width), jnp.float32),
    )
    carried = fold_pieces(
        query_heads,
        initial,
        (
            lax.all_gather(local_keys, "seq", axis=1, tiled=True),
            lax.all_gather(local_values, "seq", axis=1, tiled=True),
        ),
    )
    running, denominator, weighted = carried
    attended = (weighted / denominator[..., None]).astype(jnp.bfloat16)
    attended = attended.transpose(1, 0, 2).reshape(count, group_width)
    partial_value = jnp.dot(
        attended,
        lax.all_gather(out_weight, "seq", axis=1, tiled=True),
        preferred_element_type=jnp.float32,
    )
    partial_value = partial_value.reshape(frames_all, height, breadth, partial_value.shape[-1])
    owned = lax.psum_scatter(
        partial_value.astype(jnp.bfloat16), "head", scatter_dimension=0, tiled=True
    ).astype(jnp.float32)
    hidden = (residual.astype(jnp.float32) + out_gate * owned).astype(jnp.bfloat16)
    own_video = head_latent(hidden, head_shift, head_scale, head_weight, head_bias)
    earlier = from_behind(own_video, "head", 1)
    video = jnp.concatenate([earlier, own_video], 0)
    extended = padded_2(video, (("seq", 1),), 1)
    padded = jnp.pad(extended, ((0, 0), (0, 0), (1, 1), (0, 0)))
    features = convolve(padded, frames_dev, conv_weight, conv_bias, norm_gain)
    return (hidden, features)


MESH = pl.DeviceIdType.MESH


class Plan:
    def __init__(self, ns, nh, queries, residual, out_weight):
        self.ns, self.nh = ns, nh
        self.frames = queries.shape[0]
        self.cells = queries.shape[1] * queries.shape[2]
        self.inner = queries.shape[3]
        self.tokens = self.frames * self.cells
        self.group = self.inner // nh // HEAD_DIM
        self.few = max(1, self.group // 6)
        self.width = residual.shape[3]
        self.columns = out_weight.shape[1]
        self.slots = ns * nh
        self.chunk = 256 if self.columns % 256 == 0 else 128
        self.chunks = self.columns // self.chunk
        self.cuts = 2
        self.counts = (self.few, 2 * self.few, 2 * self.few, self.few)
        self.owner = [o for o, count in enumerate(self.counts) for _ in range(count)]

    def fits(self, queries, head_weight, conv_weight):
        return (
            self.nh == 4
            and self.ns == 4
            and self.group == 6 * self.few
            and self.inner == self.nh * self.group * HEAD_DIM
            and self.frames == 2
            and self.cells % 16 == 0
            and self.columns % 128 == 0
            and queries.shape[1] == 1
            and head_weight.shape[1] == 64
            and conv_weight.shape[3] == 16
            and conv_weight.shape[4] % 128 == 0
            and self.slots * self.tokens <= 1024
        )


def source_row(o, row):
    step = 1 if row > o else -1
    return o if o in (0, 3) and abs(row - o) < 3 else row - step


def due(o, unit, f, row):
    away = abs(row - o)
    if o in (0, 3):
        return (0, 15.0, 15.5, 18.5)[away] + 1.5 * f
    if row == 3 * (o // 2):
        return (10.0, 18.0)[unit] + 1.4 * f
    return (15.7, 19.4)[unit] + 3.0 * (away - 1) + 1.4 * f


def block_kernel(
    plan,
    q_hbm, k_hbm, v_hbm, res_hbm, w_hbm, hw_hbm,
    gate_hbm, shift_hbm, scale_hbm, bias_hbm, cw_hbm, cb_hbm, gain_hbm,
    hidden_ref, near_ref, wide_ref, rows_ref,
    qkv, got, att, weight, res, head_w, gate_ref, shift_ref, scale_ref, bias_ref, conv_w, bias_row, gain_row, term, landed0, landed1, final, patch, halo,
    load_sem, local_sem, own_sem, s1, r1, s3, r3, s4, r4, s5, r5, s6, r6, s7, r7,
):
    p = plan
    s = lax.axis_index("seq")
    h = lax.axis_index("head")
    core, across = h & 1, h >> 1
    row_pair = (bias_row, gain_row)

    def slot(seq_index, head_index):
        return ((head_index & 1) * 2 + (head_index >> 1)) * p.ns + seq_index

    here = slot(s, h)
    at_end = (s == 0) | (s == p.ns - 1)
    offsets = [(ds, dh) for ds in range(p.ns) for dh in range(p.nh) if ds or dh]
    wide = p.few * HEAD_DIM

    def columns_of(seq_index, head_index, unit):
        before = p.few * (jnp.maximum(2 * seq_index - 1, 0) + unit)
        return pl.ds(pl.multiple_of((head_index * p.group + before) * HEAD_DIM, HEAD_DIM), wide)

    sources = (q_hbm, k_hbm, v_hbm)
    loads = [pltpu.make_async_copy(ref, qkv.at[i], load_sem) for i, ref in enumerate(sources)]
    loaded = pltpu.make_async_copy(qkv, qkv, load_sem)
    late = [
        pltpu.make_async_copy(w_hbm, weight, local_sem.at[0]),
        pltpu.make_async_copy(res_hbm, res, local_sem.at[1]),
        pltpu.make_async_copy(hw_hbm, head_w, local_sem.at[2]),
        pltpu.make_async_copy(gate_hbm, gate_ref, local_sem.at[3]),
        pltpu.make_async_copy(shift_hbm, shift_ref, local_sem.at[4]),
        pltpu.make_async_copy(scale_hbm, scale_ref, local_sem.at[5]),
        pltpu.make_async_copy(bias_hbm, bias_ref, local_sem.at[6]),
        pltpu.make_async_copy(cb_hbm, row_pair[0], local_sem.at[7]),
        pltpu.make_async_copy(gain_hbm, row_pair[1], local_sem.at[8]),
    ]
    conv_load = pltpu.make_async_copy(cw_hbm, conv_w, local_sem.at[9])

    def own_copies(unit):
        cols = columns_of(s, h, unit)
        return [
            pltpu.make_async_copy(ref.at[:, :, cols], got.at[unit, i, :, here], own_sem.at[unit])
            for i, ref in enumerate(sources)
        ]

    def own_copied(unit):
        part = got.at[unit, :, :, here]
        return pltpu.make_async_copy(part, part, own_sem.at[unit])

    for copy in loads:
        copy.start()

    barrier = pltpu.get_barrier_semaphore()
    for ds, dh in offsets:
        pl.semaphore_signal(
            barrier,
            inc=1,
            device_id={"seq": lax.rem(s + ds, p.ns), "head": lax.rem(h + dh, p.nh)},
            device_id_type=MESH,
        )
    for copy in own_copies(0):
        copy.start()

    @pl.when(jnp.logical_not(at_end))
    def _():
        for copy in own_copies(1):
            copy.start()

    loaded.wait()
    pl.semaphore_wait(barrier, len(offsets))

    def exchange(stage, to_s, to_h):
        unit = stage // 2
        return pltpu.make_async_remote_copy(
            src_ref=qkv.at[:, :, :, columns_of(to_s, to_h, unit)],
            dst_ref=got.at[unit, :, :, here],
            send_sem=s1,
            recv_sem=r1.at[stage],
            device_id={"seq": to_s, "head": to_h},
            device_id_type=MESH,
        )

    for stage in (1, 0, 2):
        for ds in range(p.ns):
            to_s = lax.rem(s + ds, p.ns)

            @pl.when(((to_s == 0) | (to_s == p.ns - 1)) == (stage == 0))
            def _():
                for ds2, dh in offsets:
                    if ds2 == ds:
                        exchange(stage, to_s, lax.rem(h + dh, p.nh)).start()

    def arrived(stage):
        parts = got.at[stage // 2, :, :, pl.ds(0, p.slots - 1)]
        pltpu.make_async_copy(parts, parts, r1.at[stage]).wait()

    conv_load.start()
    for copy in late:
        copy.start()
    wide_ref[...] = jnp.zeros_like(wide_ref)
    conv_load.wait()
    spread_weights(conv_w, wide_ref)

    def hop(f, head, cut, to_s, relayed):
        rows = p.slots * p.cells // p.cuts
        piece = att.at[f, head, pl.ds(cut * rows, rows)]
        return pltpu.make_async_remote_copy(
            src_ref=piece,
            dst_ref=piece,
            send_sem=s3.at[relayed],
            recv_sem=r3.at[f, head, cut],
            device_id={"seq": to_s},
            device_id_type=MESH,
        )

    def attend(f, j):
        unit, lanes = j // p.few, pl.ds(j % p.few * HEAD_DIM, HEAD_DIM)
        q = got[unit, 0, f, :, :, lanes].reshape(-1, HEAD_DIM)
        k = got[unit, 1, :, :, :, lanes].reshape(-1, HEAD_DIM)
        v = got[unit, 2, :, :, :, lanes].reshape(-1, HEAD_DIM)
        scores = lax.dot_general(
            q, k, (((1,), (1,)), ((), ())), preferred_element_type=jnp.float32
        )
        scale = HEAD_DIM ** (-0.5) * math.log2(math.e)
        weights = jnp.exp2((scores - jnp.max(scores, -1, keepdims=True)) * scale)
        denominator = jnp.sum(weights, -1, keepdims=True)
        product = jnp.dot(weights.astype(jnp.bfloat16), v, preferred_element_type=jnp.float32)
        att[f, p.few * jnp.maximum(2 * s - 1, 0) + j] = (product / denominator).astype(jnp.bfloat16)

    def targets(head, row):
        o = p.owner[head]
        rows = [r for r in range(p.ns) if r != o and source_row(o, r) == row]
        return sorted(rows, key=lambda r: -abs(r - row))

    def send_own(f, j):
        for row in range(p.ns):
            if j < p.counts[row]:
                head = p.owner.index(row) + j

                @pl.when(s == row)
                def _():
                    for to_s in targets(head, row):
                        for cut in range(p.cuts):
                            hop(f, head, cut, to_s, 0).start()

    def order(row):
        def when(item):
            f, head = item
            o = p.owner[head]
            return (f, due(o, (head - p.owner.index(o)) // p.few, f, row), head)

        every = [(f, head) for f in range(p.frames) for head in range(p.group)]
        return sorted((item for item in every if p.owner[item[1]] != row), key=when)

    def take(f, head, row):
        for cut in range(p.cuts):
            hop(f, head, cut, row, 1).wait_recv()
            for to_s in targets(head, row):
                hop(f, head, cut, to_s, 1).start()

    def gather(todo):
        for row in range(p.ns):
            @pl.when(s == row)
            def _():
                for f, head in todo(row):
                    take(f, head, row)

    def early_part(row):
        def early(f, head):
            unit = (head - p.owner.index(p.owner[head])) // p.few
            return f == 0 and unit == 0 and row in (1, 2) and targets(head, row)

        return [item for item in order(row) if early(*item)]

    def part(f, row):
        return [item for item in order(row) if item[0] == f and item not in early_part(row)]

    own_copied(0).wait()
    pl.when(at_end)(functools.partial(arrived, 0))
    pl.when(jnp.logical_not(at_end))(functools.partial(arrived, 1))
    for f in range(p.frames):
        for j in range(p.few):
            attend(f, j)
            send_own(f, j)

    @pl.when(jnp.logical_not(at_end))
    def _():
        own_copied(1).wait()
        arrived(2)
        for f in range(p.frames):
            for j in range(p.few, 2 * p.few):
                attend(f, j)
                send_own(f, j)
            if f == 0:
                gather(early_part)

    groups = [(0, 2), (2, p.chunks - 2)] if p.chunks > 3 else [(0, p.chunks)]

    def to_partner(f, g):
        part = pl.ds(*groups[g])
        return pltpu.make_async_remote_copy(
            src_ref=term.at[f, part, 1 - core],
            dst_ref=landed0.at[f, part],
            send_sem=s4,
            recv_sem=r4.at[f, g],
            device_id={"head": h + 1 - 2 * core},
            device_id_type=MESH,
        )

    def project(f):
        rows = jnp.concatenate([att[f, head] for head in range(p.group)], axis=1)
        for g, (start, length) in enumerate(groups):
            for c in range(start, start + length):
                cols = pl.ds(c * p.chunk, p.chunk)
                product = jnp.dot(rows, weight[:, cols], preferred_element_type=jnp.float32)
                term[f, c] = product.astype(jnp.bfloat16).reshape(term.shape[2:])
            to_partner(f, g).start()

    def across_x(f, c):
        return pltpu.make_async_remote_copy(
            src_ref=landed0.at[f, c, 1 - across],
            dst_ref=landed1.at[f, c],
            send_sem=s5,
            recv_sem=r5.at[f, c],
            device_id={"head": h + 2 - 4 * across},
            device_id_type=MESH,
        )

    def pair_sum(f, c):
        for g, (start, _) in enumerate(groups):
            if c == start:
                to_partner(f, g).wait_recv()
        total = term[f, c, core].astype(jnp.float32) + landed0[f, c].astype(jnp.float32)
        landed0[f, c] = total.astype(jnp.bfloat16)
        across_x(f, c).start()

    def full_sum(f, c):
        across_x(f, c).wait_recv()
        total = landed0[f, c, across].astype(jnp.float32) + landed1[f, c].astype(jnp.float32)
        landed1[f, c] = total.astype(jnp.bfloat16)
        for ds in (2, 1, 3):
            to_s = lax.rem(s + ds, p.ns)
            pltpu.make_async_remote_copy(
                src_ref=landed1.at[f, c, to_s],
                dst_ref=final.at[f, c, ds - 1],
                send_sem=s6,
                recv_sem=r6.at[f, c],
                device_id={"seq": to_s},
                device_id_type=MESH,
            ).start()

    gather(functools.partial(part, 0))
    late[0].wait()
    project(0)
    def pair_sums():
        for c in range(p.chunks):
            pair_sum(0, c)

    pl.when(at_end)(pair_sums)
    gather(functools.partial(part, 1))
    pl.when(jnp.logical_not(at_end))(pair_sums)
    project(1)
    for c in range(p.chunks):
        pair_sum(1, c)
        full_sum(0, c)
    for copy in late[1:]:
        copy.wait()
    for i, row in enumerate(row_pair):
        rows_ref[i] = row[...]

    def finish(f, c, sums):
        pltpu.make_async_copy(final.at[f, c], final.at[f, c], r6.at[f, c]).wait()
        rows = slice(f * p.cells, (f + 1) * p.cells)
        for ds in range(p.ns):
            j = lax.rem(s - ds + p.ns, p.ns)
            cols = pl.ds(pl.multiple_of(j * p.columns + c * p.chunk, 128), p.chunk)
            part = landed1[f, c, s] if ds == 0 else final[f, c, ds - 1]
            added = gate_ref[:, cols] * part.astype(jnp.float32)
            value = (res[rows, cols].astype(jnp.float32) + added).astype(jnp.bfloat16)
            hidden_ref[rows, cols] = value
            sums = sums + jnp.sum(value.astype(jnp.float32), -1, keepdims=True)
        return sums

    patch[...] = jnp.zeros_like(patch)

    def head(f, sums):
        rows = slice(f * p.cells, (f + 1) * p.cells)
        center = hidden_ref[rows].astype(jnp.float32) - sums / p.width
        spread = jnp.mean(center * center, -1, keepdims=True)
        normed = center * lax.rsqrt(spread + 1e-06) * (1.0 + scale_ref[...]) + shift_ref[...]
        values = lax.dot_general(
            normed.astype(jnp.bfloat16),
            head_w[...],
            (((1,), (1,)), ((), ())),
            preferred_element_type=jnp.float32,
        )
        values = (values + bias_ref[...]).astype(jnp.bfloat16)
        patch[rows, : values.shape[-1]] = values

    sums = [jnp.zeros((p.cells, 1), jnp.float32) for _ in range(p.frames)]
    for c in range(p.chunks):
        full_sum(1, c)
        sums[0] = finish(0, c, sums[0])
    head(0, sums[0])
    for c in range(p.chunks):
        sums[1] = finish(1, c, sums[1])
    head(1, sums[1])
    blank = jnp.zeros(patch.shape, patch.dtype)

    moves = [(0, 1), (0, -1), (1, 0), (1, 1), (1, -1)]

    def edge(index, sign):
        dh, ds = moves[index]
        return (
            (h + sign * dh >= 0) & (h + sign * dh < p.nh)
            & (s + sign * ds >= 0) & (s + sign * ds < p.ns)
        )

    def reach(index):
        dh, ds = moves[index]
        return pltpu.make_async_remote_copy(
            src_ref=patch,
            dst_ref=halo.at[index],
            send_sem=s7.at[index],
            recv_sem=r7.at[index],
            device_id={"seq": lax.rem(s + ds + p.ns, p.ns), "head": lax.rem(h + dh, p.nh)},
            device_id_type=MESH,
        )

    for index in range(len(moves)):

        @pl.when(edge(index, 1))
        def _():
            reach(index).start()

    near_ref[1, 1] = patch[...]
    for index, (dh, ds) in enumerate(moves):

        @pl.when(edge(index, -1))
        def _():
            reach(index).wait_recv()
            near_ref[1 - dh, 1 - ds] = halo[index]

        @pl.when(jnp.logical_not(edge(index, -1)))
        def _():
            near_ref[1 - dh, 1 - ds] = blank

    for index in range(len(moves)):

        @pl.when(edge(index, 1))
        def _():
            reach(index).wait_send()

    def all_sent(part, sem):
        pltpu.make_async_copy(part, part, sem).wait()

    for row in range(p.ns):
        @pl.when(s == row)
        def _():
            foreign = (p.nh * p.group - p.counts[row]) * HEAD_DIM
            all_sent(qkv.at[:, :, :, pl.ds(0, foreign)], s1)
            for relayed in range(2):
                heads = [head for head in range(p.group) if (p.owner[head] != row) == relayed]
                sent = sum(len(targets(head, row)) for head in heads)
                if sent:
                    all_sent(att.at[:, pl.ds(0, sent)], s3.at[relayed])

    all_sent(landed0, s4)
    all_sent(landed1, s5)
    all_sent(final, s6)


def spread_weights(conv_w, wide_ref):
    taps, depth, channels = conv_w.shape
    part = depth // 3
    for a in range(2):
        for dt in range(3):
            for dy in range(3):
                base = (1 - a + dy) * 4 * part
                tap = conv_w[dt * 3 + dy]
                wide_ref[a, dt, base : base + depth, :channels] = tap
                wide_ref[a, dt, base + part : base + part + depth, channels:] = tap


def conv_kernel(
    cells, hidden_ref, near_ref, wide_ref, rows_ref, hidden_out, features_out, mixed, features, sems
):
    tokens = near_ref.shape[2]
    lanes = near_ref.shape[3]
    part = lanes // 8
    channels = features.shape[-1]
    hidden_copy = pltpu.make_async_copy(hidden_ref, hidden_out, sems.at[0])
    hidden_copy.start()

    values = near_ref[...].reshape(-1, lanes).astype(jnp.float32)
    total = values.shape[0]
    column = lax.broadcasted_iota(jnp.int32, values.shape, 0) % cells
    left = jnp.where(column == 0, 0.0, pltpu.roll(values, 1, 0))
    right = jnp.where(column == cells - 1, 0.0, pltpu.roll(values, total - 1, 0))

    source = lax.broadcasted_iota(jnp.int32, (lanes, lanes), 0)
    target = lax.broadcasted_iota(jnp.int32, (lanes, lanes), 1)
    upper, place = target // (4 * part), target % (4 * part)
    start = upper * 2 * part

    def moved(x, low, high, first):
        pick = (place >= low * part) & (place < high * part)
        pick = pick & (source == start + place + (first - low) * part)
        matrix = jnp.where(pick, 1.0, 0.0).astype(jnp.bfloat16)
        return jnp.dot(x.astype(jnp.bfloat16), matrix, preferred_element_type=jnp.float32)

    strip = moved(left, 0, 1, 1) + moved(values, 1, 3, 0) + moved(right, 3, 4, 0)
    strip = strip.reshape(2, 3, tokens, lanes).astype(jnp.bfloat16)

    def at_time(dt, row):
        if dt == 1:
            return jnp.concatenate([strip[0, row, cells:], strip[1, row, :cells]], axis=0)
        return strip[dt // 2, row]

    for a in range(2):
        taken = [at_time(dt, row) for dt in range(3) for row in (a, a + 1)]
        linear = jnp.dot(
            jnp.concatenate(taken, axis=1),
            wide_ref[a].reshape(-1, 2 * channels),
            preferred_element_type=jnp.float32,
        )
        for b in range(2):
            value = linear[:, b * channels : (b + 1) * channels] + rows_ref[0:1]
            square = jnp.mean(value * value, -1, keepdims=True)
            value = value * lax.rsqrt(square + 1e-06) * rows_ref[1:2]
            value = value / (1.0 + jnp.exp(-value))
            for k in range(channels // 128):
                for f in range(2):
                    piece = value[f * cells : (f + 1) * cells, k * 128 : (k + 1) * 128]
                    mixed[k, f, a, pl.ds(b, cells, 2)] = piece
    for k in range(channels // 128):
        features[:, :, :, k * 128 : (k + 1) * 128] = mixed[k].astype(jnp.bfloat16)
    features_copy = pltpu.make_async_copy(features, features_out, sems.at[1])
    features_copy.start()
    hidden_copy.wait()
    features_copy.wait()


def on_device(
    queries,
    attn_keys,
    attn_values,
    residual,
    out_weight,
    out_gate,
    head_shift,
    head_scale,
    head_weight,
    head_bias,
    conv_weight,
    conv_bias,
    norm_gain,
):
    ns, nh = lax.axis_size("seq"), lax.axis_size("head")
    p = Plan(ns, nh, queries, residual, out_weight)
    if not p.fits(queries, head_weight, conv_weight):
        return on_device_gathered(
            queries, attn_keys, attn_values, residual, out_weight, out_gate, head_shift,
            head_scale, head_weight, head_bias, conv_weight, conv_bias, norm_gain,
        )
    frames, height, breadth, inner = queries.shape
    t, cells, width, patch_size = p.tokens, p.cells, p.width, head_weight.shape[1]
    dma, bf16 = pltpu.SemaphoreType.DMA, jnp.bfloat16
    lanes = -(-patch_size // 128) * 128
    channels = conv_weight.shape[-1]
    hbm = pl.BlockSpec(memory_space=pltpu.HBM)
    vmem = pl.BlockSpec(memory_space=pltpu.VMEM)
    hidden, near, wide, conv_rows = pl.pallas_call(
        functools.partial(block_kernel, p),
        out_shape=(
            jax.ShapeDtypeStruct((t, width), bf16),
            jax.ShapeDtypeStruct((2, 3, t, lanes), bf16),
            jax.ShapeDtypeStruct((2, 3, 2 * lanes, 2 * channels), bf16),
            jax.ShapeDtypeStruct((2, channels), jnp.float32),
        ),
        in_specs=[hbm] * 13,
        out_specs=(vmem,) * 4,
        scratch_shapes=[
            pltpu.VMEM((3, frames, cells, inner), bf16),
            pltpu.VMEM((2, 3, frames, p.slots, cells, p.few * HEAD_DIM), bf16),
            pltpu.VMEM((frames, p.group, p.slots * cells, HEAD_DIM), bf16),
            pltpu.VMEM(out_weight.shape, bf16),
            pltpu.VMEM((t, width), bf16),
            pltpu.VMEM(head_weight.shape[::-1], bf16),
            pltpu.VMEM((1, width), jnp.float32),
            pltpu.VMEM((1, width), jnp.float32),
            pltpu.VMEM((1, width), jnp.float32),
            pltpu.VMEM((1, patch_size), jnp.float32),
            pltpu.VMEM((9, 3 * conv_weight.shape[3], channels), bf16),
            pltpu.VMEM((channels,), jnp.float32),
            pltpu.VMEM((channels,), jnp.float32),
            pltpu.VMEM((frames, p.chunks, 2, 2, ns, cells, p.chunk), bf16),
            pltpu.VMEM((frames, p.chunks, 2, ns, cells, p.chunk), bf16),
            pltpu.VMEM((frames, p.chunks, ns, cells, p.chunk), bf16),
            pltpu.VMEM((frames, p.chunks, ns - 1, cells, p.chunk), bf16),
            pltpu.VMEM((t, lanes), bf16),
            pltpu.VMEM((5, t, lanes), bf16),
            dma(()),
            dma((10,)),
            dma((2,)),
            dma(()),
            dma((3,)),
            dma((2,)),
            dma((frames, p.group, p.cuts)),
            dma(()),
            dma((frames, 2)),
            dma(()),
            dma((frames, p.chunks)),
            dma(()),
            dma((frames, p.chunks)),
            dma((5,)),
            dma((5,)),
        ],
        compiler_params=pltpu.CompilerParams(
            collective_id=0, has_side_effects=True, vmem_limit_bytes=16 * 1024 * 1024
        ),
    )(*(pltpu.with_memory_space_constraint(x, pltpu.HBM) for x in (
        queries.reshape(frames, cells, inner),
        attn_keys.reshape(frames, cells, inner),
        attn_values.reshape(frames, cells, inner),
        residual.reshape(t, width),
        out_weight,
        head_weight.T,
        out_gate.reshape(1, -1),
        head_shift.reshape(1, -1),
        head_scale.reshape(1, -1),
        head_bias.reshape(1, -1),
        conv_weight.reshape(9, -1, channels),
        conv_bias,
        norm_gain,
    )))
    hidden, features = pl.pallas_call(
        functools.partial(conv_kernel, cells),
        out_shape=(
            jax.ShapeDtypeStruct((t, width), bf16),
            jax.ShapeDtypeStruct((frames, 2, 2 * cells, channels), bf16),
        ),
        in_specs=[vmem] * 4,
        out_specs=(hbm, hbm),
        scratch_shapes=[
            pltpu.VMEM((channels // 128, frames, 2, 2 * cells, 128), jnp.float32),
            pltpu.VMEM((frames, 2, 2 * cells, channels), bf16),
            dma((2,)),
        ],
        compiler_params=pltpu.CompilerParams(vmem_limit_bytes=8 * 1024 * 1024),
    )(hidden, near, wide, conv_rows)
    return (hidden.reshape(residual.shape), features)


def solution(mesh):
    return jax.shard_map(
        on_device,
        mesh=mesh,
        in_specs=(
            P(("clip", "head"), "seq", None, None),
            P(("clip", "head"), "seq", None, None),
            P(("clip", "head"), "seq", None, None),
            P(("clip", "head"), "seq", None, None),
            P("head", "seq"),
            P(),
            P(),
            P(),
            P(),
            P(),
            P(),
            P(),
            P(),
        ),
        out_specs=(P(("clip", "head"), "seq", None, None), P(("clip", "head"), "seq", None, None)),
        check_vma=False,
    )
```

```python
import functools
import math

import jax
import jax.numpy as jnp
from jax import lax
from jax.experimental import pallas as pl
from jax.experimental.pallas import tpu as pltpu
from jax.sharding import PartitionSpec as P

HEAD_DIM = 128


def from_behind(value, axis, steps):
    count = lax.axis_size(axis)
    first, last = (max(0, -steps), min(count, count - steps))
    return lax.ppermute(value, axis, [(source, source + steps) for source in range(first, last)])


def padded_2(x, sides, width):
    for axis, dim in sides:
        peers, length = (lax.axis_size(axis), x.shape[dim])
        up = [(i, (i + 1) % peers) for i in range(peers - 1)]
        down = [(j, i) for i, j in up]
        last = lax.slice_in_dim(x, length - width, length, axis=dim)
        first = lax.slice_in_dim(x, 0, width, axis=dim)
        before = lax.ppermute(last, axis, up)
        after = lax.ppermute(first, axis, down)
        x = jnp.concatenate([before, x, after], axis=dim)
    return x


def head_latent(hidden, head_shift, head_scale, head_weight, head_bias):
    values = hidden.astype(jnp.float32)
    center = values - jnp.mean(values, -1, keepdims=True)
    spread = jnp.mean(center * center, -1, keepdims=True)
    normed = (center * lax.rsqrt(spread + 1e-06) * (1.0 + head_scale) + head_shift).astype(
        jnp.bfloat16
    )
    flat = normed.reshape(-1, normed.shape[-1])
    latent = (jnp.dot(flat, head_weight, preferred_element_type=jnp.float32) + head_bias).astype(
        jnp.bfloat16
    )
    frames, height, breadth = (hidden.shape[0], hidden.shape[1], hidden.shape[2])
    channels = head_weight.shape[1] // 4
    patches = latent.reshape(frames, height, breadth, 2, 2, channels).transpose(0, 1, 3, 2, 4, 5)
    return patches.reshape(frames, height * 2, breadth * 2, channels)


def convolve(padded, frames, conv_weight, conv_bias, norm_gain):
    height = padded.shape[1] - 2
    breadth = padded.shape[2] - 2
    stacked = jnp.concatenate(
        [
            padded[
                time_off : time_off + frames,
                row_off : row_off + height,
                col_off : col_off + breadth,
            ]
            for time_off in range(3)
            for row_off in range(3)
            for col_off in range(3)
        ],
        -1,
    )
    kernel = conv_weight.reshape(-1, conv_weight.shape[-1])
    linear = (
        jnp.dot(stacked.reshape(-1, stacked.shape[-1]), kernel, preferred_element_type=jnp.float32)
        + conv_bias
    )
    normed = linear * lax.rsqrt(jnp.mean(linear * linear, -1, keepdims=True) + 1e-06) * norm_gain
    return jax.nn.silu(normed).astype(jnp.bfloat16).reshape(frames, height, breadth, -1)


def attend_block(carried, block_keys, block_values, query_heads):
    running, denominator, weighted = carried
    scores = jnp.einsum("hqd,khd->hqk", query_heads, block_keys, preferred_element_type=jnp.float32)
    scores = scores * query_heads.shape[-1] ** (-0.5)
    newmax = jnp.maximum(running, jnp.max(scores, -1))
    factor = jnp.exp(running - newmax)
    weights = jnp.exp(scores - newmax[..., None])
    denominator = denominator * factor + jnp.sum(weights, -1)
    product = jnp.einsum(
        "hqk,khd->hqd",
        weights.astype(jnp.bfloat16),
        block_values,
        preferred_element_type=jnp.float32,
    )
    weighted = weighted * factor[..., None] + product
    return (newmax, denominator, weighted)


def fold_pieces(query_heads, carried, pieces):
    key_piece, value_piece = pieces
    frames, height, breadth = (key_piece.shape[0], key_piece.shape[1], key_piece.shape[2])
    heads_here, head_width = (query_heads.shape[0], query_heads.shape[2])
    group_rows = 4

    def regroup(one_piece):
        shaped = one_piece.reshape(
            frames, height // group_rows, group_rows, breadth, heads_here, head_width
        )
        shaped = shaped.transpose(1, 0, 2, 3, 4, 5)
        return shaped.reshape(
            height // group_rows, frames * group_rows * breadth, heads_here, head_width
        )

    def advance(inner, blocks):
        return (attend_block(inner, blocks[0], blocks[1], query_heads), None)

    carried, _ = lax.scan(advance, carried, (regroup(key_piece), regroup(value_piece)))
    return carried


def on_device_gathered(
    queries,
    attn_keys,
    attn_values,
    residual,
    out_weight,
    out_gate,
    head_shift,
    head_scale,
    head_weight,
    head_bias,
    conv_weight,
    conv_bias,
    norm_gain,
):
    head_count = lax.axis_size("head")
    frames_dev = queries.shape[0]
    group_width = queries.shape[3] // head_count
    head_width = HEAD_DIM
    heads_here = group_width // head_width
    local_queries, local_keys, local_values = (
        lax.all_to_all(queries, "head", split_axis=3, concat_axis=0, tiled=True),
        lax.all_to_all(attn_keys, "head", split_axis=3, concat_axis=0, tiled=True),
        lax.all_to_all(attn_values, "head", split_axis=3, concat_axis=0, tiled=True),
    )
    frames_all, height, breadth = (
        local_queries.shape[0],
        local_queries.shape[1],
        local_queries.shape[2],
    )
    count = frames_all * height * breadth
    query_heads = local_queries.reshape(count, heads_here, head_width).transpose(1, 0, 2)
    initial = (
        jnp.full((heads_here, count), -1e30, jnp.float32),
        jnp.zeros((heads_here, count), jnp.float32),
        jnp.zeros((heads_here, count, head_width), jnp.float32),
    )
    carried = fold_pieces(
        query_heads,
        initial,
        (
            lax.all_gather(local_keys, "seq", axis=1, tiled=True),
            lax.all_gather(local_values, "seq", axis=1, tiled=True),
        ),
    )
    running, denominator, weighted = carried
    attended = (weighted / denominator[..., None]).astype(jnp.bfloat16)
    attended = attended.transpose(1, 0, 2).reshape(count, group_width)
    partial_value = jnp.dot(
        attended,
        lax.all_gather(out_weight, "seq", axis=1, tiled=True),
        preferred_element_type=jnp.float32,
    )
    partial_value = partial_value.reshape(frames_all, height, breadth, partial_value.shape[-1])
    owned = lax.psum_scatter(
        partial_value.astype(jnp.bfloat16), "head", scatter_dimension=0, tiled=True
    ).astype(jnp.float32)
    hidden = (residual.astype(jnp.float32) + out_gate * owned).astype(jnp.bfloat16)
    own_video = head_latent(hidden, head_shift, head_scale, head_weight, head_bias)
    earlier = from_behind(own_video, "head", 1)
    video = jnp.concatenate([earlier, own_video], 0)
    extended = padded_2(video, (("seq", 1),), 1)
    padded = jnp.pad(extended, ((0, 0), (0, 0), (1, 1), (0, 0)))
    features = convolve(padded, frames_dev, conv_weight, conv_bias, norm_gain)
    return (hidden, features)


MESH = pl.DeviceIdType.MESH


class Plan:
    def __init__(self, ns, nh, queries, residual, out_weight):
        self.ns, self.nh = ns, nh
        self.frames = queries.shape[0]
        self.cells = queries.shape[1] * queries.shape[2]
        self.inner = queries.shape[3]
        self.tokens = self.frames * self.cells
        self.group = self.inner // nh // HEAD_DIM
        self.few = max(1, self.group // 6)
        self.width = residual.shape[3]
        self.columns = out_weight.shape[1]
        self.slots = ns * nh
        self.chunk = 256 if self.columns % 256 == 0 else 128
        self.chunks = self.columns // self.chunk
        self.cuts = 2
        self.counts = (self.few, 2 * self.few, 2 * self.few, self.few)
        self.owner = [o for o, count in enumerate(self.counts) for _ in range(count)]

    def fits(self, queries, head_weight, conv_weight):
        return (
            self.nh == 4
            and self.ns == 4
            and self.group == 6 * self.few
            and self.inner == self.nh * self.group * HEAD_DIM
            and self.frames == 2
            and self.cells % 16 == 0
            and self.columns % 128 == 0
            and queries.shape[1] == 1
            and head_weight.shape[1] == 64
            and conv_weight.shape[3] == 16
            and conv_weight.shape[4] % 128 == 0
            and self.slots * self.tokens <= 1024
        )


def source_row(o, row):
    step = 1 if row > o else -1
    return o if o in (0, 3) and abs(row - o) < 3 else row - step


def due(o, unit, f, row):
    away = abs(row - o)
    if o in (0, 3):
        return (0, 15.0, 15.5, 18.5)[away] + 6.5 * f
    if row == 3 * (o // 2):
        return (10.0, 18.0)[unit] + 1.4 * f
    return (15.7, 19.4)[unit] + 3.0 * (away - 1) + 1.4 * f


def block_kernel(
    plan,
    q_hbm, k_hbm, v_hbm, res_hbm, w_hbm, hw_hbm,
    gate_hbm, shift_hbm, scale_hbm, bias_hbm, cw_hbm, cb_hbm, gain_hbm,
    hidden_ref, near_ref, wide_ref, rows_ref,
    qkv, got, att, weight, res, head_w, gate_ref, shift_ref, scale_ref, bias_ref, conv_w, bias_row, gain_row, term, landed0, landed1, final, patch, halo,
    load_sem, local_sem, own_sem, s1, r1, s3, r3, s4, r4, s5, r5, s6, r6, s7, r7,
):
    p = plan
    s = lax.axis_index("seq")
    h = lax.axis_index("head")
    core, across = h & 1, h >> 1
    row_pair = (bias_row, gain_row)

    def pair_of(seq_index):
        return ((seq_index + 1) >> 1) & 1

    place = s >> 1
    here = ((pair_of(s) * 2 + core) * 2 + across) * 2 + place
    at_end = (s == 0) | (s == p.ns - 1)
    offsets = [(ds, dh) for ds in range(p.ns) for dh in range(p.nh) if ds or dh]
    wide = p.few * HEAD_DIM

    def columns_of(seq_index, head_index, unit):
        before = p.few * (jnp.maximum(2 * seq_index - 1, 0) + unit)
        return pl.ds(pl.multiple_of((head_index * p.group + before) * HEAD_DIM, HEAD_DIM), wide)

    sources = (q_hbm, k_hbm, v_hbm)
    loads = [pltpu.make_async_copy(ref, qkv.at[i], load_sem) for i, ref in enumerate(sources)]
    loaded = pltpu.make_async_copy(qkv, qkv, load_sem)
    late = [
        pltpu.make_async_copy(w_hbm, weight, local_sem.at[0]),
        pltpu.make_async_copy(res_hbm, res, local_sem.at[1]),
        pltpu.make_async_copy(hw_hbm, head_w, local_sem.at[2]),
        pltpu.make_async_copy(gate_hbm, gate_ref, local_sem.at[3]),
        pltpu.make_async_copy(shift_hbm, shift_ref, local_sem.at[4]),
        pltpu.make_async_copy(scale_hbm, scale_ref, local_sem.at[5]),
        pltpu.make_async_copy(bias_hbm, bias_ref, local_sem.at[6]),
        pltpu.make_async_copy(cb_hbm, row_pair[0], local_sem.at[7]),
        pltpu.make_async_copy(gain_hbm, row_pair[1], local_sem.at[8]),
    ]
    conv_load = pltpu.make_async_copy(cw_hbm, conv_w, local_sem.at[9])

    def own_copies(unit):
        cols = columns_of(s, h, unit)
        return [
            pltpu.make_async_copy(ref.at[:, :, cols], got.at[unit, i, :, here], own_sem.at[unit])
            for i, ref in enumerate(sources)
        ]

    def own_copied(unit):
        part = got.at[unit, :, :, here]
        return pltpu.make_async_copy(part, part, own_sem.at[unit])

    for copy in loads:
        copy.start()

    barrier = pltpu.get_barrier_semaphore()
    for ds, dh in offsets:
        pl.semaphore_signal(
            barrier,
            inc=1,
            device_id={"seq": lax.rem(s + ds, p.ns), "head": lax.rem(h + dh, p.nh)},
            device_id_type=MESH,
        )
    for copy in own_copies(0):
        copy.start()

    @pl.when(jnp.logical_not(at_end))
    def _():
        for copy in own_copies(1):
            copy.start()

    loaded.wait()
    pl.semaphore_wait(barrier, len(offsets))

    def exchange(stage, to_s, to_h):
        unit = stage // 2
        return pltpu.make_async_remote_copy(
            src_ref=qkv.at[:, :, :, columns_of(to_s, to_h, unit)],
            dst_ref=got.at[unit, :, :, here],
            send_sem=s1,
            recv_sem=r1.at[stage],
            device_id={"seq": to_s, "head": to_h},
            device_id_type=MESH,
        )

    for stage in (1, 0, 2):
        for ds in range(p.ns):
            to_s = lax.rem(s + ds, p.ns)

            @pl.when(((to_s == 0) | (to_s == p.ns - 1)) == (stage == 0))
            def _():
                for ds2, dh in offsets:
                    if ds2 == ds:
                        exchange(stage, to_s, lax.rem(h + dh, p.nh)).start()

    def arrived(stage):
        parts = got.at[stage // 2, :, :, pl.ds(0, p.slots - 1)]
        pltpu.make_async_copy(parts, parts, r1.at[stage]).wait()

    conv_load.start()
    for copy in late:
        copy.start()
    wide_ref[...] = jnp.zeros_like(wide_ref)
    conv_load.wait()
    spread_weights(conv_w, wide_ref)

    def hop(f, head, cut, to_s, relayed):
        rows = p.slots * p.cells // p.cuts
        piece = att.at[f, head, pl.ds(cut * rows, rows)]
        return pltpu.make_async_remote_copy(
            src_ref=piece,
            dst_ref=piece,
            send_sem=s3.at[relayed],
            recv_sem=r3.at[f, head, cut],
            device_id={"seq": to_s},
            device_id_type=MESH,
        )

    def attend(f, j):
        unit, lanes = j // p.few, pl.ds(j % p.few * HEAD_DIM, HEAD_DIM)
        q = got[unit, 0, f, :, :, lanes].reshape(-1, HEAD_DIM)
        k = got[unit, 1, :, :, :, lanes].reshape(-1, HEAD_DIM)
        v = got[unit, 2, :, :, :, lanes].reshape(-1, HEAD_DIM)
        scores = lax.dot_general(
            q, k, (((1,), (1,)), ((), ())), preferred_element_type=jnp.float32
        )
        scale = HEAD_DIM ** (-0.5) * math.log2(math.e)
        weights = jnp.exp2((scores - jnp.max(scores, -1, keepdims=True)) * scale)
        denominator = jnp.sum(weights, -1, keepdims=True)
        product = jnp.dot(weights.astype(jnp.bfloat16), v, preferred_element_type=jnp.float32)
        att[f, p.few * jnp.maximum(2 * s - 1, 0) + j] = (product / denominator).astype(jnp.bfloat16)

    parts = [(f, cut) for f in range(p.frames) for cut in range(p.cuts)]

    def targets(head, row):
        o = p.owner[head]
        rows = [r for r in range(p.ns) if r != o and source_row(o, r) == row]
        return sorted(rows, key=lambda r: -abs(r - row))

    def send_own(f, j, outward=(True, False)):
        for row in range(p.ns):
            if j < p.counts[row]:
                head = p.owner.index(row) + j

                @pl.when(s == row)
                def _():
                    rows = [r for r in targets(head, row) if (r in (0, p.ns - 1)) in outward]
                    pieces = [(cut, to_s) for cut in range(p.cuts) for to_s in rows]
                    for cut, to_s in pieces:
                        hop(f, head, cut, to_s, 0).start()

    def order(row):
        def when(item):
            f, cut, head = item
            o = p.owner[head]
            passive = not targets(head, row)
            return (f, cut, passive, due(o, (head - p.owner.index(o)) // p.few, f, row), head)

        heads = [head for head in range(p.group) if p.owner[head] != row]
        return sorted(((f, cut, head) for f, cut in parts for head in heads), key=when)

    def gather(todo):
        for row in range(p.ns):
            @pl.when(s == row)
            def _():
                for f, cut, head in todo(row):
                    hop(f, head, cut, row, 1).wait_recv()
                    for to_s in targets(head, row):
                        hop(f, head, cut, to_s, 1).start()

    def early_part(row):
        def early(f, cut, head):
            unit = (head - p.owner.index(p.owner[head])) // p.few
            return f == 0 and unit == 0 and row in (1, 2) and targets(head, row)

        return [item for item in order(row) if early(*item)]

    def first_part(row):
        if row not in (0, p.ns - 1):
            return []
        return [(0, 0, head) for head in range(p.group) if p.owner[head] == (1, 2)[row // 3]]

    def gather_part(f, cut):
        def todo(row):
            done = early_part(row) + first_part(row)
            return [item for item in order(row) if item[:2] == (f, cut) and item not in done]

        gather(todo)

    own_copied(0).wait()
    pl.when(at_end)(functools.partial(arrived, 0))
    pl.when(jnp.logical_not(at_end))(functools.partial(arrived, 1))
    def at_ends(act, *of):
        pl.when(at_end)(functools.partial(act, *of))

    def at_middle(act, *of):
        pl.when(jnp.logical_not(at_end))(functools.partial(act, *of))

    for f in range(p.frames):
        for j in range(p.few):
            attend(f, j)
            if f == 0:
                send_own(f, j)
            else:
                at_middle(send_own, f, j, (True,))

    @at_middle
    def _():
        own_copied(1).wait()
        arrived(2)
        for f in range(p.frames):
            for j in range(p.few, 2 * p.few):
                attend(f, j)
                send_own(f, j, (True, False) if f == 0 else (False,))
            if f == 0:
                for j in range(p.few):
                    send_own(1, j, (False,))
                gather(early_part)

    @at_ends
    def _():
        gather(first_part)
        for j in range(p.few):
            send_own(1, j)

    groups = [(0, 2), (2, p.chunks - 2)] if p.chunks > 3 else [(0, p.chunks)]

    def to_partner(f, cut, g):
        part = pl.ds(*groups[g])
        return pltpu.make_async_remote_copy(
            src_ref=term.at[f, cut, part, 1 - core],
            dst_ref=landed0.at[f, cut, part],
            send_sem=s4,
            recv_sem=r4.at[f, cut, g],
            device_id={"head": h + 1 - 2 * core},
            device_id_type=MESH,
        )

    def project(f, cut):
        length = p.slots * p.cells // p.cuts
        own = pl.ds(cut * length, length)
        rows = jnp.concatenate([att[f, head, own] for head in range(p.group)], axis=1)
        for g, (start, count) in enumerate(groups):
            for c in range(start, start + count):
                cols = pl.ds(c * p.chunk, p.chunk)
                product = jnp.dot(rows, weight[:, cols], preferred_element_type=jnp.float32)
                term[f, cut, c] = product.astype(jnp.bfloat16).reshape(term.shape[3:])
            to_partner(f, cut, g).start()

    def across_x(f, cut, g):
        part = pl.ds(*groups[g])
        return pltpu.make_async_remote_copy(
            src_ref=landed0.at[f, cut, part, 1 - across],
            dst_ref=landed1.at[f, cut, part],
            send_sem=s5,
            recv_sem=r5.at[f, cut, g],
            device_id={"head": h + 2 - 4 * across},
            device_id_type=MESH,
        )

    def pair_sum(f, cut, g):
        part = pl.ds(*groups[g])
        to_partner(f, cut, g).wait_recv()
        total = term[f, cut, part, core].astype(jnp.float32)
        total = total + landed0[f, cut, part].astype(jnp.float32)
        landed0[f, cut, part] = total.astype(jnp.bfloat16)
        across_x(f, cut, g).start()

    def full_sum(f, cut, g):
        part = pl.ds(*groups[g])
        across_x(f, cut, g).wait_recv()
        total = landed0[f, cut, part, across].astype(jnp.float32)
        total = total + landed1[f, cut, part].astype(jnp.float32)
        landed1[f, cut, part] = total.astype(jnp.bfloat16)
        for ds in (2, 1, 3):
            to_s = lax.rem(s + ds, p.ns)

            @pl.when(pair_of(to_s) == cut)
            def _():
                pltpu.make_async_remote_copy(
                    src_ref=landed1.at[f, cut, part, to_s >> 1],
                    dst_ref=final.at[f, part, ds - 1],
                    send_sem=s6,
                    recv_sem=r6.at[f, g],
                    device_id={"seq": to_s},
                    device_id_type=MESH,
                ).start()

    both = range(len(groups))

    def pair_sums(f, cut):
        for g in both:
            pair_sum(f, cut, g)

    def full_sums(f, cut):
        for g in both:
            full_sum(f, cut, g)

    gather_part(*parts[0])
    at_middle(gather_part, *parts[1])

    @at_middle
    def _():
        for j in range(p.few, 2 * p.few):
            send_own(1, j, (True,))

    late[0].wait()
    project(*parts[0])
    at_ends(gather_part, *parts[1])
    project(*parts[1])
    pair_sums(*parts[0])
    at_middle(gather_part, *parts[2])
    at_middle(gather_part, *parts[3])
    pair_sums(*parts[1])
    at_ends(gather_part, *parts[2])
    project(*parts[2])
    at_ends(pair_sums, *parts[2])
    at_ends(full_sums, *parts[0])
    at_ends(gather_part, *parts[3])
    project(*parts[3])
    at_middle(pair_sums, *parts[2])
    pair_sums(*parts[3])
    full_sums(*parts[1])
    at_middle(full_sums, *parts[0])
    at_middle(full_sums, *parts[3])
    full_sums(*parts[2])
    at_ends(full_sums, *parts[3])
    for copy in late[1:]:
        copy.wait()
    for i, row in enumerate(row_pair):
        rows_ref[i] = row[...]

    def finish(f, c, sums):
        for g, (start, count) in enumerate(groups):
            if c == start:
                pieces = final.at[f, pl.ds(start, count)]
                pltpu.make_async_copy(pieces, pieces, r6.at[f, g]).wait()
        rows = slice(f * p.cells, (f + 1) * p.cells)
        for ds in range(p.ns):
            j = lax.rem(s - ds + p.ns, p.ns)
            cols = pl.ds(pl.multiple_of(j * p.columns + c * p.chunk, 128), p.chunk)
            part = landed1[f, pair_of(s), c, place] if ds == 0 else final[f, c, ds - 1]
            added = gate_ref[:, cols] * part.astype(jnp.float32)
            value = (res[rows, cols].astype(jnp.float32) + added).astype(jnp.bfloat16)
            hidden_ref[rows, cols] = value
            sums = sums + jnp.sum(value.astype(jnp.float32), -1, keepdims=True)
        return sums

    patch[...] = jnp.zeros_like(patch)

    def head(f, sums):
        rows = slice(f * p.cells, (f + 1) * p.cells)
        center = hidden_ref[rows].astype(jnp.float32) - sums / p.width
        spread = jnp.mean(center * center, -1, keepdims=True)
        normed = center * lax.rsqrt(spread + 1e-06) * (1.0 + scale_ref[...]) + shift_ref[...]
        values = lax.dot_general(
            normed.astype(jnp.bfloat16),
            head_w[...],
            (((1,), (1,)), ((), ())),
            preferred_element_type=jnp.float32,
        )
        values = (values + bias_ref[...]).astype(jnp.bfloat16)
        patch[rows, : values.shape[-1]] = values

    sums = [jnp.zeros((p.cells, 1), jnp.float32) for _ in range(p.frames)]
    for c in range(p.chunks):
        sums[0] = finish(0, c, sums[0])
    head(0, sums[0])
    for c in range(p.chunks):
        sums[1] = finish(1, c, sums[1])
    head(1, sums[1])
    blank = jnp.zeros(patch.shape, patch.dtype)

    moves = [(0, 1), (0, -1), (1, 0), (1, 1), (1, -1)]

    def edge(index, sign):
        dh, ds = moves[index]
        return (
            (h + sign * dh >= 0) & (h + sign * dh < p.nh)
            & (s + sign * ds >= 0) & (s + sign * ds < p.ns)
        )

    def reach(index):
        dh, ds = moves[index]
        return pltpu.make_async_remote_copy(
            src_ref=patch,
            dst_ref=halo.at[index],
            send_sem=s7.at[index],
            recv_sem=r7.at[index],
            device_id={"seq": lax.rem(s + ds + p.ns, p.ns), "head": lax.rem(h + dh, p.nh)},
            device_id_type=MESH,
        )

    for index in range(len(moves)):

        @pl.when(edge(index, 1))
        def _():
            reach(index).start()

    near_ref[1, 1] = patch[...]
    for index, (dh, ds) in enumerate(moves):

        @pl.when(edge(index, -1))
        def _():
            reach(index).wait_recv()
            near_ref[1 - dh, 1 - ds] = halo[index]

        @pl.when(jnp.logical_not(edge(index, -1)))
        def _():
            near_ref[1 - dh, 1 - ds] = blank

    for index in range(len(moves)):

        @pl.when(edge(index, 1))
        def _():
            reach(index).wait_send()

    def all_sent(part, sem):
        pltpu.make_async_copy(part, part, sem).wait()

    for row in range(p.ns):
        @pl.when(s == row)
        def _():
            foreign = (p.nh * p.group - p.counts[row]) * HEAD_DIM
            all_sent(qkv.at[:, :, :, pl.ds(0, foreign)], s1)
            for relayed in range(2):
                heads = [head for head in range(p.group) if (p.owner[head] != row) == relayed]
                sent = sum(len(targets(head, row)) for head in heads)
                if sent:
                    all_sent(att.at[:, pl.ds(0, sent)], s3.at[relayed])

    all_sent(landed0, s4)
    all_sent(landed1, s5)
    all_sent(final, s6)


def spread_weights(conv_w, wide_ref):
    taps, depth, channels = conv_w.shape
    part = depth // 3
    for a in range(2):
        for dt in range(3):
            for dy in range(3):
                base = (1 - a + dy) * 4 * part
                tap = conv_w[dt * 3 + dy]
                wide_ref[a, dt, base : base + depth, :channels] = tap
                wide_ref[a, dt, base + part : base + part + depth, channels:] = tap


def conv_kernel(
    cells, hidden_ref, near_ref, wide_ref, rows_ref, hidden_out, features_out, mixed, features, sems
):
    tokens = near_ref.shape[2]
    lanes = near_ref.shape[3]
    part = lanes // 8
    channels = features.shape[-1]
    hidden_copy = pltpu.make_async_copy(hidden_ref, hidden_out, sems.at[0])
    hidden_copy.start()

    values = near_ref[...].reshape(-1, lanes).astype(jnp.float32)
    total = values.shape[0]
    column = lax.broadcasted_iota(jnp.int32, values.shape, 0) % cells
    left = jnp.where(column == 0, 0.0, pltpu.roll(values, 1, 0))
    right = jnp.where(column == cells - 1, 0.0, pltpu.roll(values, total - 1, 0))

    source = lax.broadcasted_iota(jnp.int32, (lanes, lanes), 0)
    target = lax.broadcasted_iota(jnp.int32, (lanes, lanes), 1)
    upper, place = target // (4 * part), target % (4 * part)
    start = upper * 2 * part

    def moved(x, low, high, first):
        pick = (place >= low * part) & (place < high * part)
        pick = pick & (source == start + place + (first - low) * part)
        matrix = jnp.where(pick, 1.0, 0.0).astype(jnp.bfloat16)
        return jnp.dot(x.astype(jnp.bfloat16), matrix, preferred_element_type=jnp.float32)

    strip = moved(left, 0, 1, 1) + moved(values, 1, 3, 0) + moved(right, 3, 4, 0)
    strip = strip.reshape(2, 3, tokens, lanes).astype(jnp.bfloat16)

    def at_time(dt, row):
        if dt == 1:
            return jnp.concatenate([strip[0, row, cells:], strip[1, row, :cells]], axis=0)
        return strip[dt // 2, row]

    for a in range(2):
        taken = [at_time(dt, row) for dt in range(3) for row in (a, a + 1)]
        linear = jnp.dot(
            jnp.concatenate(taken, axis=1),
            wide_ref[a].reshape(-1, 2 * channels),
            preferred_element_type=jnp.float32,
        )
        for b in range(2):
            value = linear[:, b * channels : (b + 1) * channels] + rows_ref[0:1]
            square = jnp.mean(value * value, -1, keepdims=True)
            value = value * lax.rsqrt(square + 1e-06) * rows_ref[1:2]
            value = value / (1.0 + jnp.exp(-value))
            for k in range(channels // 128):
                for f in range(2):
                    piece = value[f * cells : (f + 1) * cells, k * 128 : (k + 1) * 128]
                    mixed[k, f, a, pl.ds(b, cells, 2)] = piece
    for k in range(channels // 128):
        features[:, :, :, k * 128 : (k + 1) * 128] = mixed[k].astype(jnp.bfloat16)
    features_copy = pltpu.make_async_copy(features, features_out, sems.at[1])
    features_copy.start()
    hidden_copy.wait()
    features_copy.wait()


def on_device(
    queries,
    attn_keys,
    attn_values,
    residual,
    out_weight,
    out_gate,
    head_shift,
    head_scale,
    head_weight,
    head_bias,
    conv_weight,
    conv_bias,
    norm_gain,
):
    ns, nh = lax.axis_size("seq"), lax.axis_size("head")
    p = Plan(ns, nh, queries, residual, out_weight)
    if not p.fits(queries, head_weight, conv_weight):
        return on_device_gathered(
            queries, attn_keys, attn_values, residual, out_weight, out_gate, head_shift,
            head_scale, head_weight, head_bias, conv_weight, conv_bias, norm_gain,
        )
    frames, height, breadth, inner = queries.shape
    t, cells, width, patch_size = p.tokens, p.cells, p.width, head_weight.shape[1]
    dma, bf16 = pltpu.SemaphoreType.DMA, jnp.bfloat16
    lanes = -(-patch_size // 128) * 128
    channels = conv_weight.shape[-1]
    hbm = pl.BlockSpec(memory_space=pltpu.HBM)
    vmem = pl.BlockSpec(memory_space=pltpu.VMEM)
    hidden, near, wide, conv_rows = pl.pallas_call(
        functools.partial(block_kernel, p),
        out_shape=(
            jax.ShapeDtypeStruct((t, width), bf16),
            jax.ShapeDtypeStruct((2, 3, t, lanes), bf16),
            jax.ShapeDtypeStruct((2, 3, 2 * lanes, 2 * channels), bf16),
            jax.ShapeDtypeStruct((2, channels), jnp.float32),
        ),
        in_specs=[hbm] * 13,
        out_specs=(vmem,) * 4,
        scratch_shapes=[
            pltpu.VMEM((3, frames, cells, inner), bf16),
            pltpu.VMEM((2, 3, frames, p.slots, cells, p.few * HEAD_DIM), bf16),
            pltpu.VMEM((frames, p.group, p.slots * cells, HEAD_DIM), bf16),
            pltpu.VMEM(out_weight.shape, bf16),
            pltpu.VMEM((t, width), bf16),
            pltpu.VMEM(head_weight.shape[::-1], bf16),
            pltpu.VMEM((1, width), jnp.float32),
            pltpu.VMEM((1, width), jnp.float32),
            pltpu.VMEM((1, width), jnp.float32),
            pltpu.VMEM((1, patch_size), jnp.float32),
            pltpu.VMEM((9, 3 * conv_weight.shape[3], channels), bf16),
            pltpu.VMEM((channels,), jnp.float32),
            pltpu.VMEM((channels,), jnp.float32),
            pltpu.VMEM((frames, p.cuts, p.chunks, 2, 2, 2, cells, p.chunk), bf16),
            pltpu.VMEM((frames, p.cuts, p.chunks, 2, 2, cells, p.chunk), bf16),
            pltpu.VMEM((frames, p.cuts, p.chunks, 2, cells, p.chunk), bf16),
            pltpu.VMEM((frames, p.chunks, ns - 1, cells, p.chunk), bf16),
            pltpu.VMEM((t, lanes), bf16),
            pltpu.VMEM((5, t, lanes), bf16),
            dma(()),
            dma((10,)),
            dma((2,)),
            dma(()),
            dma((3,)),
            dma((2,)),
            dma((frames, p.group, p.cuts)),
            dma(()),
            dma((frames, p.cuts, 2)),
            dma(()),
            dma((frames, p.cuts, 2)),
            dma(()),
            dma((frames, 2)),
            dma((5,)),
            dma((5,)),
        ],
        compiler_params=pltpu.CompilerParams(
            collective_id=0, has_side_effects=True, vmem_limit_bytes=16 * 1024 * 1024
        ),
    )(*(pltpu.with_memory_space_constraint(x, pltpu.HBM) for x in (
        queries.reshape(frames, cells, inner),
        attn_keys.reshape(frames, cells, inner),
        attn_values.reshape(frames, cells, inner),
        residual.reshape(t, width),
        out_weight,
        head_weight.T,
        out_gate.reshape(1, -1),
        head_shift.reshape(1, -1),
        head_scale.reshape(1, -1),
        head_bias.reshape(1, -1),
        conv_weight.reshape(9, -1, channels),
        conv_bias,
        norm_gain,
    )))
    hidden, features = pl.pallas_call(
        functools.partial(conv_kernel, cells),
        out_shape=(
            jax.ShapeDtypeStruct((t, width), bf16),
            jax.ShapeDtypeStruct((frames, 2, 2 * cells, channels), bf16),
        ),
        in_specs=[vmem] * 4,
        out_specs=(hbm, hbm),
        scratch_shapes=[
            pltpu.VMEM((channels // 128, frames, 2, 2 * cells, 128), jnp.float32),
            pltpu.VMEM((frames, 2, 2 * cells, channels), bf16),
            dma((2,)),
        ],
        compiler_params=pltpu.CompilerParams(vmem_limit_bytes=8 * 1024 * 1024),
    )(hidden, near, wide, conv_rows)
    return (hidden.reshape(residual.shape), features)


def solution(mesh):
    return jax.shard_map(
        on_device,
        mesh=mesh,
        in_specs=(
            P(("clip", "head"), "seq", None, None),
            P(("clip", "head"), "seq", None, None),
            P(("clip", "head"), "seq", None, None),
            P(("clip", "head"), "seq", None, None),
            P("head", "seq"),
            P(),
            P(),
            P(),
            P(),
            P(),
            P(),
            P(),
            P(),
        ),
        out_specs=(P(("clip", "head"), "seq", None, None), P(("clip", "head"), "seq", None, None)),
        check_vma=False,
    )
```

```python
import functools
import math

import jax
import jax.numpy as jnp
from jax import lax
from jax.experimental import pallas as pl
from jax.experimental.pallas import tpu as pltpu
from jax.sharding import PartitionSpec as P

HEAD_DIM = 128


def from_behind(value, axis, steps):
    count = lax.axis_size(axis)
    first, last = (max(0, -steps), min(count, count - steps))
    return lax.ppermute(value, axis, [(source, source + steps) for source in range(first, last)])


def padded_2(x, sides, width):
    for axis, dim in sides:
        peers, length = (lax.axis_size(axis), x.shape[dim])
        up = [(i, (i + 1) % peers) for i in range(peers - 1)]
        down = [(j, i) for i, j in up]
        last = lax.slice_in_dim(x, length - width, length, axis=dim)
        first = lax.slice_in_dim(x, 0, width, axis=dim)
        before = lax.ppermute(last, axis, up)
        after = lax.ppermute(first, axis, down)
        x = jnp.concatenate([before, x, after], axis=dim)
    return x


def head_latent(hidden, head_shift, head_scale, head_weight, head_bias):
    values = hidden.astype(jnp.float32)
    center = values - jnp.mean(values, -1, keepdims=True)
    spread = jnp.mean(center * center, -1, keepdims=True)
    normed = (center * lax.rsqrt(spread + 1e-06) * (1.0 + head_scale) + head_shift).astype(
        jnp.bfloat16
    )
    flat = normed.reshape(-1, normed.shape[-1])
    latent = (jnp.dot(flat, head_weight, preferred_element_type=jnp.float32) + head_bias).astype(
        jnp.bfloat16
    )
    frames, height, breadth = (hidden.shape[0], hidden.shape[1], hidden.shape[2])
    channels = head_weight.shape[1] // 4
    patches = latent.reshape(frames, height, breadth, 2, 2, channels).transpose(0, 1, 3, 2, 4, 5)
    return patches.reshape(frames, height * 2, breadth * 2, channels)


def convolve(padded, frames, conv_weight, conv_bias, norm_gain):
    height = padded.shape[1] - 2
    breadth = padded.shape[2] - 2
    stacked = jnp.concatenate(
        [
            padded[
                time_off : time_off + frames,
                row_off : row_off + height,
                col_off : col_off + breadth,
            ]
            for time_off in range(3)
            for row_off in range(3)
            for col_off in range(3)
        ],
        -1,
    )
    kernel = conv_weight.reshape(-1, conv_weight.shape[-1])
    linear = (
        jnp.dot(stacked.reshape(-1, stacked.shape[-1]), kernel, preferred_element_type=jnp.float32)
        + conv_bias
    )
    normed = linear * lax.rsqrt(jnp.mean(linear * linear, -1, keepdims=True) + 1e-06) * norm_gain
    return jax.nn.silu(normed).astype(jnp.bfloat16).reshape(frames, height, breadth, -1)


def attend_block(carried, block_keys, block_values, query_heads):
    running, denominator, weighted = carried
    scores = jnp.einsum("hqd,khd->hqk", query_heads, block_keys, preferred_element_type=jnp.float32)
    scores = scores * query_heads.shape[-1] ** (-0.5)
    newmax = jnp.maximum(running, jnp.max(scores, -1))
    factor = jnp.exp(running - newmax)
    weights = jnp.exp(scores - newmax[..., None])
    denominator = denominator * factor + jnp.sum(weights, -1)
    product = jnp.einsum(
        "hqk,khd->hqd",
        weights.astype(jnp.bfloat16),
        block_values,
        preferred_element_type=jnp.float32,
    )
    weighted = weighted * factor[..., None] + product
    return (newmax, denominator, weighted)


def fold_pieces(query_heads, carried, pieces):
    key_piece, value_piece = pieces
    frames, height, breadth = (key_piece.shape[0], key_piece.shape[1], key_piece.shape[2])
    heads_here, head_width = (query_heads.shape[0], query_heads.shape[2])
    group_rows = 4

    def regroup(one_piece):
        shaped = one_piece.reshape(
            frames, height // group_rows, group_rows, breadth, heads_here, head_width
        )
        shaped = shaped.transpose(1, 0, 2, 3, 4, 5)
        return shaped.reshape(
            height // group_rows, frames * group_rows * breadth, heads_here, head_width
        )

    def advance(inner, blocks):
        return (attend_block(inner, blocks[0], blocks[1], query_heads), None)

    carried, _ = lax.scan(advance, carried, (regroup(key_piece), regroup(value_piece)))
    return carried


def on_device_gathered(
    queries,
    attn_keys,
    attn_values,
    residual,
    out_weight,
    out_gate,
    head_shift,
    head_scale,
    head_weight,
    head_bias,
    conv_weight,
    conv_bias,
    norm_gain,
):
    head_count = lax.axis_size("head")
    frames_dev = queries.shape[0]
    group_width = queries.shape[3] // head_count
    head_width = HEAD_DIM
    heads_here = group_width // head_width
    local_queries, local_keys, local_values = (
        lax.all_to_all(queries, "head", split_axis=3, concat_axis=0, tiled=True),
        lax.all_to_all(attn_keys, "head", split_axis=3, concat_axis=0, tiled=True),
        lax.all_to_all(attn_values, "head", split_axis=3, concat_axis=0, tiled=True),
    )
    frames_all, height, breadth = (
        local_queries.shape[0],
        local_queries.shape[1],
        local_queries.shape[2],
    )
    count = frames_all * height * breadth
    query_heads = local_queries.reshape(count, heads_here, head_width).transpose(1, 0, 2)
    initial = (
        jnp.full((heads_here, count), -1e30, jnp.float32),
        jnp.zeros((heads_here, count), jnp.float32),
        jnp.zeros((heads_here, count, head_width), jnp.float32),
    )
    carried = fold_pieces(
        query_heads,
        initial,
        (
            lax.all_gather(local_keys, "seq", axis=1, tiled=True),
            lax.all_gather(local_values, "seq", axis=1, tiled=True),
        ),
    )
    running, denominator, weighted = carried
    attended = (weighted / denominator[..., None]).astype(jnp.bfloat16)
    attended = attended.transpose(1, 0, 2).reshape(count, group_width)
    partial_value = jnp.dot(
        attended,
        lax.all_gather(out_weight, "seq", axis=1, tiled=True),
        preferred_element_type=jnp.float32,
    )
    partial_value = partial_value.reshape(frames_all, height, breadth, partial_value.shape[-1])
    owned = lax.psum_scatter(
        partial_value.astype(jnp.bfloat16), "head", scatter_dimension=0, tiled=True
    ).astype(jnp.float32)
    hidden = (residual.astype(jnp.float32) + out_gate * owned).astype(jnp.bfloat16)
    own_video = head_latent(hidden, head_shift, head_scale, head_weight, head_bias)
    earlier = from_behind(own_video, "head", 1)
    video = jnp.concatenate([earlier, own_video], 0)
    extended = padded_2(video, (("seq", 1),), 1)
    padded = jnp.pad(extended, ((0, 0), (0, 0), (1, 1), (0, 0)))
    features = convolve(padded, frames_dev, conv_weight, conv_bias, norm_gain)
    return (hidden, features)


MESH = pl.DeviceIdType.MESH


class Plan:
    def __init__(self, ns, nh, queries, residual, out_weight):
        self.ns, self.nh = ns, nh
        self.frames = queries.shape[0]
        self.cells = queries.shape[1] * queries.shape[2]
        self.inner = queries.shape[3]
        self.tokens = self.frames * self.cells
        self.group = self.inner // nh // HEAD_DIM
        self.few = max(1, self.group // 6)
        self.width = residual.shape[3]
        self.columns = out_weight.shape[1]
        self.slots = ns * nh
        self.chunk = 256 if self.columns % 256 == 0 else 128
        self.chunks = self.columns // self.chunk
        self.cuts = 2
        self.counts = (self.few, 2 * self.few, 2 * self.few, self.few)
        self.owner = [o for o, count in enumerate(self.counts) for _ in range(count)]

    def fits(self, queries, head_weight, conv_weight):
        return (
            self.nh == 4
            and self.ns == 4
            and self.group == 6 * self.few
            and self.inner == self.nh * self.group * HEAD_DIM
            and self.frames == 2
            and self.cells % 16 == 0
            and self.columns % 128 == 0
            and queries.shape[1] == 1
            and head_weight.shape[1] == 64
            and conv_weight.shape[3] == 16
            and conv_weight.shape[4] % 128 == 0
            and self.slots * self.tokens <= 1024
        )


def source_row(o, row):
    step = 1 if row > o else -1
    return o if o in (0, 3) and abs(row - o) < 3 else row - step


def due(o, unit, f, row):
    away = abs(row - o)
    if o in (0, 3):
        return (0, 15.0, 16.5, 18.5)[away] + 6.5 * f
    if row == 3 * (o // 2):
        return (10.0, 18.0)[unit] + 1.4 * f
    return (15.7, 19.4)[unit] + 3.0 * (away - 1) + 1.4 * f


def block_kernel(
    plan,
    q_hbm, k_hbm, v_hbm, res_hbm, w_hbm, hw_hbm,
    gate_hbm, shift_hbm, scale_hbm, bias_hbm, cw_hbm, cb_hbm, gain_hbm,
    hidden_ref, near_ref, wide_ref, rows_ref,
    qkv, got, att, weight, res, head_w, gate_ref, shift_ref, scale_ref, bias_ref, conv_w, bias_row, gain_row, term, landed0, landed1, final, patch, halo,
    far, load_sem, local_sem, own_sem, s1, r1, s3, r3, s4, r4, s5, r5, s6, r6, s7, r7,
):
    p = plan
    s = lax.axis_index("seq")
    h = lax.axis_index("head")
    core, across = h & 1, h >> 1
    row_pair = (bias_row, gain_row)

    def pair_of(seq_index):
        return ((seq_index + 1) >> 1) & 1

    place = s >> 1
    here = ((pair_of(s) * 2 + core) * 2 + across) * 2 + place
    at_end = (s == 0) | (s == p.ns - 1)
    wide = p.few * HEAD_DIM

    def columns_of(seq_index, head_index, unit):
        before = p.few * (jnp.maximum(2 * seq_index - 1, 0) + unit)
        return pl.ds(pl.multiple_of((head_index * p.group + before) * HEAD_DIM, HEAD_DIM), wide)

    sources = (q_hbm, k_hbm, v_hbm)
    loads = [pltpu.make_async_copy(ref, qkv.at[i], load_sem) for i, ref in enumerate(sources)]
    loaded = pltpu.make_async_copy(qkv, qkv, load_sem)
    late = [
        pltpu.make_async_copy(w_hbm, weight, local_sem.at[0]),
        pltpu.make_async_copy(res_hbm, res, local_sem.at[1]),
        pltpu.make_async_copy(hw_hbm, head_w, local_sem.at[2]),
        pltpu.make_async_copy(gate_hbm, gate_ref, local_sem.at[3]),
        pltpu.make_async_copy(shift_hbm, shift_ref, local_sem.at[4]),
        pltpu.make_async_copy(scale_hbm, scale_ref, local_sem.at[5]),
        pltpu.make_async_copy(bias_hbm, bias_ref, local_sem.at[6]),
        pltpu.make_async_copy(cb_hbm, row_pair[0], local_sem.at[7]),
        pltpu.make_async_copy(gain_hbm, row_pair[1], local_sem.at[8]),
    ]
    conv_load = pltpu.make_async_copy(cw_hbm, conv_w, local_sem.at[9])

    def own_copies(unit):
        cols = columns_of(s, h, unit)
        return [
            pltpu.make_async_copy(ref.at[:, :, cols], got.at[unit, i, :, here], own_sem.at[unit])
            for i, ref in enumerate(sources)
        ]

    def own_copied(unit):
        part = got.at[unit, :, :, here]
        return pltpu.make_async_copy(part, part, own_sem.at[unit])

    for copy in loads:
        copy.start()

    def others(row, to_s):
        for dh in range(p.nh):
            if row != to_s or dh:
                yield lax.rem(h + dh, p.nh)

    def say(sem, **to):
        pl.semaphore_signal(sem, inc=1, device_id=to, device_id_type=MESH)

    barrier = pltpu.get_barrier_semaphore()
    for row in range(p.ns):
        @pl.when(s == row)
        def _():
            for to_s in range(max(row - 1, 0), min(row + 2, p.ns)):
                for to_h in others(row, to_s):
                    say(barrier, seq=to_s, head=to_h)

    for copy in own_copies(0):
        copy.start()

    @pl.when(jnp.logical_not(at_end))
    def _():
        for copy in own_copies(1):
            copy.start()

    loaded.wait()

    def exchange(stage, to_s, to_h):
        unit = stage // 2
        return pltpu.make_async_remote_copy(
            src_ref=qkv.at[:, :, :, columns_of(to_s, to_h, unit)],
            dst_ref=got.at[unit, :, :, here],
            send_sem=s1,
            recv_sem=r1.at[stage],
            device_id={"seq": to_s, "head": to_h},
            device_id_type=MESH,
        )

    def send_to(row, stages, away):
        for stage in stages:
            for to_s in range(p.ns):
                if (to_s in (0, p.ns - 1)) == (stage == 0) and abs(to_s - row) in away:
                    for to_h in others(row, to_s):
                        exchange(stage, to_s, to_h).start()

    for row in range(p.ns):
        @pl.when(s == row)
        def _():
            beside = [r for r in (row - 1, row + 1) if 0 <= r < p.ns]
            pl.semaphore_wait(barrier, p.nh * (1 + len(beside)) - 1)
            if len(beside) == 2:
                for to_s in beside:
                    say(far.at[0], seq=to_s)
            send_to(row, (1, 0), (0, 1))
            pl.semaphore_wait(far.at[0], 1)
            if len(beside) == 2:
                say(far.at[1], seq=3 * (row // 2))
            send_to(row, (1, 0), (2,))
            if len(beside) == 1:
                pl.semaphore_wait(far.at[1], 1)
                send_to(row, (0,), (3,))
            send_to(row, (2,), range(p.ns))

    def arrived(stage):
        parts = got.at[stage // 2, :, :, pl.ds(0, p.slots - 1)]
        pltpu.make_async_copy(parts, parts, r1.at[stage]).wait()

    conv_load.start()
    for copy in late:
        copy.start()
    wide_ref[...] = jnp.zeros_like(wide_ref)
    conv_load.wait()
    spread_weights(conv_w, wide_ref)

    def hop(f, head, cut, to_s, relayed):
        rows = p.slots * p.cells // p.cuts
        piece = att.at[f, head, pl.ds(cut * rows, rows)]
        return pltpu.make_async_remote_copy(
            src_ref=piece,
            dst_ref=piece,
            send_sem=s3.at[relayed],
            recv_sem=r3.at[f, head, cut],
            device_id={"seq": to_s},
            device_id_type=MESH,
        )

    def attend(f, j):
        unit, lanes = j // p.few, pl.ds(j % p.few * HEAD_DIM, HEAD_DIM)
        q = got[unit, 0, f, :, :, lanes].reshape(-1, HEAD_DIM)
        k = got[unit, 1, :, :, :, lanes].reshape(-1, HEAD_DIM)
        v = got[unit, 2, :, :, :, lanes].reshape(-1, HEAD_DIM)
        scores = lax.dot_general(
            q, k, (((1,), (1,)), ((), ())), preferred_element_type=jnp.float32
        )
        scale = HEAD_DIM ** (-0.5) * math.log2(math.e)
        weights = jnp.exp2((scores - jnp.max(scores, -1, keepdims=True)) * scale)
        denominator = jnp.sum(weights, -1, keepdims=True)
        product = jnp.dot(weights.astype(jnp.bfloat16), v, preferred_element_type=jnp.float32)
        att[f, p.few * jnp.maximum(2 * s - 1, 0) + j] = (product / denominator).astype(jnp.bfloat16)

    parts = [(f, cut) for f in range(p.frames) for cut in range(p.cuts)]

    def targets(head, row):
        o = p.owner[head]
        rows = [r for r in range(p.ns) if r != o and source_row(o, r) == row]
        return sorted(rows, key=lambda r: -abs(r - row))

    def send_own(f, j, outward=(True, False)):
        for row in range(p.ns):
            if j < p.counts[row]:
                head = p.owner.index(row) + j

                @pl.when(s == row)
                def _():
                    rows = [r for r in targets(head, row) if (r in (0, p.ns - 1)) in outward]
                    pieces = [(cut, to_s) for cut in range(p.cuts) for to_s in rows]
                    for cut, to_s in pieces:
                        hop(f, head, cut, to_s, 0).start()

    def order(row):
        def when(item):
            f, cut, head = item
            o = p.owner[head]
            passive = not targets(head, row)
            return (f, cut, passive, due(o, (head - p.owner.index(o)) // p.few, f, row), head)

        heads = [head for head in range(p.group) if p.owner[head] != row]
        return sorted(((f, cut, head) for f, cut in parts for head in heads), key=when)

    def gather(todo):
        for row in range(p.ns):
            @pl.when(s == row)
            def _():
                for f, cut, head in todo(row):
                    hop(f, head, cut, row, 1).wait_recv()
                    for to_s in targets(head, row):
                        hop(f, head, cut, to_s, 1).start()

    def early_part(row):
        def early(f, cut, head):
            unit = (head - p.owner.index(p.owner[head])) // p.few
            return f == 0 and unit == 0 and row in (1, 2) and targets(head, row)

        return [item for item in order(row) if early(*item)]

    def first_part(row):
        if row not in (0, p.ns - 1):
            return []
        return [(0, 0, head) for head in range(p.group) if p.owner[head] == (1, 2)[row // 3]]

    def gather_part(f, cut):
        def todo(row):
            done = early_part(row) + first_part(row)
            return [item for item in order(row) if item[:2] == (f, cut) and item not in done]

        gather(todo)

    own_copied(0).wait()
    pl.when(at_end)(functools.partial(arrived, 0))
    pl.when(jnp.logical_not(at_end))(functools.partial(arrived, 1))
    def at_ends(act, *of):
        pl.when(at_end)(functools.partial(act, *of))

    def at_middle(act, *of):
        pl.when(jnp.logical_not(at_end))(functools.partial(act, *of))

    for f in range(p.frames):
        for j in range(p.few):
            attend(f, j)
            if f == 0:
                send_own(f, j)
            else:
                at_middle(send_own, f, j, (True,))

    @at_middle
    def _():
        own_copied(1).wait()
        arrived(2)
        for f in range(p.frames):
            for j in range(p.few, 2 * p.few):
                attend(f, j)
                send_own(f, j, (True, False) if f == 0 else (False,))
            if f == 0:
                for j in range(p.few):
                    send_own(1, j, (False,))
                gather(early_part)

    @at_ends
    def _():
        gather(first_part)
        for j in range(p.few):
            send_own(1, j)

    groups = [(0, 2), (2, p.chunks - 2)] if p.chunks > 3 else [(0, p.chunks)]

    def to_partner(f, cut, g):
        part = pl.ds(*groups[g])
        return pltpu.make_async_remote_copy(
            src_ref=term.at[f, cut, part, 1 - core],
            dst_ref=landed0.at[f, cut, part],
            send_sem=s4,
            recv_sem=r4.at[f, cut, g],
            device_id={"head": h + 1 - 2 * core},
            device_id_type=MESH,
        )

    def project(f, cut):
        length = p.slots * p.cells // p.cuts
        own = pl.ds(cut * length, length)
        rows = jnp.concatenate([att[f, head, own] for head in range(p.group)], axis=1)
        for g, (start, count) in enumerate(groups):
            for c in range(start, start + count):
                cols = pl.ds(c * p.chunk, p.chunk)
                product = jnp.dot(rows, weight[:, cols], preferred_element_type=jnp.float32)
                term[f, cut, c] = product.astype(jnp.bfloat16).reshape(term.shape[3:])
            to_partner(f, cut, g).start()

    def across_x(f, cut, g):
        part = pl.ds(*groups[g])
        return pltpu.make_async_remote_copy(
            src_ref=landed0.at[f, cut, part, 1 - across],
            dst_ref=landed1.at[f, cut, part],
            send_sem=s5,
            recv_sem=r5.at[f, cut, g],
            device_id={"head": h + 2 - 4 * across},
            device_id_type=MESH,
        )

    def pair_sum(f, cut, g):
        part = pl.ds(*groups[g])
        to_partner(f, cut, g).wait_recv()
        total = term[f, cut, part, core].astype(jnp.float32)
        total = total + landed0[f, cut, part].astype(jnp.float32)
        landed0[f, cut, part] = total.astype(jnp.bfloat16)
        across_x(f, cut, g).start()

    def full_sum(f, cut, g):
        part = pl.ds(*groups[g])
        across_x(f, cut, g).wait_recv()
        total = landed0[f, cut, part, across].astype(jnp.float32)
        total = total + landed1[f, cut, part].astype(jnp.float32)
        landed1[f, cut, part] = total.astype(jnp.bfloat16)
        for ds in (2, 1, 3):
            to_s = lax.rem(s + ds, p.ns)

            @pl.when(pair_of(to_s) == cut)
            def _():
                pltpu.make_async_remote_copy(
                    src_ref=landed1.at[f, cut, part, to_s >> 1],
                    dst_ref=final.at[f, part, ds - 1],
                    send_sem=s6,
                    recv_sem=r6.at[f, g],
                    device_id={"seq": to_s},
                    device_id_type=MESH,
                ).start()

    both = range(len(groups))

    def pair_sums(f, cut):
        for g in both:
            pair_sum(f, cut, g)

    def full_sums(f, cut):
        for g in both:
            full_sum(f, cut, g)

    gather_part(*parts[0])
    at_middle(gather_part, *parts[1])

    @at_middle
    def _():
        for j in range(p.few, 2 * p.few):
            send_own(1, j, (True,))

    late[0].wait()
    project(*parts[0])
    at_ends(gather_part, *parts[1])
    project(*parts[1])
    pair_sums(*parts[0])
    at_middle(gather_part, *parts[2])
    at_middle(gather_part, *parts[3])
    pair_sums(*parts[1])
    at_ends(gather_part, *parts[2])
    project(*parts[2])
    at_ends(pair_sums, *parts[2])
    at_ends(full_sums, *parts[0])
    at_ends(gather_part, *parts[3])
    project(*parts[3])
    at_middle(pair_sums, *parts[2])
    pair_sums(*parts[3])
    full_sums(*parts[1])
    at_middle(full_sums, *parts[0])
    at_middle(full_sums, *parts[3])
    full_sums(*parts[2])
    at_ends(full_sums, *parts[3])
    for copy in late[1:]:
        copy.wait()
    for i, row in enumerate(row_pair):
        rows_ref[i] = row[...]

    def finish(f, c, sums):
        for g, (start, count) in enumerate(groups):
            if c == start:
                pieces = final.at[f, pl.ds(start, count)]
                pltpu.make_async_copy(pieces, pieces, r6.at[f, g]).wait()
        rows = slice(f * p.cells, (f + 1) * p.cells)
        for ds in range(p.ns):
            j = lax.rem(s - ds + p.ns, p.ns)
            cols = pl.ds(pl.multiple_of(j * p.columns + c * p.chunk, 128), p.chunk)
            part = landed1[f, pair_of(s), c, place] if ds == 0 else final[f, c, ds - 1]
            added = gate_ref[:, cols] * part.astype(jnp.float32)
            value = (res[rows, cols].astype(jnp.float32) + added).astype(jnp.bfloat16)
            hidden_ref[rows, cols] = value
            sums = sums + jnp.sum(value.astype(jnp.float32), -1, keepdims=True)
        return sums

    patch[...] = jnp.zeros_like(patch)

    def head(f, sums):
        rows = slice(f * p.cells, (f + 1) * p.cells)
        center = hidden_ref[rows].astype(jnp.float32) - sums / p.width
        spread = jnp.mean(center * center, -1, keepdims=True)
        normed = center * lax.rsqrt(spread + 1e-06) * (1.0 + scale_ref[...]) + shift_ref[...]
        values = lax.dot_general(
            normed.astype(jnp.bfloat16),
            head_w[...],
            (((1,), (1,)), ((), ())),
            preferred_element_type=jnp.float32,
        )
        values = (values + bias_ref[...]).astype(jnp.bfloat16)
        patch[rows, : values.shape[-1]] = values

    sums = [jnp.zeros((p.cells, 1), jnp.float32) for _ in range(p.frames)]
    for c in range(p.chunks):
        sums[0] = finish(0, c, sums[0])
    head(0, sums[0])
    for c in range(p.chunks):
        sums[1] = finish(1, c, sums[1])
    head(1, sums[1])
    blank = jnp.zeros(patch.shape, patch.dtype)

    moves = [(0, 1), (0, -1), (1, 0), (1, 1), (1, -1)]

    def edge(index, sign):
        dh, ds = moves[index]
        return (
            (h + sign * dh >= 0) & (h + sign * dh < p.nh)
            & (s + sign * ds >= 0) & (s + sign * ds < p.ns)
        )

    def reach(index):
        dh, ds = moves[index]
        return pltpu.make_async_remote_copy(
            src_ref=patch,
            dst_ref=halo.at[index],
            send_sem=s7.at[index],
            recv_sem=r7.at[index],
            device_id={"seq": lax.rem(s + ds + p.ns, p.ns), "head": lax.rem(h + dh, p.nh)},
            device_id_type=MESH,
        )

    for index in range(len(moves)):

        @pl.when(edge(index, 1))
        def _():
            reach(index).start()

    near_ref[1, 1] = patch[...]
    for index, (dh, ds) in enumerate(moves):

        @pl.when(edge(index, -1))
        def _():
            reach(index).wait_recv()
            near_ref[1 - dh, 1 - ds] = halo[index]

        @pl.when(jnp.logical_not(edge(index, -1)))
        def _():
            near_ref[1 - dh, 1 - ds] = blank

    for index in range(len(moves)):

        @pl.when(edge(index, 1))
        def _():
            reach(index).wait_send()

    def all_sent(part, sem):
        pltpu.make_async_copy(part, part, sem).wait()

    for row in range(p.ns):
        @pl.when(s == row)
        def _():
            foreign = (p.nh * p.group - p.counts[row]) * HEAD_DIM
            all_sent(qkv.at[:, :, :, pl.ds(0, foreign)], s1)
            for relayed in range(2):
                heads = [head for head in range(p.group) if (p.owner[head] != row) == relayed]
                sent = sum(len(targets(head, row)) for head in heads)
                if sent:
                    all_sent(att.at[:, pl.ds(0, sent)], s3.at[relayed])

    all_sent(landed0, s4)
    all_sent(landed1, s5)
    all_sent(final, s6)


def spread_weights(conv_w, wide_ref):
    taps, depth, channels = conv_w.shape
    part = depth // 3
    for a in range(2):
        for dt in range(3):
            for dy in range(3):
                base = (1 - a + dy) * 4 * part
                tap = conv_w[dt * 3 + dy]
                wide_ref[a, dt, base : base + depth, :channels] = tap
                wide_ref[a, dt, base + part : base + part + depth, channels:] = tap


def conv_kernel(
    cells, hidden_ref, near_ref, wide_ref, rows_ref, hidden_out, features_out, mixed, features, sems
):
    tokens = near_ref.shape[2]
    lanes = near_ref.shape[3]
    part = lanes // 8
    channels = features.shape[-1]
    hidden_copy = pltpu.make_async_copy(hidden_ref, hidden_out, sems.at[0])
    hidden_copy.start()

    values = near_ref[...].reshape(-1, lanes).astype(jnp.float32)
    total = values.shape[0]
    column = lax.broadcasted_iota(jnp.int32, values.shape, 0) % cells
    left = jnp.where(column == 0, 0.0, pltpu.roll(values, 1, 0))
    right = jnp.where(column == cells - 1, 0.0, pltpu.roll(values, total - 1, 0))

    source = lax.broadcasted_iota(jnp.int32, (lanes, lanes), 0)
    target = lax.broadcasted_iota(jnp.int32, (lanes, lanes), 1)
    upper, place = target // (4 * part), target % (4 * part)
    start = upper * 2 * part

    def moved(x, low, high, first):
        pick = (place >= low * part) & (place < high * part)
        pick = pick & (source == start + place + (first - low) * part)
        matrix = jnp.where(pick, 1.0, 0.0).astype(jnp.bfloat16)
        return jnp.dot(x.astype(jnp.bfloat16), matrix, preferred_element_type=jnp.float32)

    strip = moved(left, 0, 1, 1) + moved(values, 1, 3, 0) + moved(right, 3, 4, 0)
    strip = strip.reshape(2, 3, tokens, lanes).astype(jnp.bfloat16)

    def at_time(dt, row):
        if dt == 1:
            return jnp.concatenate([strip[0, row, cells:], strip[1, row, :cells]], axis=0)
        return strip[dt // 2, row]

    for a in range(2):
        taken = [at_time(dt, row) for dt in range(3) for row in (a, a + 1)]
        linear = jnp.dot(
            jnp.concatenate(taken, axis=1),
            wide_ref[a].reshape(-1, 2 * channels),
            preferred_element_type=jnp.float32,
        )
        for b in range(2):
            value = linear[:, b * channels : (b + 1) * channels] + rows_ref[0:1]
            square = jnp.mean(value * value, -1, keepdims=True)
            value = value * lax.rsqrt(square + 1e-06) * rows_ref[1:2]
            value = value / (1.0 + jnp.exp(-value))
            for k in range(channels // 128):
                for f in range(2):
                    piece = value[f * cells : (f + 1) * cells, k * 128 : (k + 1) * 128]
                    mixed[k, f, a, pl.ds(b, cells, 2)] = piece
    for k in range(channels // 128):
        features[:, :, :, k * 128 : (k + 1) * 128] = mixed[k].astype(jnp.bfloat16)
    features_copy = pltpu.make_async_copy(features, features_out, sems.at[1])
    features_copy.start()
    hidden_copy.wait()
    features_copy.wait()


def on_device(
    queries,
    attn_keys,
    attn_values,
    residual,
    out_weight,
    out_gate,
    head_shift,
    head_scale,
    head_weight,
    head_bias,
    conv_weight,
    conv_bias,
    norm_gain,
):
    ns, nh = lax.axis_size("seq"), lax.axis_size("head")
    p = Plan(ns, nh, queries, residual, out_weight)
    if not p.fits(queries, head_weight, conv_weight):
        return on_device_gathered(
            queries, attn_keys, attn_values, residual, out_weight, out_gate, head_shift,
            head_scale, head_weight, head_bias, conv_weight, conv_bias, norm_gain,
        )
    frames, height, breadth, inner = queries.shape
    t, cells, width, patch_size = p.tokens, p.cells, p.width, head_weight.shape[1]
    dma, bf16 = pltpu.SemaphoreType.DMA, jnp.bfloat16
    lanes = -(-patch_size // 128) * 128
    channels = conv_weight.shape[-1]
    hbm = pl.BlockSpec(memory_space=pltpu.HBM)
    vmem = pl.BlockSpec(memory_space=pltpu.VMEM)
    hidden, near, wide, conv_rows = pl.pallas_call(
        functools.partial(block_kernel, p),
        out_shape=(
            jax.ShapeDtypeStruct((t, width), bf16),
            jax.ShapeDtypeStruct((2, 3, t, lanes), bf16),
            jax.ShapeDtypeStruct((2, 3, 2 * lanes, 2 * channels), bf16),
            jax.ShapeDtypeStruct((2, channels), jnp.float32),
        ),
        in_specs=[hbm] * 13,
        out_specs=(vmem,) * 4,
        scratch_shapes=[
            pltpu.VMEM((3, frames, cells, inner), bf16),
            pltpu.VMEM((2, 3, frames, p.slots, cells, p.few * HEAD_DIM), bf16),
            pltpu.VMEM((frames, p.group, p.slots * cells, HEAD_DIM), bf16),
            pltpu.VMEM(out_weight.shape, bf16),
            pltpu.VMEM((t, width), bf16),
            pltpu.VMEM(head_weight.shape[::-1], bf16),
            pltpu.VMEM((1, width), jnp.float32),
            pltpu.VMEM((1, width), jnp.float32),
            pltpu.VMEM((1, width), jnp.float32),
            pltpu.VMEM((1, patch_size), jnp.float32),
            pltpu.VMEM((9, 3 * conv_weight.shape[3], channels), bf16),
            pltpu.VMEM((channels,), jnp.float32),
            pltpu.VMEM((channels,), jnp.float32),
            pltpu.VMEM((frames, p.cuts, p.chunks, 2, 2, 2, cells, p.chunk), bf16),
            pltpu.VMEM((frames, p.cuts, p.chunks, 2, 2, cells, p.chunk), bf16),
            pltpu.VMEM((frames, p.cuts, p.chunks, 2, cells, p.chunk), bf16),
            pltpu.VMEM((frames, p.chunks, ns - 1, cells, p.chunk), bf16),
            pltpu.VMEM((t, lanes), bf16),
            pltpu.VMEM((5, t, lanes), bf16),
            pltpu.SemaphoreType.REGULAR((2,)),
            dma(()),
            dma((10,)),
            dma((2,)),
            dma(()),
            dma((3,)),
            dma((2,)),
            dma((frames, p.group, p.cuts)),
            dma(()),
            dma((frames, p.cuts, 2)),
            dma(()),
            dma((frames, p.cuts, 2)),
            dma(()),
            dma((frames, 2)),
            dma((5,)),
            dma((5,)),
        ],
        compiler_params=pltpu.CompilerParams(
            collective_id=0, has_side_effects=True, vmem_limit_bytes=16 * 1024 * 1024
        ),
    )(*(pltpu.with_memory_space_constraint(x, pltpu.HBM) for x in (
        queries.reshape(frames, cells, inner),
        attn_keys.reshape(frames, cells, inner),
        attn_values.reshape(frames, cells, inner),
        residual.reshape(t, width),
        out_weight,
        head_weight.T,
        out_gate.reshape(1, -1),
        head_shift.reshape(1, -1),
        head_scale.reshape(1, -1),
        head_bias.reshape(1, -1),
        conv_weight.reshape(9, -1, channels),
        conv_bias,
        norm_gain,
    )))
    hidden, features = pl.pallas_call(
        functools.partial(conv_kernel, cells),
        out_shape=(
            jax.ShapeDtypeStruct((t, width), bf16),
            jax.ShapeDtypeStruct((frames, 2, 2 * cells, channels), bf16),
        ),
        in_specs=[vmem] * 4,
        out_specs=(hbm, hbm),
        scratch_shapes=[
            pltpu.VMEM((channels // 128, frames, 2, 2 * cells, 128), jnp.float32),
            pltpu.VMEM((frames, 2, 2 * cells, channels), bf16),
            dma((2,)),
        ],
        compiler_params=pltpu.CompilerParams(vmem_limit_bytes=8 * 1024 * 1024),
    )(hidden, near, wide, conv_rows)
    return (hidden.reshape(residual.shape), features)


def solution(mesh):
    return jax.shard_map(
        on_device,
        mesh=mesh,
        in_specs=(
            P(("clip", "head"), "seq", None, None),
            P(("clip", "head"), "seq", None, None),
            P(("clip", "head"), "seq", None, None),
            P(("clip", "head"), "seq", None, None),
            P("head", "seq"),
            P(),
            P(),
            P(),
            P(),
            P(),
            P(),
            P(),
            P(),
        ),
        out_specs=(P(("clip", "head"), "seq", None, None), P(("clip", "head"), "seq", None, None)),
        check_vma=False,
    )
```

```python
import functools
import math

import jax
import jax.numpy as jnp
from jax import lax
from jax.experimental import pallas as pl
from jax.experimental.pallas import tpu as pltpu
from jax.sharding import PartitionSpec as P

HEAD_DIM = 128


def from_behind(value, axis, steps):
    count = lax.axis_size(axis)
    first, last = (max(0, -steps), min(count, count - steps))
    return lax.ppermute(value, axis, [(source, source + steps) for source in range(first, last)])


def padded_2(x, sides, width):
    for axis, dim in sides:
        peers, length = (lax.axis_size(axis), x.shape[dim])
        up = [(i, (i + 1) % peers) for i in range(peers - 1)]
        down = [(j, i) for i, j in up]
        last = lax.slice_in_dim(x, length - width, length, axis=dim)
        first = lax.slice_in_dim(x, 0, width, axis=dim)
        before = lax.ppermute(last, axis, up)
        after = lax.ppermute(first, axis, down)
        x = jnp.concatenate([before, x, after], axis=dim)
    return x


def head_latent(hidden, head_shift, head_scale, head_weight, head_bias):
    values = hidden.astype(jnp.float32)
    center = values - jnp.mean(values, -1, keepdims=True)
    spread = jnp.mean(center * center, -1, keepdims=True)
    normed = (center * lax.rsqrt(spread + 1e-06) * (1.0 + head_scale) + head_shift).astype(
        jnp.bfloat16
    )
    flat = normed.reshape(-1, normed.shape[-1])
    latent = (jnp.dot(flat, head_weight, preferred_element_type=jnp.float32) + head_bias).astype(
        jnp.bfloat16
    )
    frames, height, breadth = (hidden.shape[0], hidden.shape[1], hidden.shape[2])
    channels = head_weight.shape[1] // 4
    patches = latent.reshape(frames, height, breadth, 2, 2, channels).transpose(0, 1, 3, 2, 4, 5)
    return patches.reshape(frames, height * 2, breadth * 2, channels)


def convolve(padded, frames, conv_weight, conv_bias, norm_gain):
    height = padded.shape[1] - 2
    breadth = padded.shape[2] - 2
    stacked = jnp.concatenate(
        [
            padded[
                time_off : time_off + frames,
                row_off : row_off + height,
                col_off : col_off + breadth,
            ]
            for time_off in range(3)
            for row_off in range(3)
            for col_off in range(3)
        ],
        -1,
    )
    kernel = conv_weight.reshape(-1, conv_weight.shape[-1])
    linear = (
        jnp.dot(stacked.reshape(-1, stacked.shape[-1]), kernel, preferred_element_type=jnp.float32)
        + conv_bias
    )
    normed = linear * lax.rsqrt(jnp.mean(linear * linear, -1, keepdims=True) + 1e-06) * norm_gain
    return jax.nn.silu(normed).astype(jnp.bfloat16).reshape(frames, height, breadth, -1)


def attend_block(carried, block_keys, block_values, query_heads):
    running, denominator, weighted = carried
    scores = jnp.einsum("hqd,khd->hqk", query_heads, block_keys, preferred_element_type=jnp.float32)
    scores = scores * query_heads.shape[-1] ** (-0.5)
    newmax = jnp.maximum(running, jnp.max(scores, -1))
    factor = jnp.exp(running - newmax)
    weights = jnp.exp(scores - newmax[..., None])
    denominator = denominator * factor + jnp.sum(weights, -1)
    product = jnp.einsum(
        "hqk,khd->hqd",
        weights.astype(jnp.bfloat16),
        block_values,
        preferred_element_type=jnp.float32,
    )
    weighted = weighted * factor[..., None] + product
    return (newmax, denominator, weighted)


def fold_pieces(query_heads, carried, pieces):
    key_piece, value_piece = pieces
    frames, height, breadth = (key_piece.shape[0], key_piece.shape[1], key_piece.shape[2])
    heads_here, head_width = (query_heads.shape[0], query_heads.shape[2])
    group_rows = 4

    def regroup(one_piece):
        shaped = one_piece.reshape(
            frames, height // group_rows, group_rows, breadth, heads_here, head_width
        )
        shaped = shaped.transpose(1, 0, 2, 3, 4, 5)
        return shaped.reshape(
            height // group_rows, frames * group_rows * breadth, heads_here, head_width
        )

    def advance(inner, blocks):
        return (attend_block(inner, blocks[0], blocks[1], query_heads), None)

    carried, _ = lax.scan(advance, carried, (regroup(key_piece), regroup(value_piece)))
    return carried


def on_device_gathered(
    queries,
    attn_keys,
    attn_values,
    residual,
    out_weight,
    out_gate,
    head_shift,
    head_scale,
    head_weight,
    head_bias,
    conv_weight,
    conv_bias,
    norm_gain,
):
    head_count = lax.axis_size("head")
    frames_dev = queries.shape[0]
    group_width = queries.shape[3] // head_count
    head_width = HEAD_DIM
    heads_here = group_width // head_width
    local_queries, local_keys, local_values = (
        lax.all_to_all(queries, "head", split_axis=3, concat_axis=0, tiled=True),
        lax.all_to_all(attn_keys, "head", split_axis=3, concat_axis=0, tiled=True),
        lax.all_to_all(attn_values, "head", split_axis=3, concat_axis=0, tiled=True),
    )
    frames_all, height, breadth = (
        local_queries.shape[0],
        local_queries.shape[1],
        local_queries.shape[2],
    )
    count = frames_all * height * breadth
    query_heads = local_queries.reshape(count, heads_here, head_width).transpose(1, 0, 2)
    initial = (
        jnp.full((heads_here, count), -1e30, jnp.float32),
        jnp.zeros((heads_here, count), jnp.float32),
        jnp.zeros((heads_here, count, head_width), jnp.float32),
    )
    carried = fold_pieces(
        query_heads,
        initial,
        (
            lax.all_gather(local_keys, "seq", axis=1, tiled=True),
            lax.all_gather(local_values, "seq", axis=1, tiled=True),
        ),
    )
    running, denominator, weighted = carried
    attended = (weighted / denominator[..., None]).astype(jnp.bfloat16)
    attended = attended.transpose(1, 0, 2).reshape(count, group_width)
    partial_value = jnp.dot(
        attended,
        lax.all_gather(out_weight, "seq", axis=1, tiled=True),
        preferred_element_type=jnp.float32,
    )
    partial_value = partial_value.reshape(frames_all, height, breadth, partial_value.shape[-1])
    owned = lax.psum_scatter(
        partial_value.astype(jnp.bfloat16), "head", scatter_dimension=0, tiled=True
    ).astype(jnp.float32)
    hidden = (residual.astype(jnp.float32) + out_gate * owned).astype(jnp.bfloat16)
    own_video = head_latent(hidden, head_shift, head_scale, head_weight, head_bias)
    earlier = from_behind(own_video, "head", 1)
    video = jnp.concatenate([earlier, own_video], 0)
    extended = padded_2(video, (("seq", 1),), 1)
    padded = jnp.pad(extended, ((0, 0), (0, 0), (1, 1), (0, 0)))
    features = convolve(padded, frames_dev, conv_weight, conv_bias, norm_gain)
    return (hidden, features)


MESH = pl.DeviceIdType.MESH


class Plan:
    def __init__(self, ns, nh, queries, residual, out_weight):
        self.ns, self.nh = ns, nh
        self.frames = queries.shape[0]
        self.cells = queries.shape[1] * queries.shape[2]
        self.inner = queries.shape[3]
        self.tokens = self.frames * self.cells
        self.group = self.inner // nh // HEAD_DIM
        self.few = max(1, self.group // 6)
        self.width = residual.shape[3]
        self.columns = out_weight.shape[1]
        self.slots = ns * nh
        self.chunk = 256 if self.columns % 256 == 0 else 128
        self.chunks = self.columns // self.chunk
        self.cuts = 2
        self.counts = (self.few, 2 * self.few, 2 * self.few, self.few)
        self.owner = [o for o, count in enumerate(self.counts) for _ in range(count)]

    def fits(self, queries, head_weight, conv_weight):
        return (
            self.nh == 4
            and self.ns == 4
            and self.group == 6 * self.few
            and self.inner == self.nh * self.group * HEAD_DIM
            and self.frames == 2
            and self.cells % 16 == 0
            and self.columns % 128 == 0
            and queries.shape[1] == 1
            and head_weight.shape[1] == 64
            and conv_weight.shape[3] == 16
            and conv_weight.shape[4] % 128 == 0
            and self.slots * self.tokens <= 1024
        )


def source_row(o, row):
    step = 1 if row > o else -1
    return o if o in (0, 3) and abs(row - o) < 3 else row - step


def due(o, unit, f, row):
    away = abs(row - o)
    if o in (0, 3):
        return (0, 15.0, 16.5, 18.5)[away] + 6.5 * f
    if row == 3 * (o // 2):
        return (10.0, 18.0)[unit] + 1.4 * f
    return (15.7, 19.4)[unit] + 3.0 * (away - 1) + 1.4 * f


def block_kernel(
    plan,
    q_hbm, k_hbm, v_hbm, res_hbm, w_hbm, hw_hbm,
    gate_hbm, shift_hbm, scale_hbm, bias_hbm, cw_hbm, cb_hbm, gain_hbm,
    hidden_ref, near_ref, wide_ref, rows_ref,
    qkv, got, att, weight, res, head_w, head_t, gate_ref, shift_ref, scale_ref, bias_ref, wide_bias, conv_w, bias_row, gain_row, term, landed0, landed1, final, patch, halo,
    far, load_sem, local_sem, own_sem, s1, r1, s3, r3, s4, r4, s5, r5, s6, r6, s7, r7,
):
    p = plan
    s = lax.axis_index("seq")
    h = lax.axis_index("head")
    core, across = h & 1, h >> 1
    row_pair = (bias_row, gain_row)

    def pair_of(seq_index):
        return ((seq_index + 1) >> 1) & 1

    place = s >> 1
    here = ((pair_of(s) * 2 + core) * 2 + across) * 2 + place
    at_end = (s == 0) | (s == p.ns - 1)
    wide = p.few * HEAD_DIM

    def columns_of(seq_index, head_index, unit):
        before = p.few * (jnp.maximum(2 * seq_index - 1, 0) + unit)
        return pl.ds(pl.multiple_of((head_index * p.group + before) * HEAD_DIM, HEAD_DIM), wide)

    sources = (q_hbm, k_hbm, v_hbm)
    loads = [pltpu.make_async_copy(ref, qkv.at[i], load_sem) for i, ref in enumerate(sources)]
    loaded = pltpu.make_async_copy(qkv, qkv, load_sem)
    late = [
        pltpu.make_async_copy(w_hbm, weight, local_sem.at[0]),
        pltpu.make_async_copy(res_hbm, res, local_sem.at[1]),
        pltpu.make_async_copy(head_w, head_w, local_sem.at[2]),
        pltpu.make_async_copy(gate_hbm, gate_ref, local_sem.at[3]),
        pltpu.make_async_copy(shift_hbm, shift_ref, local_sem.at[4]),
        pltpu.make_async_copy(scale_hbm, scale_ref, local_sem.at[5]),
        pltpu.make_async_copy(bias_hbm, bias_ref, local_sem.at[6]),
        pltpu.make_async_copy(cb_hbm, row_pair[0], local_sem.at[7]),
        pltpu.make_async_copy(gain_hbm, row_pair[1], local_sem.at[8]),
    ]
    quarter = hw_hbm.shape[0] // 4
    strips = [
        pltpu.make_async_copy(
            hw_hbm.at[pl.ds((2 * a + first) * quarter, count * quarter)],
            head_w.at[pl.ds((4 * a + place) * quarter, count * quarter)],
            local_sem.at[2],
        )
        for a in range(2)
        for place, first, count in ((0, 1, 1), (1, 0, 2), (3, 0, 1))
    ]
    conv_load = pltpu.make_async_copy(cw_hbm, conv_w, local_sem.at[9])

    def own_copies(unit):
        cols = columns_of(s, h, unit)
        return [
            pltpu.make_async_copy(ref.at[:, :, cols], got.at[unit, i, :, here], own_sem.at[unit])
            for i, ref in enumerate(sources)
        ]

    def own_copied(unit):
        part = got.at[unit, :, :, here]
        return pltpu.make_async_copy(part, part, own_sem.at[unit])

    for copy in loads:
        copy.start()

    def others(row, to_s):
        for dh in range(p.nh):
            if row != to_s or dh:
                yield lax.rem(h + dh, p.nh)

    def say(sem, **to):
        pl.semaphore_signal(sem, inc=1, device_id=to, device_id_type=MESH)

    barrier = pltpu.get_barrier_semaphore()
    for row in range(p.ns):
        @pl.when(s == row)
        def _():
            for to_s in range(max(row - 1, 0), min(row + 2, p.ns)):
                for to_h in others(row, to_s):
                    say(barrier, seq=to_s, head=to_h)

    for copy in own_copies(0):
        copy.start()

    @pl.when(jnp.logical_not(at_end))
    def _():
        for copy in own_copies(1):
            copy.start()

    loaded.wait()

    def exchange(stage, to_s, to_h):
        unit = stage // 2
        return pltpu.make_async_remote_copy(
            src_ref=qkv.at[:, :, :, columns_of(to_s, to_h, unit)],
            dst_ref=got.at[unit, :, :, here],
            send_sem=s1,
            recv_sem=r1.at[stage],
            device_id={"seq": to_s, "head": to_h},
            device_id_type=MESH,
        )

    def send_to(row, stages, away):
        for stage in stages:
            for to_s in range(p.ns):
                if (to_s in (0, p.ns - 1)) == (stage == 0) and abs(to_s - row) in away:
                    for to_h in others(row, to_s):
                        exchange(stage, to_s, to_h).start()

    for row in range(p.ns):
        @pl.when(s == row)
        def _():
            beside = [r for r in (row - 1, row + 1) if 0 <= r < p.ns]
            pl.semaphore_wait(barrier, p.nh * (1 + len(beside)) - 1)
            if len(beside) == 2:
                for to_s in beside:
                    say(far.at[0], seq=to_s)
            send_to(row, (1, 0), (0, 1))
            pl.semaphore_wait(far.at[0], 1)
            if len(beside) == 2:
                say(far.at[1], seq=3 * (row // 2))
            send_to(row, (1, 0), (2,))
            if len(beside) == 1:
                pl.semaphore_wait(far.at[1], 1)
                send_to(row, (0,), (3,))
            send_to(row, (2,), range(p.ns))

    def arrived(stage):
        parts = got.at[stage // 2, :, :, pl.ds(0, p.slots - 1)]
        pltpu.make_async_copy(parts, parts, r1.at[stage]).wait()

    conv_load.start()
    for copy in late[:2] + strips + late[3:]:
        copy.start()
    wide_ref[...] = jnp.zeros_like(wide_ref)
    conv_load.wait()
    spread_weights(conv_w, wide_ref)
    for copy in late:
        copy.wait()
    for i, row in enumerate(row_pair):
        rows_ref[i] = row[...]
    wide_bias[...] = spread_bias(bias_ref[...])
    head_t[...] = head_w[...].T

    def hop(f, head, cut, to_s, relayed):
        rows = p.slots * p.cells // p.cuts
        piece = att.at[f, head, pl.ds(cut * rows, rows)]
        return pltpu.make_async_remote_copy(
            src_ref=piece,
            dst_ref=piece,
            send_sem=s3.at[relayed],
            recv_sem=r3.at[f, head, cut],
            device_id={"seq": to_s},
            device_id_type=MESH,
        )

    def attend(f, j, cuts=slice(None)):
        unit, lanes = j // p.few, pl.ds(j % p.few * HEAD_DIM, HEAD_DIM)
        q = got[unit, 0, f, cuts, :, lanes].reshape(-1, HEAD_DIM)
        k = got[unit, 1, :, :, :, lanes].reshape(-1, HEAD_DIM)
        v = got[unit, 2, :, :, :, lanes].reshape(-1, HEAD_DIM)
        scores = lax.dot_general(
            q, k, (((1,), (1,)), ((), ())), preferred_element_type=jnp.float32
        )
        scale = HEAD_DIM ** (-0.5) * math.log2(math.e)
        weights = jnp.exp2((scores - jnp.max(scores, -1, keepdims=True)) * scale)
        denominator = jnp.sum(weights, -1, keepdims=True)
        product = jnp.dot(weights.astype(jnp.bfloat16), v, preferred_element_type=jnp.float32)
        rows = slice((cuts.start or 0) * p.cells, (cuts.stop or p.slots) * p.cells)
        head = p.few * jnp.maximum(2 * s - 1, 0) + j
        att[f, head, rows] = (product / denominator).astype(jnp.bfloat16)

    parts = [(f, cut) for f in range(p.frames) for cut in range(p.cuts)]

    def targets(head, row):
        o = p.owner[head]
        rows = [r for r in range(p.ns) if r != o and source_row(o, r) == row]
        return sorted(rows, key=lambda r: -abs(r - row))

    def send_own(f, j, outward=(True, False), cuts=range(p.cuts)):
        for row in range(p.ns):
            if j < p.counts[row]:
                head = p.owner.index(row) + j

                @pl.when(s == row)
                def _():
                    rows = [r for r in targets(head, row) if (r in (0, p.ns - 1)) in outward]
                    for cut in cuts:
                        for to_s in rows:
                            hop(f, head, cut, to_s, 0).start()

    def order(row):
        def when(item):
            f, cut, head = item
            o = p.owner[head]
            passive = not targets(head, row)
            return (f, cut, passive, due(o, (head - p.owner.index(o)) // p.few, f, row), head)

        heads = [head for head in range(p.group) if p.owner[head] != row]
        return sorted(((f, cut, head) for f, cut in parts for head in heads), key=when)

    def gather(todo):
        for row in range(p.ns):
            @pl.when(s == row)
            def _():
                for f, cut, head in todo(row):
                    hop(f, head, cut, row, 1).wait_recv()
                    for to_s in targets(head, row):
                        hop(f, head, cut, to_s, 1).start()

    def early_part(row):
        def early(f, cut, head):
            unit = (head - p.owner.index(p.owner[head])) // p.few
            return f == 0 and unit == 0 and row in (1, 2) and targets(head, row)

        return [item for item in order(row) if early(*item)]

    def first_part(row):
        if row not in (0, p.ns - 1):
            return []
        return [(0, 0, head) for head in range(p.group) if p.owner[head] == (1, 2)[row // 3]]

    def gather_part(f, cut):
        def todo(row):
            done = early_part(row) + first_part(row)
            return [item for item in order(row) if item[:2] == (f, cut) and item not in done]

        gather(todo)

    own_copied(0).wait()
    pl.when(at_end)(functools.partial(arrived, 0))
    pl.when(jnp.logical_not(at_end))(functools.partial(arrived, 1))
    def at_ends(act, *of):
        pl.when(at_end)(functools.partial(act, *of))

    def at_middle(act, *of):
        pl.when(jnp.logical_not(at_end))(functools.partial(act, *of))

    for f in range(p.frames):
        for j in range(p.few):
            attend(f, j)
            if f == 0:
                send_own(f, j)
            else:
                at_middle(send_own, f, j, (True,))

    @at_middle
    def _():
        own_copied(1).wait()
        arrived(2)
        half = p.slots // p.cuts
        for cut in range(p.cuts):
            for j in range(p.few, 2 * p.few):
                attend(0, j, slice(cut * half, (cut + 1) * half))
                send_own(0, j, cuts=(cut,))
        for j in range(p.few):
            send_own(1, j, (False,))
        gather(early_part)
        for j in range(p.few, 2 * p.few):
            attend(1, j)
            send_own(1, j, (False,))

    @at_ends
    def _():
        gather(first_part)
        for j in range(p.few):
            send_own(1, j)

    groups = [(0, 2), (2, p.chunks - 2)] if p.chunks > 3 else [(0, p.chunks)]

    def to_partner(f, cut, g):
        part = pl.ds(*groups[g])
        return pltpu.make_async_remote_copy(
            src_ref=term.at[f, cut, part, 1 - core],
            dst_ref=landed0.at[f, cut, part],
            send_sem=s4,
            recv_sem=r4.at[f, cut, g],
            device_id={"head": h + 1 - 2 * core},
            device_id_type=MESH,
        )

    def project(f, cut):
        length = p.slots * p.cells // p.cuts
        own = pl.ds(cut * length, length)
        rows = jnp.concatenate([att[f, head, own] for head in range(p.group)], axis=1)
        for g, (start, count) in enumerate(groups):
            for c in range(start, start + count):
                cols = pl.ds(c * p.chunk, p.chunk)
                product = jnp.dot(rows, weight[:, cols], preferred_element_type=jnp.float32)
                term[f, cut, c] = product.astype(jnp.bfloat16).reshape(term.shape[3:])
            to_partner(f, cut, g).start()

    def across_x(f, cut, g):
        part = pl.ds(*groups[g])
        return pltpu.make_async_remote_copy(
            src_ref=landed0.at[f, cut, part, 1 - across],
            dst_ref=landed1.at[f, cut, part],
            send_sem=s5,
            recv_sem=r5.at[f, cut, g],
            device_id={"head": h + 2 - 4 * across},
            device_id_type=MESH,
        )

    def pair_sum(f, cut, g):
        part = pl.ds(*groups[g])
        to_partner(f, cut, g).wait_recv()
        total = term[f, cut, part, core].astype(jnp.float32)
        total = total + landed0[f, cut, part].astype(jnp.float32)
        landed0[f, cut, part] = total.astype(jnp.bfloat16)
        across_x(f, cut, g).start()

    def full_sum(f, cut, g):
        part = pl.ds(*groups[g])
        across_x(f, cut, g).wait_recv()
        total = landed0[f, cut, part, across].astype(jnp.float32)
        total = total + landed1[f, cut, part].astype(jnp.float32)
        landed1[f, cut, part] = total.astype(jnp.bfloat16)
        for ds in (2, 1, 3):
            to_s = lax.rem(s + ds, p.ns)

            @pl.when(pair_of(to_s) == cut)
            def _():
                pltpu.make_async_remote_copy(
                    src_ref=landed1.at[f, cut, part, to_s >> 1],
                    dst_ref=final.at[f, part, ds - 1],
                    send_sem=s6,
                    recv_sem=r6.at[f, g],
                    device_id={"seq": to_s},
                    device_id_type=MESH,
                ).start()

    both = range(len(groups))

    def pair_sums(f, cut):
        for g in both:
            pair_sum(f, cut, g)

    def full_sums(f, cut):
        for g in both:
            full_sum(f, cut, g)

    gather_part(*parts[0])
    at_middle(gather_part, *parts[1])

    @at_middle
    def _():
        for j in range(p.few, 2 * p.few):
            send_own(1, j, (True,))

    project(*parts[0])
    at_ends(gather_part, *parts[1])
    project(*parts[1])
    pair_sums(*parts[0])
    at_middle(gather_part, *parts[2])
    at_middle(gather_part, *parts[3])
    pair_sums(*parts[1])
    at_ends(gather_part, *parts[2])
    project(*parts[2])

    def third_sums():
        pair_sums(*parts[2])
        full_sums(*parts[0])

    pl.when(at_end & (core == 0))(third_sums)
    at_ends(gather_part, *parts[3])
    project(*parts[3])
    pl.when(at_end & (core == 1))(third_sums)
    at_middle(pair_sums, *parts[2])
    pair_sums(*parts[3])
    full_sums(*parts[1])
    at_middle(full_sums, *parts[0])
    at_middle(full_sums, *parts[3])
    full_sums(*parts[2])
    at_ends(full_sums, *parts[3])
    def finish(f, c, sums):
        for g, (start, count) in enumerate(groups):
            if c == start:
                pieces = final.at[f, pl.ds(start, count)]
                pltpu.make_async_copy(pieces, pieces, r6.at[f, g]).wait()
        rows = slice(f * p.cells, (f + 1) * p.cells)
        for ds in range(p.ns):
            j = lax.rem(s - ds + p.ns, p.ns)
            cols = pl.ds(pl.multiple_of(j * p.columns + c * p.chunk, 128), p.chunk)
            part = landed1[f, pair_of(s), c, place] if ds == 0 else final[f, c, ds - 1]
            added = gate_ref[:, cols] * part.astype(jnp.float32)
            value = (res[rows, cols].astype(jnp.float32) + added).astype(jnp.bfloat16)
            hidden_ref[rows, cols] = value
            sums = sums + jnp.sum(value.astype(jnp.float32), -1, keepdims=True)
        return sums

    def head(f, sums):
        rows = slice(f * p.cells, (f + 1) * p.cells)
        center = hidden_ref[rows].astype(jnp.float32) - sums / p.width
        spread = jnp.mean(center * center, -1, keepdims=True)
        normed = center * lax.rsqrt(spread + 1e-06) * (1.0 + scale_ref[...]) + shift_ref[...]
        values = jnp.dot(
            normed.astype(jnp.bfloat16), head_t[...], preferred_element_type=jnp.float32
        )
        values = (values + wide_bias[...]).astype(jnp.bfloat16).astype(jnp.float32)
        column = lax.broadcasted_iota(jnp.int32, values.shape, 0)
        place = lax.broadcasted_iota(jnp.int32, values.shape, 1) % (4 * quarter)
        left = jnp.where(column == 0, 0.0, pltpu.roll(values, 1, 0))
        right = jnp.where(column == p.cells - 1, 0.0, pltpu.roll(values, p.cells - 1, 0))
        strip = jnp.where(place < quarter, left, jnp.where(place < 3 * quarter, values, right))
        patch[rows] = strip.astype(jnp.bfloat16)

    sums = [jnp.zeros((p.cells, 1), jnp.float32) for _ in range(p.frames)]
    for c in range(p.chunks):
        sums[0] = finish(0, c, sums[0])
    head(0, sums[0])
    for c in range(p.chunks):
        sums[1] = finish(1, c, sums[1])
    head(1, sums[1])
    blank = jnp.zeros(patch.shape, patch.dtype)

    moves = [(0, 1), (0, -1), (1, 0), (1, 1), (1, -1)]

    def edge(index, sign):
        dh, ds = moves[index]
        return (
            (h + sign * dh >= 0) & (h + sign * dh < p.nh)
            & (s + sign * ds >= 0) & (s + sign * ds < p.ns)
        )

    def reach(index):
        dh, ds = moves[index]
        return pltpu.make_async_remote_copy(
            src_ref=patch,
            dst_ref=halo.at[index],
            send_sem=s7.at[index],
            recv_sem=r7.at[index],
            device_id={"seq": lax.rem(s + ds + p.ns, p.ns), "head": lax.rem(h + dh, p.nh)},
            device_id_type=MESH,
        )

    for index in range(len(moves)):

        @pl.when(edge(index, 1))
        def _():
            reach(index).start()

    near_ref[1, 1] = patch[...]
    for index, (dh, ds) in enumerate(moves):

        @pl.when(edge(index, -1))
        def _():
            reach(index).wait_recv()
            near_ref[1 - dh, 1 - ds] = halo[index]

        @pl.when(jnp.logical_not(edge(index, -1)))
        def _():
            near_ref[1 - dh, 1 - ds] = blank

    for index in range(len(moves)):

        @pl.when(edge(index, 1))
        def _():
            reach(index).wait_send()

    def all_sent(part, sem):
        pltpu.make_async_copy(part, part, sem).wait()

    for row in range(p.ns):
        @pl.when(s == row)
        def _():
            foreign = (p.nh * p.group - p.counts[row]) * HEAD_DIM
            all_sent(qkv.at[:, :, :, pl.ds(0, foreign)], s1)
            for relayed in range(2):
                heads = [head for head in range(p.group) if (p.owner[head] != row) == relayed]
                sent = sum(len(targets(head, row)) for head in heads)
                if sent:
                    all_sent(att.at[:, pl.ds(0, sent)], s3.at[relayed])

    all_sent(landed0, s4)
    all_sent(landed1, s5)
    all_sent(final, s6)


def spread_weights(conv_w, wide_ref):
    taps, depth, channels = conv_w.shape
    part = depth // 3
    for a in range(2):
        for dt in range(3):
            for dy in range(3):
                base = (1 - a + dy) * 4 * part
                tap = conv_w[dt * 3 + dy]
                wide_ref[a, dt, base : base + depth, :channels] = tap
                wide_ref[a, dt, base + part : base + part + depth, channels:] = tap


def spread_bias(bias):
    size = bias.shape[1]
    part = size // 4
    source = lax.broadcasted_iota(jnp.int32, (size, 2 * size), 0)
    target = lax.broadcasted_iota(jnp.int32, (size, 2 * size), 1)
    place = target % size
    moved = jnp.where(place < part, part, jnp.where(place < 3 * part, -part, -3 * part))
    pick = jnp.where(source == target // size * 2 * part + place + moved, 1.0, 0.0)
    total, rest = 0.0, bias
    for _ in range(3):
        piece = rest.astype(jnp.bfloat16)
        rest = rest - piece.astype(jnp.float32)
        total = total + jnp.dot(
            piece, pick.astype(jnp.bfloat16), preferred_element_type=jnp.float32
        )
    return total


def conv_kernel(
    cells, hidden_ref, strip, wide_ref, rows_ref, hidden_out, features_out, mixed, features, sems
):
    channels = features.shape[-1]
    hidden_copy = pltpu.make_async_copy(hidden_ref, hidden_out, sems.at[0])
    hidden_copy.start()

    def at_time(dt, row):
        if dt == 1:
            return jnp.concatenate([strip[0, row, cells:], strip[1, row, :cells]], axis=0)
        return strip[dt // 2, row]

    for a in range(2):
        taken = [at_time(dt, row) for dt in range(3) for row in (a, a + 1)]
        linear = jnp.dot(
            jnp.concatenate(taken, axis=1),
            wide_ref[a].reshape(-1, 2 * channels),
            preferred_element_type=jnp.float32,
        )
        for b in range(2):
            value = linear[:, b * channels : (b + 1) * channels] + rows_ref[0:1]
            square = jnp.mean(value * value, -1, keepdims=True)
            value = value * lax.rsqrt(square + 1e-06) * rows_ref[1:2]
            value = value / (1.0 + jnp.exp(-value))
            for k in range(channels // 128):
                for f in range(2):
                    piece = value[f * cells : (f + 1) * cells, k * 128 : (k + 1) * 128]
                    mixed[k, f, a, pl.ds(b, cells, 2)] = piece
    for k in range(channels // 128):
        features[:, :, :, k * 128 : (k + 1) * 128] = mixed[k].astype(jnp.bfloat16)
    features_copy = pltpu.make_async_copy(features, features_out, sems.at[1])
    features_copy.start()
    hidden_copy.wait()
    features_copy.wait()


def on_device(
    queries,
    attn_keys,
    attn_values,
    residual,
    out_weight,
    out_gate,
    head_shift,
    head_scale,
    head_weight,
    head_bias,
    conv_weight,
    conv_bias,
    norm_gain,
):
    ns, nh = lax.axis_size("seq"), lax.axis_size("head")
    p = Plan(ns, nh, queries, residual, out_weight)
    if not p.fits(queries, head_weight, conv_weight):
        return on_device_gathered(
            queries, attn_keys, attn_values, residual, out_weight, out_gate, head_shift,
            head_scale, head_weight, head_bias, conv_weight, conv_bias, norm_gain,
        )
    frames, height, breadth, inner = queries.shape
    t, cells, width, patch_size = p.tokens, p.cells, p.width, head_weight.shape[1]
    dma, bf16 = pltpu.SemaphoreType.DMA, jnp.bfloat16
    lanes = 2 * patch_size
    channels = conv_weight.shape[-1]
    hbm = pl.BlockSpec(memory_space=pltpu.HBM)
    vmem = pl.BlockSpec(memory_space=pltpu.VMEM)
    hidden, near, wide, conv_rows = pl.pallas_call(
        functools.partial(block_kernel, p),
        out_shape=(
            jax.ShapeDtypeStruct((t, width), bf16),
            jax.ShapeDtypeStruct((2, 3, t, lanes), bf16),
            jax.ShapeDtypeStruct((2, 3, 2 * lanes, 2 * channels), bf16),
            jax.ShapeDtypeStruct((2, channels), jnp.float32),
        ),
        in_specs=[hbm] * 13,
        out_specs=(vmem,) * 4,
        scratch_shapes=[
            pltpu.VMEM((3, frames, cells, inner), bf16),
            pltpu.VMEM((2, 3, frames, p.slots, cells, p.few * HEAD_DIM), bf16),
            pltpu.VMEM((frames, p.group, p.slots * cells, HEAD_DIM), bf16),
            pltpu.VMEM(out_weight.shape, bf16),
            pltpu.VMEM((t, width), bf16),
            pltpu.VMEM((lanes, width), bf16),
            pltpu.VMEM((width, lanes), bf16),
            pltpu.VMEM((1, width), jnp.float32),
            pltpu.VMEM((1, width), jnp.float32),
            pltpu.VMEM((1, width), jnp.float32),
            pltpu.VMEM((1, patch_size), jnp.float32),
            pltpu.VMEM((1, lanes), jnp.float32),
            pltpu.VMEM((9, 3 * conv_weight.shape[3], channels), bf16),
            pltpu.VMEM((channels,), jnp.float32),
            pltpu.VMEM((channels,), jnp.float32),
            pltpu.VMEM((frames, p.cuts, p.chunks, 2, 2, 2, cells, p.chunk), bf16),
            pltpu.VMEM((frames, p.cuts, p.chunks, 2, 2, cells, p.chunk), bf16),
            pltpu.VMEM((frames, p.cuts, p.chunks, 2, cells, p.chunk), bf16),
            pltpu.VMEM((frames, p.chunks, ns - 1, cells, p.chunk), bf16),
            pltpu.VMEM((t, lanes), bf16),
            pltpu.VMEM((5, t, lanes), bf16),
            pltpu.SemaphoreType.REGULAR((2,)),
            dma(()),
            dma((10,)),
            dma((2,)),
            dma(()),
            dma((3,)),
            dma((2,)),
            dma((frames, p.group, p.cuts)),
            dma(()),
            dma((frames, p.cuts, 2)),
            dma(()),
            dma((frames, p.cuts, 2)),
            dma(()),
            dma((frames, 2)),
            dma((5,)),
            dma((5,)),
        ],
        compiler_params=pltpu.CompilerParams(
            collective_id=0, has_side_effects=True, vmem_limit_bytes=16 * 1024 * 1024
        ),
    )(*(pltpu.with_memory_space_constraint(x, pltpu.HBM) for x in (
        queries.reshape(frames, cells, inner),
        attn_keys.reshape(frames, cells, inner),
        attn_values.reshape(frames, cells, inner),
        residual.reshape(t, width),
        out_weight,
        head_weight.T,
        out_gate.reshape(1, -1),
        head_shift.reshape(1, -1),
        head_scale.reshape(1, -1),
        head_bias.reshape(1, -1),
        conv_weight.reshape(9, -1, channels),
        conv_bias,
        norm_gain,
    )))
    hidden, features = pl.pallas_call(
        functools.partial(conv_kernel, cells),
        out_shape=(
            jax.ShapeDtypeStruct((t, width), bf16),
            jax.ShapeDtypeStruct((frames, 2, 2 * cells, channels), bf16),
        ),
        in_specs=[vmem] * 4,
        out_specs=(hbm, hbm),
        scratch_shapes=[
            pltpu.VMEM((channels // 128, frames, 2, 2 * cells, 128), jnp.float32),
            pltpu.VMEM((frames, 2, 2 * cells, channels), bf16),
            dma((2,)),
        ],
        compiler_params=pltpu.CompilerParams(vmem_limit_bytes=8 * 1024 * 1024),
    )(hidden, near, wide, conv_rows)
    return (hidden.reshape(residual.shape), features)


def solution(mesh):
    return jax.shard_map(
        on_device,
        mesh=mesh,
        in_specs=(
            P(("clip", "head"), "seq", None, None),
            P(("clip", "head"), "seq", None, None),
            P(("clip", "head"), "seq", None, None),
            P(("clip", "head"), "seq", None, None),
            P("head", "seq"),
            P(),
            P(),
            P(),
            P(),
            P(),
            P(),
            P(),
            P(),
        ),
        out_specs=(P(("clip", "head"), "seq", None, None), P(("clip", "head"), "seq", None, None)),
        check_vma=False,
    )
```

```python
import functools
import math

import jax
import jax.numpy as jnp
from jax import lax
from jax.experimental import pallas as pl
from jax.experimental.pallas import tpu as pltpu
from jax.sharding import PartitionSpec as P

HEAD_DIM = 128


def from_behind(value, axis, steps):
    count = lax.axis_size(axis)
    first, last = (max(0, -steps), min(count, count - steps))
    return lax.ppermute(value, axis, [(source, source + steps) for source in range(first, last)])


def padded_2(x, sides, width):
    for axis, dim in sides:
        peers, length = (lax.axis_size(axis), x.shape[dim])
        up = [(i, (i + 1) % peers) for i in range(peers - 1)]
        down = [(j, i) for i, j in up]
        last = lax.slice_in_dim(x, length - width, length, axis=dim)
        first = lax.slice_in_dim(x, 0, width, axis=dim)
        before = lax.ppermute(last, axis, up)
        after = lax.ppermute(first, axis, down)
        x = jnp.concatenate([before, x, after], axis=dim)
    return x


def head_latent(hidden, head_shift, head_scale, head_weight, head_bias):
    values = hidden.astype(jnp.float32)
    center = values - jnp.mean(values, -1, keepdims=True)
    spread = jnp.mean(center * center, -1, keepdims=True)
    normed = (center * lax.rsqrt(spread + 1e-06) * (1.0 + head_scale) + head_shift).astype(
        jnp.bfloat16
    )
    flat = normed.reshape(-1, normed.shape[-1])
    latent = (jnp.dot(flat, head_weight, preferred_element_type=jnp.float32) + head_bias).astype(
        jnp.bfloat16
    )
    frames, height, breadth = (hidden.shape[0], hidden.shape[1], hidden.shape[2])
    channels = head_weight.shape[1] // 4
    patches = latent.reshape(frames, height, breadth, 2, 2, channels).transpose(0, 1, 3, 2, 4, 5)
    return patches.reshape(frames, height * 2, breadth * 2, channels)


def convolve(padded, frames, conv_weight, conv_bias, norm_gain):
    height = padded.shape[1] - 2
    breadth = padded.shape[2] - 2
    stacked = jnp.concatenate(
        [
            padded[
                time_off : time_off + frames,
                row_off : row_off + height,
                col_off : col_off + breadth,
            ]
            for time_off in range(3)
            for row_off in range(3)
            for col_off in range(3)
        ],
        -1,
    )
    kernel = conv_weight.reshape(-1, conv_weight.shape[-1])
    linear = (
        jnp.dot(stacked.reshape(-1, stacked.shape[-1]), kernel, preferred_element_type=jnp.float32)
        + conv_bias
    )
    normed = linear * lax.rsqrt(jnp.mean(linear * linear, -1, keepdims=True) + 1e-06) * norm_gain
    return jax.nn.silu(normed).astype(jnp.bfloat16).reshape(frames, height, breadth, -1)


def attend_block(carried, block_keys, block_values, query_heads):
    running, denominator, weighted = carried
    scores = jnp.einsum("hqd,khd->hqk", query_heads, block_keys, preferred_element_type=jnp.float32)
    scores = scores * query_heads.shape[-1] ** (-0.5)
    newmax = jnp.maximum(running, jnp.max(scores, -1))
    factor = jnp.exp(running - newmax)
    weights = jnp.exp(scores - newmax[..., None])
    denominator = denominator * factor + jnp.sum(weights, -1)
    product = jnp.einsum(
        "hqk,khd->hqd",
        weights.astype(jnp.bfloat16),
        block_values,
        preferred_element_type=jnp.float32,
    )
    weighted = weighted * factor[..., None] + product
    return (newmax, denominator, weighted)


def fold_pieces(query_heads, carried, pieces):
    key_piece, value_piece = pieces
    frames, height, breadth = (key_piece.shape[0], key_piece.shape[1], key_piece.shape[2])
    heads_here, head_width = (query_heads.shape[0], query_heads.shape[2])
    group_rows = 4

    def regroup(one_piece):
        shaped = one_piece.reshape(
            frames, height // group_rows, group_rows, breadth, heads_here, head_width
        )
        shaped = shaped.transpose(1, 0, 2, 3, 4, 5)
        return shaped.reshape(
            height // group_rows, frames * group_rows * breadth, heads_here, head_width
        )

    def advance(inner, blocks):
        return (attend_block(inner, blocks[0], blocks[1], query_heads), None)

    carried, _ = lax.scan(advance, carried, (regroup(key_piece), regroup(value_piece)))
    return carried


def on_device_gathered(
    queries,
    attn_keys,
    attn_values,
    residual,
    out_weight,
    out_gate,
    head_shift,
    head_scale,
    head_weight,
    head_bias,
    conv_weight,
    conv_bias,
    norm_gain,
):
    head_count = lax.axis_size("head")
    frames_dev = queries.shape[0]
    group_width = queries.shape[3] // head_count
    head_width = HEAD_DIM
    heads_here = group_width // head_width
    local_queries, local_keys, local_values = (
        lax.all_to_all(queries, "head", split_axis=3, concat_axis=0, tiled=True),
        lax.all_to_all(attn_keys, "head", split_axis=3, concat_axis=0, tiled=True),
        lax.all_to_all(attn_values, "head", split_axis=3, concat_axis=0, tiled=True),
    )
    frames_all, height, breadth = (
        local_queries.shape[0],
        local_queries.shape[1],
        local_queries.shape[2],
    )
    count = frames_all * height * breadth
    query_heads = local_queries.reshape(count, heads_here, head_width).transpose(1, 0, 2)
    initial = (
        jnp.full((heads_here, count), -1e30, jnp.float32),
        jnp.zeros((heads_here, count), jnp.float32),
        jnp.zeros((heads_here, count, head_width), jnp.float32),
    )
    carried = fold_pieces(
        query_heads,
        initial,
        (
            lax.all_gather(local_keys, "seq", axis=1, tiled=True),
            lax.all_gather(local_values, "seq", axis=1, tiled=True),
        ),
    )
    running, denominator, weighted = carried
    attended = (weighted / denominator[..., None]).astype(jnp.bfloat16)
    attended = attended.transpose(1, 0, 2).reshape(count, group_width)
    partial_value = jnp.dot(
        attended,
        lax.all_gather(out_weight, "seq", axis=1, tiled=True),
        preferred_element_type=jnp.float32,
    )
    partial_value = partial_value.reshape(frames_all, height, breadth, partial_value.shape[-1])
    owned = lax.psum_scatter(
        partial_value.astype(jnp.bfloat16), "head", scatter_dimension=0, tiled=True
    ).astype(jnp.float32)
    hidden = (residual.astype(jnp.float32) + out_gate * owned).astype(jnp.bfloat16)
    own_video = head_latent(hidden, head_shift, head_scale, head_weight, head_bias)
    earlier = from_behind(own_video, "head", 1)
    video = jnp.concatenate([earlier, own_video], 0)
    extended = padded_2(video, (("seq", 1),), 1)
    padded = jnp.pad(extended, ((0, 0), (0, 0), (1, 1), (0, 0)))
    features = convolve(padded, frames_dev, conv_weight, conv_bias, norm_gain)
    return (hidden, features)


MESH = pl.DeviceIdType.MESH


class Plan:
    def __init__(self, ns, nh, queries, residual, out_weight):
        self.ns, self.nh = ns, nh
        self.frames = queries.shape[0]
        self.cells = queries.shape[1] * queries.shape[2]
        self.inner = queries.shape[3]
        self.tokens = self.frames * self.cells
        self.group = self.inner // nh // HEAD_DIM
        self.few = max(1, self.group // 6)
        self.width = residual.shape[3]
        self.columns = out_weight.shape[1]
        self.slots = ns * nh
        self.chunk = 256 if self.columns % 256 == 0 else 128
        self.chunks = self.columns // self.chunk
        self.cuts = 2
        self.counts = (self.few, 2 * self.few, 2 * self.few, self.few)
        self.owner = [o for o, count in enumerate(self.counts) for _ in range(count)]

    def fits(self, queries, head_weight, conv_weight):
        return (
            self.nh == 4
            and self.ns == 4
            and self.group == 6 * self.few
            and self.inner == self.nh * self.group * HEAD_DIM
            and self.frames == 2
            and self.cells % 16 == 0
            and self.columns % 128 == 0
            and queries.shape[1] == 1
            and head_weight.shape[1] == 64
            and conv_weight.shape[3] == 16
            and conv_weight.shape[4] % 128 == 0
            and self.slots * self.tokens <= 1024
        )


def source_row(o, row):
    step = 1 if row > o else -1
    return o if o in (0, 3) and abs(row - o) < 3 else row - step


def due(o, unit, f, row):
    away = abs(row - o)
    if o in (0, 3):
        return (0, 15.0, 16.5, 18.5)[away] + 6.5 * f
    if row == 3 * (o // 2):
        return (10.0, 18.0)[unit] + 1.4 * f
    return (15.7, 19.4)[unit] + 3.0 * (away - 1) + 1.4 * f


def block_kernel(
    plan,
    q_hbm, k_hbm, v_hbm, res_hbm, w_hbm, hw_hbm,
    gate_hbm, shift_hbm, scale_hbm, bias_hbm, cw_hbm, cb_hbm, gain_hbm,
    hidden_ref, near_ref, wide_ref, rows_ref,
    qkv, got, att, weight, res, head_w, head_t, gate_ref, shift_ref, scale_ref, bias_ref, wide_bias, conv_w, bias_row, gain_row, term, landed0, landed1, final, patch, halo,
    far, load_sem, local_sem, own_sem, s1, r1, s3, r3, s4, r4, s5, r5, s6, r6, s7, r7,
):
    p = plan
    s = lax.axis_index("seq")
    h = lax.axis_index("head")
    core, across = h & 1, h >> 1
    row_pair = (bias_row, gain_row)

    def pair_of(seq_index):
        return ((seq_index + 1) >> 1) & 1

    place = s >> 1
    here = ((pair_of(s) * 2 + core) * 2 + across) * 2 + place
    at_end = (s == 0) | (s == p.ns - 1)
    wide = p.few * HEAD_DIM

    def columns_of(seq_index, head_index, unit):
        before = p.few * (jnp.maximum(2 * seq_index - 1, 0) + unit)
        return pl.ds(pl.multiple_of((head_index * p.group + before) * HEAD_DIM, HEAD_DIM), wide)

    sources = (q_hbm, k_hbm, v_hbm)
    loads = [pltpu.make_async_copy(ref, qkv.at[i], load_sem) for i, ref in enumerate(sources)]
    loaded = pltpu.make_async_copy(qkv, qkv, load_sem)
    late = [
        pltpu.make_async_copy(w_hbm, weight, local_sem.at[0]),
        pltpu.make_async_copy(res_hbm, res, local_sem.at[1]),
        pltpu.make_async_copy(head_w, head_w, local_sem.at[2]),
        pltpu.make_async_copy(gate_hbm, gate_ref, local_sem.at[3]),
        pltpu.make_async_copy(shift_hbm, shift_ref, local_sem.at[4]),
        pltpu.make_async_copy(scale_hbm, scale_ref, local_sem.at[5]),
        pltpu.make_async_copy(bias_hbm, bias_ref, local_sem.at[6]),
        pltpu.make_async_copy(cb_hbm, row_pair[0], local_sem.at[7]),
        pltpu.make_async_copy(gain_hbm, row_pair[1], local_sem.at[8]),
    ]
    quarter = hw_hbm.shape[0] // 4
    strips = [
        pltpu.make_async_copy(
            hw_hbm.at[pl.ds((2 * a + first) * quarter, count * quarter)],
            head_w.at[pl.ds((4 * a + place) * quarter, count * quarter)],
            local_sem.at[2],
        )
        for a in range(2)
        for place, first, count in ((0, 1, 1), (1, 0, 2), (3, 0, 1))
    ]
    conv_load = pltpu.make_async_copy(cw_hbm, conv_w, local_sem.at[9])

    def own_copies(unit):
        cols = columns_of(s, h, unit)
        return [
            pltpu.make_async_copy(ref.at[:, :, cols], got.at[unit, i, :, here], own_sem.at[unit])
            for i, ref in enumerate(sources)
        ]

    def own_copied(unit):
        part = got.at[unit, :, :, here]
        return pltpu.make_async_copy(part, part, own_sem.at[unit])

    for copy in loads:
        copy.start()

    def others(row, to_s):
        for dh in range(p.nh):
            if row != to_s or dh:
                yield lax.rem(h + dh, p.nh)

    def say(sem, **to):
        pl.semaphore_signal(sem, inc=1, device_id=to, device_id_type=MESH)

    barrier = pltpu.get_barrier_semaphore()
    for row in range(p.ns):
        @pl.when(s == row)
        def _():
            for to_s in range(max(row - 1, 0), min(row + 2, p.ns)):
                for to_h in others(row, to_s):
                    say(barrier, seq=to_s, head=to_h)

    for copy in own_copies(0):
        copy.start()

    @pl.when(jnp.logical_not(at_end))
    def _():
        for copy in own_copies(1):
            copy.start()

    loaded.wait()

    def exchange(stage, to_s, to_h):
        unit = stage // 2
        return pltpu.make_async_remote_copy(
            src_ref=qkv.at[:, :, :, columns_of(to_s, to_h, unit)],
            dst_ref=got.at[unit, :, :, here],
            send_sem=s1,
            recv_sem=r1.at[stage],
            device_id={"seq": to_s, "head": to_h},
            device_id_type=MESH,
        )

    def send_to(row, stages, away):
        for stage in stages:
            for to_s in range(p.ns):
                if (to_s in (0, p.ns - 1)) == (stage == 0) and abs(to_s - row) in away:
                    for to_h in others(row, to_s):
                        exchange(stage, to_s, to_h).start()

    for row in range(p.ns):
        @pl.when(s == row)
        def _():
            beside = [r for r in (row - 1, row + 1) if 0 <= r < p.ns]
            pl.semaphore_wait(barrier, p.nh * (1 + len(beside)) - 1)
            if len(beside) == 2:
                for to_s in beside:
                    say(far.at[0], seq=to_s)
            send_to(row, (1, 0), (0, 1))
            pl.semaphore_wait(far.at[0], 1)
            if len(beside) == 2:
                say(far.at[1], seq=3 * (row // 2))
            send_to(row, (1, 0), (2,))
            if len(beside) == 1:
                pl.semaphore_wait(far.at[1], 1)
                send_to(row, (0,), (3,))
            send_to(row, (2,), range(p.ns))

    def arrived(stage):
        parts = got.at[stage // 2, :, :, pl.ds(0, p.slots - 1)]
        pltpu.make_async_copy(parts, parts, r1.at[stage]).wait()

    conv_load.start()
    for copy in late[:2] + strips + late[3:]:
        copy.start()
    wide_ref[...] = jnp.zeros_like(wide_ref)
    conv_load.wait()
    spread_weights(conv_w, wide_ref)
    for copy in late:
        copy.wait()
    for i, row in enumerate(row_pair):
        rows_ref[i] = row[...]
    wide_bias[...] = spread_bias(bias_ref[...])
    head_t[...] = head_w[...].T

    def hop(f, head, cut, to_s, relayed):
        rows = p.slots * p.cells // p.cuts
        piece = att.at[f, head, pl.ds(cut * rows, rows)]
        return pltpu.make_async_remote_copy(
            src_ref=piece,
            dst_ref=piece,
            send_sem=s3.at[relayed],
            recv_sem=r3.at[f, head, cut],
            device_id={"seq": to_s},
            device_id_type=MESH,
        )

    def attend(f, j, cuts=slice(None)):
        unit, lanes = j // p.few, pl.ds(j % p.few * HEAD_DIM, HEAD_DIM)
        q = got[unit, 0, f, cuts, :, lanes].reshape(-1, HEAD_DIM)
        k = got[unit, 1, :, :, :, lanes].reshape(-1, HEAD_DIM)
        v = got[unit, 2, :, :, :, lanes].reshape(-1, HEAD_DIM)
        scores = lax.dot_general(
            q, k, (((1,), (1,)), ((), ())), preferred_element_type=jnp.float32
        )
        scale = HEAD_DIM ** (-0.5) * math.log2(math.e)
        weights = jnp.exp2((scores - jnp.max(scores, -1, keepdims=True)) * scale)
        denominator = jnp.sum(weights, -1, keepdims=True)
        product = jnp.dot(weights.astype(jnp.bfloat16), v, preferred_element_type=jnp.float32)
        rows = slice((cuts.start or 0) * p.cells, (cuts.stop or p.slots) * p.cells)
        head = p.few * jnp.maximum(2 * s - 1, 0) + j
        att[f, head, rows] = (product / denominator).astype(jnp.bfloat16)

    parts = [(f, cut) for f in range(p.frames) for cut in range(p.cuts)]

    def targets(head, row):
        o = p.owner[head]
        rows = [r for r in range(p.ns) if r != o and source_row(o, r) == row]
        return sorted(rows, key=lambda r: -abs(r - row))

    def send_own(f, j, outward=(True, False), cuts=range(p.cuts)):
        for row in range(p.ns):
            if j < p.counts[row]:
                head = p.owner.index(row) + j

                @pl.when(s == row)
                def _():
                    rows = [r for r in targets(head, row) if (r in (0, p.ns - 1)) in outward]
                    for cut in cuts:
                        for to_s in rows:
                            hop(f, head, cut, to_s, 0).start()

    def order(row):
        def when(item):
            f, cut, head = item
            o = p.owner[head]
            passive = not targets(head, row)
            return (f, cut, passive, due(o, (head - p.owner.index(o)) // p.few, f, row), head)

        heads = [head for head in range(p.group) if p.owner[head] != row]
        return sorted(((f, cut, head) for f, cut in parts for head in heads), key=when)

    def gather(todo):
        for row in range(p.ns):
            @pl.when(s == row)
            def _():
                for f, cut, head in todo(row):
                    hop(f, head, cut, row, 1).wait_recv()
                    for to_s in targets(head, row):
                        hop(f, head, cut, to_s, 1).start()

    def early_part(row):
        def early(f, cut, head):
            unit = (head - p.owner.index(p.owner[head])) // p.few
            return f == 0 and unit == 0 and row in (1, 2) and targets(head, row)

        return [item for item in order(row) if early(*item)]

    def first_part(row):
        if row not in (0, p.ns - 1):
            return []
        return [(0, 0, head) for head in range(p.group) if p.owner[head] == (1, 2)[row // 3]]

    def gather_part(f, cut):
        def todo(row):
            done = early_part(row) + first_part(row)
            return [item for item in order(row) if item[:2] == (f, cut) and item not in done]

        gather(todo)

    own_copied(0).wait()
    pl.when(at_end)(functools.partial(arrived, 0))
    pl.when(jnp.logical_not(at_end))(functools.partial(arrived, 1))
    def at_ends(act, *of):
        pl.when(at_end)(functools.partial(act, *of))

    def at_middle(act, *of):
        pl.when(jnp.logical_not(at_end))(functools.partial(act, *of))

    for f in range(p.frames):
        for j in range(p.few):
            attend(f, j)
            if f == 0:
                send_own(f, j)
            else:
                at_middle(send_own, f, j, (True,))

    @at_middle
    def _():
        own_copied(1).wait()
        arrived(2)
        half = p.slots // p.cuts
        for cut in range(p.cuts):
            for j in range(p.few, 2 * p.few):
                attend(0, j, slice(cut * half, (cut + 1) * half))
                send_own(0, j, cuts=(cut,))
        for j in range(p.few):
            send_own(1, j, (False,))
        for j in range(p.few, 2 * p.few):
            attend(1, j)
        gather(early_part)
        for j in range(p.few, 2 * p.few):
            send_own(1, j, (False,))

    @at_ends
    def _():
        gather(first_part)
        for j in range(p.few):
            send_own(1, j)

    groups = [(0, 2), (2, p.chunks - 2)] if p.chunks > 3 else [(0, p.chunks)]

    def to_partner(f, cut, g):
        part = pl.ds(*groups[g])
        return pltpu.make_async_remote_copy(
            src_ref=term.at[f, cut, part, 1 - core],
            dst_ref=landed0.at[f, cut, part],
            send_sem=s4,
            recv_sem=r4.at[f, cut, g],
            device_id={"head": h + 1 - 2 * core},
            device_id_type=MESH,
        )

    def project(f, cut):
        length = p.slots * p.cells // p.cuts
        own = pl.ds(cut * length, length)
        rows = jnp.concatenate([att[f, head, own] for head in range(p.group)], axis=1)
        for g, (start, count) in enumerate(groups):
            for c in range(start, start + count):
                cols = pl.ds(c * p.chunk, p.chunk)
                product = jnp.dot(rows, weight[:, cols], preferred_element_type=jnp.float32)
                term[f, cut, c] = product.astype(jnp.bfloat16).reshape(term.shape[3:])
            to_partner(f, cut, g).start()

    def across_x(f, cut, g):
        part = pl.ds(*groups[g])
        return pltpu.make_async_remote_copy(
            src_ref=landed0.at[f, cut, part, 1 - across],
            dst_ref=landed1.at[f, cut, part],
            send_sem=s5,
            recv_sem=r5.at[f, cut, g],
            device_id={"head": h + 2 - 4 * across},
            device_id_type=MESH,
        )

    def pair_sum(f, cut, g):
        part = pl.ds(*groups[g])
        to_partner(f, cut, g).wait_recv()
        total = term[f, cut, part, core].astype(jnp.float32)
        total = total + landed0[f, cut, part].astype(jnp.float32)
        landed0[f, cut, part] = total.astype(jnp.bfloat16)
        across_x(f, cut, g).start()

    def full_sum(f, cut, g):
        part = pl.ds(*groups[g])
        across_x(f, cut, g).wait_recv()
        total = landed0[f, cut, part, across].astype(jnp.float32)
        total = total + landed1[f, cut, part].astype(jnp.float32)
        landed1[f, cut, part] = total.astype(jnp.bfloat16)
        for ds in (2, 1, 3):
            to_s = lax.rem(s + ds, p.ns)

            @pl.when(pair_of(to_s) == cut)
            def _():
                pltpu.make_async_remote_copy(
                    src_ref=landed1.at[f, cut, part, to_s >> 1],
                    dst_ref=final.at[f, part, ds - 1],
                    send_sem=s6,
                    recv_sem=r6.at[f, g],
                    device_id={"seq": to_s},
                    device_id_type=MESH,
                ).start()

    both = range(len(groups))

    def pair_sums(f, cut):
        for g in both:
            pair_sum(f, cut, g)

    def full_sums(f, cut):
        for g in both:
            full_sum(f, cut, g)

    gather_part(*parts[0])
    at_middle(gather_part, *parts[1])

    @at_middle
    def _():
        for j in range(p.few, 2 * p.few):
            send_own(1, j, (True,))

    project(*parts[0])
    at_ends(gather_part, *parts[1])
    project(*parts[1])
    pair_sums(*parts[0])
    at_middle(gather_part, *parts[2])
    at_middle(gather_part, *parts[3])
    pair_sums(*parts[1])
    at_ends(gather_part, *parts[2])
    project(*parts[2])

    def third_sums():
        pair_sums(*parts[2])
        full_sums(*parts[0])

    pl.when(at_end & (core == 0))(third_sums)
    at_ends(gather_part, *parts[3])
    project(*parts[3])
    pl.when(at_end & (core == 1))(third_sums)
    at_middle(pair_sums, *parts[2])
    pair_sums(*parts[3])
    full_sums(*parts[1])
    at_middle(full_sums, *parts[0])
    at_middle(full_sums, *parts[3])
    full_sums(*parts[2])
    at_ends(full_sums, *parts[3])
    def finish(f, c, sums):
        for g, (start, count) in enumerate(groups):
            if c == start:
                pieces = final.at[f, pl.ds(start, count)]
                pltpu.make_async_copy(pieces, pieces, r6.at[f, g]).wait()
        rows = slice(f * p.cells, (f + 1) * p.cells)
        for ds in range(p.ns):
            j = lax.rem(s - ds + p.ns, p.ns)
            cols = pl.ds(pl.multiple_of(j * p.columns + c * p.chunk, 128), p.chunk)
            part = landed1[f, pair_of(s), c, place] if ds == 0 else final[f, c, ds - 1]
            added = gate_ref[:, cols] * part.astype(jnp.float32)
            value = (res[rows, cols].astype(jnp.float32) + added).astype(jnp.bfloat16)
            hidden_ref[rows, cols] = value
            sums = sums + jnp.sum(value.astype(jnp.float32), -1, keepdims=True)
        return sums

    def head(f, sums):
        rows = slice(f * p.cells, (f + 1) * p.cells)
        center = hidden_ref[rows].astype(jnp.float32) - sums / p.width
        spread = jnp.mean(center * center, -1, keepdims=True)
        normed = center * lax.rsqrt(spread + 1e-06) * (1.0 + scale_ref[...]) + shift_ref[...]
        values = jnp.dot(
            normed.astype(jnp.bfloat16), head_t[...], preferred_element_type=jnp.float32
        )
        values = (values + wide_bias[...]).astype(jnp.bfloat16).astype(jnp.float32)
        column = lax.broadcasted_iota(jnp.int32, values.shape, 0)
        place = lax.broadcasted_iota(jnp.int32, values.shape, 1) % (4 * quarter)
        left = jnp.where(column == 0, 0.0, pltpu.roll(values, 1, 0))
        right = jnp.where(column == p.cells - 1, 0.0, pltpu.roll(values, p.cells - 1, 0))
        strip = jnp.where(place < quarter, left, jnp.where(place < 3 * quarter, values, right))
        patch[rows] = strip.astype(jnp.bfloat16)

    sums = [jnp.zeros((p.cells, 1), jnp.float32) for _ in range(p.frames)]
    for c in range(p.chunks):
        sums[0] = finish(0, c, sums[0])
    head(0, sums[0])
    for c in range(p.chunks):
        sums[1] = finish(1, c, sums[1])
    head(1, sums[1])
    blank = jnp.zeros(patch.shape, patch.dtype)

    moves = [(0, 1), (0, -1), (1, 0), (1, 1), (1, -1)]

    def edge(index, sign):
        dh, ds = moves[index]
        return (
            (h + sign * dh >= 0) & (h + sign * dh < p.nh)
            & (s + sign * ds >= 0) & (s + sign * ds < p.ns)
        )

    def reach(index):
        dh, ds = moves[index]
        return pltpu.make_async_remote_copy(
            src_ref=patch,
            dst_ref=halo.at[index],
            send_sem=s7.at[index],
            recv_sem=r7.at[index],
            device_id={"seq": lax.rem(s + ds + p.ns, p.ns), "head": lax.rem(h + dh, p.nh)},
            device_id_type=MESH,
        )

    for index in range(len(moves)):

        @pl.when(edge(index, 1))
        def _():
            reach(index).start()

    near_ref[1, 1] = patch[...]
    for index, (dh, ds) in enumerate(moves):

        @pl.when(edge(index, -1))
        def _():
            reach(index).wait_recv()
            near_ref[1 - dh, 1 - ds] = halo[index]

        @pl.when(jnp.logical_not(edge(index, -1)))
        def _():
            near_ref[1 - dh, 1 - ds] = blank

    for index in range(len(moves)):

        @pl.when(edge(index, 1))
        def _():
            reach(index).wait_send()

    def all_sent(part, sem):
        pltpu.make_async_copy(part, part, sem).wait()

    for row in range(p.ns):
        @pl.when(s == row)
        def _():
            foreign = (p.nh * p.group - p.counts[row]) * HEAD_DIM
            all_sent(qkv.at[:, :, :, pl.ds(0, foreign)], s1)
            for relayed in range(2):
                heads = [head for head in range(p.group) if (p.owner[head] != row) == relayed]
                sent = sum(len(targets(head, row)) for head in heads)
                if sent:
                    all_sent(att.at[:, pl.ds(0, sent)], s3.at[relayed])

    all_sent(landed0, s4)
    all_sent(landed1, s5)
    all_sent(final, s6)


def spread_weights(conv_w, wide_ref):
    taps, depth, channels = conv_w.shape
    part = depth // 3
    for a in range(2):
        for dt in range(3):
            for dy in range(3):
                base = (1 - a + dy) * 4 * part
                tap = conv_w[dt * 3 + dy]
                wide_ref[a, dt, base : base + depth, :channels] = tap
                wide_ref[a, dt, base + part : base + part + depth, channels:] = tap


def spread_bias(bias):
    size = bias.shape[1]
    part = size // 4
    source = lax.broadcasted_iota(jnp.int32, (size, 2 * size), 0)
    target = lax.broadcasted_iota(jnp.int32, (size, 2 * size), 1)
    place = target % size
    moved = jnp.where(place < part, part, jnp.where(place < 3 * part, -part, -3 * part))
    pick = jnp.where(source == target // size * 2 * part + place + moved, 1.0, 0.0)
    total, rest = 0.0, bias
    for _ in range(3):
        piece = rest.astype(jnp.bfloat16)
        rest = rest - piece.astype(jnp.float32)
        total = total + jnp.dot(
            piece, pick.astype(jnp.bfloat16), preferred_element_type=jnp.float32
        )
    return total


def conv_kernel(
    cells, hidden_ref, strip, wide_ref, rows_ref, hidden_out, features_out, mixed, features, sems
):
    channels = features.shape[-1]
    hidden_copy = pltpu.make_async_copy(hidden_ref, hidden_out, sems.at[0])
    hidden_copy.start()

    def at_time(dt, row):
        if dt == 1:
            return jnp.concatenate([strip[0, row, cells:], strip[1, row, :cells]], axis=0)
        return strip[dt // 2, row]

    for a in range(2):
        taken = [at_time(dt, row) for dt in range(3) for row in (a, a + 1)]
        linear = jnp.dot(
            jnp.concatenate(taken, axis=1),
            wide_ref[a].reshape(-1, 2 * channels),
            preferred_element_type=jnp.float32,
        )
        for b in range(2):
            value = linear[:, b * channels : (b + 1) * channels] + rows_ref[0:1]
            square = jnp.mean(value * value, -1, keepdims=True)
            value = value * lax.rsqrt(square + 1e-06) * rows_ref[1:2]
            value = value / (1.0 + jnp.exp(-value))
            for k in range(channels // 128):
                for f in range(2):
                    piece = value[f * cells : (f + 1) * cells, k * 128 : (k + 1) * 128]
                    mixed[k, f, a, pl.ds(b, cells, 2)] = piece
    for k in range(channels // 128):
        features[:, :, :, k * 128 : (k + 1) * 128] = mixed[k].astype(jnp.bfloat16)
    features_copy = pltpu.make_async_copy(features, features_out, sems.at[1])
    features_copy.start()
    hidden_copy.wait()
    features_copy.wait()


def on_device(
    queries,
    attn_keys,
    attn_values,
    residual,
    out_weight,
    out_gate,
    head_shift,
    head_scale,
    head_weight,
    head_bias,
    conv_weight,
    conv_bias,
    norm_gain,
):
    ns, nh = lax.axis_size("seq"), lax.axis_size("head")
    p = Plan(ns, nh, queries, residual, out_weight)
    if not p.fits(queries, head_weight, conv_weight):
        return on_device_gathered(
            queries, attn_keys, attn_values, residual, out_weight, out_gate, head_shift,
            head_scale, head_weight, head_bias, conv_weight, conv_bias, norm_gain,
        )
    frames, height, breadth, inner = queries.shape
    t, cells, width, patch_size = p.tokens, p.cells, p.width, head_weight.shape[1]
    dma, bf16 = pltpu.SemaphoreType.DMA, jnp.bfloat16
    lanes = 2 * patch_size
    channels = conv_weight.shape[-1]
    hbm = pl.BlockSpec(memory_space=pltpu.HBM)
    vmem = pl.BlockSpec(memory_space=pltpu.VMEM)
    hidden, near, wide, conv_rows = pl.pallas_call(
        functools.partial(block_kernel, p),
        out_shape=(
            jax.ShapeDtypeStruct((t, width), bf16),
            jax.ShapeDtypeStruct((2, 3, t, lanes), bf16),
            jax.ShapeDtypeStruct((2, 3, 2 * lanes, 2 * channels), bf16),
            jax.ShapeDtypeStruct((2, channels), jnp.float32),
        ),
        in_specs=[hbm] * 13,
        out_specs=(vmem,) * 4,
        scratch_shapes=[
            pltpu.VMEM((3, frames, cells, inner), bf16),
            pltpu.VMEM((2, 3, frames, p.slots, cells, p.few * HEAD_DIM), bf16),
            pltpu.VMEM((frames, p.group, p.slots * cells, HEAD_DIM), bf16),
            pltpu.VMEM(out_weight.shape, bf16),
            pltpu.VMEM((t, width), bf16),
            pltpu.VMEM((lanes, width), bf16),
            pltpu.VMEM((width, lanes), bf16),
            pltpu.VMEM((1, width), jnp.float32),
            pltpu.VMEM((1, width), jnp.float32),
            pltpu.VMEM((1, width), jnp.float32),
            pltpu.VMEM((1, patch_size), jnp.float32),
            pltpu.VMEM((1, lanes), jnp.float32),
            pltpu.VMEM((9, 3 * conv_weight.shape[3], channels), bf16),
            pltpu.VMEM((channels,), jnp.float32),
            pltpu.VMEM((channels,), jnp.float32),
            pltpu.VMEM((frames, p.cuts, p.chunks, 2, 2, 2, cells, p.chunk), bf16),
            pltpu.VMEM((frames, p.cuts, p.chunks, 2, 2, cells, p.chunk), bf16),
            pltpu.VMEM((frames, p.cuts, p.chunks, 2, cells, p.chunk), bf16),
            pltpu.VMEM((frames, p.chunks, ns - 1, cells, p.chunk), bf16),
            pltpu.VMEM((t, lanes), bf16),
            pltpu.VMEM((5, t, lanes), bf16),
            pltpu.SemaphoreType.REGULAR((2,)),
            dma(()),
            dma((10,)),
            dma((2,)),
            dma(()),
            dma((3,)),
            dma((2,)),
            dma((frames, p.group, p.cuts)),
            dma(()),
            dma((frames, p.cuts, 2)),
            dma(()),
            dma((frames, p.cuts, 2)),
            dma(()),
            dma((frames, 2)),
            dma((5,)),
            dma((5,)),
        ],
        compiler_params=pltpu.CompilerParams(
            collective_id=0, has_side_effects=True, vmem_limit_bytes=16 * 1024 * 1024
        ),
    )(*(pltpu.with_memory_space_constraint(x, pltpu.HBM) for x in (
        queries.reshape(frames, cells, inner),
        attn_keys.reshape(frames, cells, inner),
        attn_values.reshape(frames, cells, inner),
        residual.reshape(t, width),
        out_weight,
        head_weight.T,
        out_gate.reshape(1, -1),
        head_shift.reshape(1, -1),
        head_scale.reshape(1, -1),
        head_bias.reshape(1, -1),
        conv_weight.reshape(9, -1, channels),
        conv_bias,
        norm_gain,
    )))
    hidden, features = pl.pallas_call(
        functools.partial(conv_kernel, cells),
        out_shape=(
            jax.ShapeDtypeStruct((t, width), bf16),
            jax.ShapeDtypeStruct((frames, 2, 2 * cells, channels), bf16),
        ),
        in_specs=[vmem] * 4,
        out_specs=(hbm, hbm),
        scratch_shapes=[
            pltpu.VMEM((channels // 128, frames, 2, 2 * cells, 128), jnp.float32),
            pltpu.VMEM((frames, 2, 2 * cells, channels), bf16),
            dma((2,)),
        ],
        compiler_params=pltpu.CompilerParams(vmem_limit_bytes=8 * 1024 * 1024),
    )(hidden, near, wide, conv_rows)
    return (hidden.reshape(residual.shape), features)


def solution(mesh):
    return jax.shard_map(
        on_device,
        mesh=mesh,
        in_specs=(
            P(("clip", "head"), "seq", None, None),
            P(("clip", "head"), "seq", None, None),
            P(("clip", "head"), "seq", None, None),
            P(("clip", "head"), "seq", None, None),
            P("head", "seq"),
            P(),
            P(),
            P(),
            P(),
            P(),
            P(),
            P(),
            P(),
        ),
        out_specs=(P(("clip", "head"), "seq", None, None), P(("clip", "head"), "seq", None, None)),
        check_vma=False,
    )
```
